32 devices in a mesh: parts: 2 (over y), step: 4 (over z), frame: 2 (over x), head: 2 (over core).
Axes of the slice: x: 2, y: 2, z: 4, core: 2. Of those that a mesh axis runs over, the one named last changes fastest.
Arguments:
- start_noise: float32 [32, 256], P('parts', 'frame'), parts along dimension 0, may hold values from -6 to 6
- position: bfloat16 [256, 1152], P('frame'), may hold values from -6 to 6
- time_table: bfloat16 [128, 1152], replicated, may hold values from -6 to 6
- time_index: int32 [4], P('step'), may hold values from 0 to 127
- sched_index: int32 [4], P('step'), may hold values from 0 to 127
- coef_keep: float32 [128], replicated, may hold values from -0.06 to -0.01
- coef_noise: float32 [128], replicated, may hold values from 0.03 to 0.12
- w_in: bfloat16 [16, 1152], replicated, may hold values from -1.5 to 1.5
- norm_gain: float32 [1152], replicated, may hold values from 0.5 to 1.5
- w_qkv: bfloat16 [1152, 3, 1152], P('step', None, 'head'), may hold values from -4 to 4
- w_proj: bfloat16 [1152, 1152], P('step', 'head'), may hold values from -0.1875 to 0.1875
- w_final: bfloat16 [16, 1152], replicated, may hold values from -0.1875 to 0.1875
Outputs:
- trajectory: float32 [4, 32, 256], P('step', 'parts', 'frame'), parts along dimension 1
- residual_norms: float32 [8], P('parts'), parts along dimension 0
The draws below stay inside these ranges and needn't reach their ends.
There are 2 independent parts, one for each index of `parts`. The reference program is written for one: setup_inputs(seed, part) draws one part's arguments, and reference() takes and returns one part's arrays. A program takes and returns all parts, laid end to end along the dimension named above; an argument that names none is the same for every part. Nothing has to cross between parts.
All inputs are finite; a program needn't handle non-finite values.
Results may differ from the reference program's by a relative error of at most 0.0044.
Values may be sent and summed in bfloat16 or wider, within the bound.
A program may use at most 64 MiB of HBM per device.

```python
import math
import jax
import jax.numpy as jnp
from jax import lax

D = 1152
HEADS = 16
HDIM = 72
HQ = 1152
LAT_C = 16
NTOK = 256
STEPS = 4
SCHED = 128
ITERS = 4


def draw_w_qkv(key, part):
    base_key = jax.random.fold_in(jax.random.fold_in(key, 17), 0)
    base = jnp.clip(jax.random.normal(base_key, (D, 3, HQ), jnp.float32), -6.0, 6.0) * D ** (-0.5)
    return base.astype(jnp.bfloat16)


def place_ends(drawn, key, least, top_value):
    dims = drawn.shape
    place = [jax.random.randint(jax.random.fold_in(key, axis), (), 0, dims[axis]) for axis in range(len(dims))]
    drawn = drawn.at[tuple(place)].set(least)
    longest = dims.index(max(dims))
    place[longest] = (place[longest] + 1) % dims[longest]
    return drawn.at[tuple(place)].set(top_value)


def level_of(stream_key, shape, pieces, least, top_value):
    loudness, own = 1.0, jax.random.fold_in(stream_key, 6)
    for axis_at, parts in pieces:
        draws = jnp.exp(jax.random.uniform(jax.random.fold_in(own, axis_at), (parts,), jnp.float32, least / len(pieces), top_value / len(pieces)))
        loudness = loudness * jnp.repeat(draws, shape[axis_at] // parts).reshape([-1 if axis == axis_at else 1 for axis in range(len(shape))])
    return loudness


def scatter_about(own_key, dims, spread, most, shards=(), kind=jnp.bfloat16):
    array = spread * jax.random.normal(own_key, dims, jnp.float32)
    if shards:
        array = array * level_of(own_key, dims, shards, -0.22, 0.18)
    return jnp.clip(array, -most, most).astype(kind)


def setup_inputs(seed: int = 0, part: int = 0) -> dict:
    keys = jax.random.split(jax.random.key(seed), 13)
    part_keys = jax.random.split(jax.random.fold_in(keys[12], part), 13)
    start_noise = scatter_about(part_keys[0], (LAT_C, NTOK), 1.0, 6.0, ((1, 2),), jnp.float32)
    position = scatter_about(keys[1], (NTOK, D), 1.0, 6.0, ((0, 2),))
    time_table = scatter_about(keys[2], (SCHED, D), 1.0, 6.0)
    time_index = place_ends(jax.random.randint(keys[3], (STEPS,), 0, SCHED), jax.random.fold_in(keys[3], 1), 0, SCHED - 1).astype(jnp.int32)
    sched_index = place_ends(jax.random.randint(keys[4], (STEPS,), 0, SCHED), jax.random.fold_in(keys[4], 1), 0, SCHED - 1).astype(jnp.int32)
    coef_keep = jnp.clip(jax.random.uniform(keys[5], (SCHED,), jnp.float32, -0.06, -0.01), -0.06, -0.01)
    coef_noise = jnp.clip(jax.random.uniform(keys[6], (SCHED,), jnp.float32, 0.03, 0.12), 0.03, 0.12)
    w_in = scatter_about(keys[7], (LAT_C, D), LAT_C ** -0.5, 1.5)
    norm_gain = jnp.clip(1.0 + 0.1 * jax.random.normal(keys[8], (D,), jnp.float32), 0.5, 1.5)
    w_qkv = draw_w_qkv(jax.random.fold_in(keys[12], 71), part)
    w_proj = scatter_about(keys[10], (D, HQ), HQ ** -0.5, 0.1875, ((0, 4), (1, 2)))
    w_final = scatter_about(keys[11], (LAT_C, D), D ** -0.5, 0.1875)
    return dict(start_noise=start_noise, position=position, time_table=time_table, time_index=time_index, sched_index=sched_index, coef_keep=coef_keep, coef_noise=coef_noise, w_in=w_in, norm_gain=norm_gain, w_qkv=w_qkv, w_proj=w_proj, w_final=w_final)


def one_head(packed):
    queries, keys_part, values_part = packed
    scores = jnp.dot(queries, keys_part.T, preferred_element_type=jnp.float32) / math.sqrt(HDIM)
    top_score = lax.optimization_barrier(jnp.max(scores, axis=1, keepdims=True))
    weights_exp = jnp.exp(scores - top_score)
    totals = lax.optimization_barrier(jnp.sum(weights_exp, axis=1, keepdims=True))
    attended = jnp.dot(weights_exp.astype(jnp.bfloat16), values_part, preferred_element_type=jnp.float32)
    return (attended / totals).astype(jnp.bfloat16)

def denoise(latent, time_row, position, w_in, norm_gain, w_qkv, w_proj, w_final):
    latent_bf = latent.astype(jnp.bfloat16)
    hidden = jnp.dot(latent_bf.T, w_in, preferred_element_type=jnp.float32) + position.astype(jnp.float32) + time_row[None, :]
    normed = (hidden * lax.rsqrt(lax.optimization_barrier(jnp.mean(hidden * hidden, axis=1, keepdims=True)) + 1e-06) * norm_gain[None, :]).astype(jnp.bfloat16)
    projected = jnp.einsum('nd,dkq->nkq', normed.astype(jnp.float32), w_qkv.astype(jnp.float32)).astype(jnp.bfloat16)
    token_count = projected.shape[0]
    split_heads = projected.reshape(token_count, 3, HEADS, HDIM).transpose(1, 2, 0, 3)
    attended = lax.map(one_head, (split_heads[0], split_heads[1], split_heads[2]))
    attended = attended.transpose(1, 0, 2).reshape(token_count, HEADS * HDIM)
    branch = jnp.dot(attended, w_proj.T, preferred_element_type=jnp.float32)
    joined = (hidden + branch).astype(jnp.bfloat16)
    return jnp.dot(w_final, joined.T, preferred_element_type=jnp.float32)

def reference(start_noise, position, time_table, time_index, sched_index, coef_keep, coef_noise, w_in, norm_gain, w_qkv, w_proj, w_final):
    time_embed = time_table[time_index].astype(jnp.float32)
    keep_rate = coef_keep[sched_index]
    noise_rate = coef_noise[sched_index]
    states = jnp.broadcast_to(start_noise[None], (STEPS,) + start_noise.shape)

    def one_step(packed):
        return denoise(packed[0], packed[1], position, w_in, norm_gain, w_qkv, w_proj, w_final)
    residual_list = []
    drift_term = jnp.zeros_like(states)
    for iteration in range(ITERS):
        predicted = lax.map(one_step, (states, time_embed))
        drift_term = keep_rate[:, None, None] * states + noise_rate[:, None, None] * predicted
        running = jnp.cumsum(drift_term, axis=0)
        before = jnp.concatenate([jnp.zeros_like(running[:1]), running[:-1]], axis=0)
        new_states = start_noise[None] + before
        change = new_states - states
        residual_list.append(jnp.sqrt(jnp.mean(change * change) + 1e-06))
        states = new_states
    trajectory = states + drift_term
    return (trajectory, jnp.stack(residual_list))
```

```python
import functools
import math

import jax
import jax.numpy as jnp
from jax import lax
from jax.experimental import pallas as pl
from jax.experimental.pallas import tpu as pltpu
from jax.sharding import PartitionSpec as P

HDIM = 72
ITERS = 4


def entering(value, axis, combine, identity):
    count, here = (lax.axis_size(axis), lax.axis_index(axis))
    everything = lax.all_gather(value, axis)
    start = jnp.broadcast_to(jnp.asarray(identity, value.dtype), value.shape)

    def hop(k, before):
        reached = k < here
        new = combine(before, everything[k])
        return jnp.where(reached, new, before)

    return lax.fori_loop(0, count, hop, start)


def add_terms(first, second):
    return first + second


def local_any(
    start_noise,
    position,
    time_table,
    time_index,
    sched_index,
    coef_keep,
    coef_noise,
    w_in,
    norm_gain,
    w_qkv,
    w_proj,
    w_final,
):
    w_qkv_all, w_proj_all = (
        lax.all_gather(w_qkv, "step", axis=0, tiled=True),
        lax.all_gather(w_proj, "step", axis=0, tiled=True),
    )
    batch_steps = time_index.shape[0]
    row_count = start_noise.shape[1]
    table_rows = time_table.shape[0]
    pick_time = (time_index[:, None] == jnp.arange(table_rows)[None, :]).astype(jnp.bfloat16)
    time_embed = jnp.dot(pick_time, time_table, preferred_element_type=jnp.float32)
    pick_sched = (sched_index[:, None] == jnp.arange(table_rows)[None, :]).astype(jnp.float32)
    keep_rate = jnp.sum(pick_sched * coef_keep[None, :], axis=1)
    noise_rate = jnp.sum(pick_sched * coef_noise[None, :], axis=1)
    heads_local = w_qkv_all.shape[2] // HDIM
    cell_count = (
        batch_steps
        * lax.axis_size("step")
        * start_noise.shape[0]
        * row_count
        * lax.axis_size("frame")
    )
    states = start_noise[None]
    drift_term = jnp.zeros_like(states)
    residual_list = []
    for iteration in range(ITERS):
        latent_bf = states.astype(jnp.bfloat16)
        hidden = (
            jnp.einsum("bcr,cd->brd", latent_bf, w_in, preferred_element_type=jnp.float32)
            + position
            + time_embed[:, None, :]
        )
        normed = (
            hidden * lax.rsqrt(jnp.mean(hidden * hidden, axis=2, keepdims=True) + 1e-06) * norm_gain
        ).astype(jnp.bfloat16)
        projected = jnp.einsum(
            "brd,dkq->brkq", normed, w_qkv_all, preferred_element_type=jnp.float32
        ).astype(jnp.bfloat16)
        queries = projected[:, :, 0].reshape(batch_steps, row_count, heads_local, HDIM)
        score_scale = 1.0 / math.sqrt(HDIM)
        keys_values = projected[:, :, 1:3]
        piece = lax.all_gather(keys_values, "frame", axis=1, tiled=True)
        top_old = jnp.full((batch_steps, heads_local, row_count), -1e30, jnp.float32)
        piece_rows = piece.shape[1]
        keys_blk = piece[:, :, 0].reshape(batch_steps, piece_rows, heads_local, HDIM)
        values_blk = piece[:, :, 1].reshape(batch_steps, piece_rows, heads_local, HDIM)
        scores = (
            jnp.einsum("bqhe,bkhe->bhqk", queries, keys_blk, preferred_element_type=jnp.float32)
            * score_scale
        )
        top_new = jnp.maximum(top_old, jnp.max(scores, axis=3))
        weights_exp = jnp.exp(scores - top_new[:, :, :, None])
        total_new = jnp.sum(weights_exp, axis=3)
        update = jnp.einsum(
            "bhqk,bkhe->bqhe",
            weights_exp.astype(jnp.bfloat16),
            values_blk,
            preferred_element_type=jnp.float32,
        )
        accum = update
        top_final, total_final, accum = (top_new, total_new, accum)
        attended = accum / jnp.transpose(total_final, (0, 2, 1))[:, :, :, None]
        attn_mixed = attended.reshape(batch_steps, row_count, heads_local * HDIM).astype(
            jnp.bfloat16
        )
        partial_value = jnp.einsum(
            "brq,dq->brd", attn_mixed, w_proj_all, preferred_element_type=jnp.float32
        )
        head_total = lax.psum(partial_value, "head")
        joined = (hidden + head_total).astype(jnp.bfloat16)
        predicted = jnp.einsum("cd,brd->bcr", w_final, joined, preferred_element_type=jnp.float32)
        drift_term = keep_rate[:, None, None] * states + noise_rate[:, None, None] * predicted
        local_incl = jnp.cumsum(drift_term, axis=0)
        local_total = local_incl[-1]
        earlier = entering(local_total, "step", add_terms, jnp.zeros_like(local_total))
        before = earlier[None] + (local_incl - drift_term)
        new_states = start_noise[None] + before
        change = new_states - states
        square_sum = jnp.sum(change * change)
        summed = lax.psum(square_sum, ("step", "frame"))
        residual_list.append(jnp.sqrt(summed / cell_count + 1e-06))
        states = new_states
    residual_norms = jnp.stack(residual_list)
    trajectory = states + drift_term
    return (trajectory, residual_norms)


MESH = pl.DeviceIdType.MESH
F32 = jnp.float32
BF16 = jnp.bfloat16


def dot(a, b, ca=1, cb=0):
    return lax.dot_general(a, b, (((ca,), (cb,)), ((), ())), preferred_element_type=F32)


def dot_exact(a, b):
    return lax.dot_general(
        a, b, (((1,), (0,)), ((), ())), precision=lax.Precision.HIGHEST, preferred_element_type=F32
    )


def two(a):
    high = a.astype(BF16)
    return high, (a - high.astype(F32)).astype(BF16)


def evals_of(steps):
    return [(i, j) for j in range(steps - 1) for i in range(min(j, ITERS - 1) + 1)] + [
        (min(ITERS, steps) - 1, steps - 1)
    ]


def kernel(
    S,
    F,
    H,
    noise_hbm,
    pos_hbm,
    table_hbm,
    tidx_ref,
    sidx_ref,
    keep_hbm,
    coef_hbm,
    win_hbm,
    gain_hbm,
    wqkv_hbm,
    wproj_hbm,
    wfin_hbm,
    traj_ref,
    res_ref,
    pos_ref,
    table_ref,
    keep_ref,
    coef_ref,
    win_ref,
    gain_ref,
    wqkv_ref,
    wproj_ref,
    wfin_ref,
    wt_ref,
    at_ref,
    at_peer,
    side_ref,
    pv_ref,
    own_ref,
    near_send,
    near_recv,
    far_send,
    far_recv,
    mix_send,
    mix_buf,
    noise_buf,
    meta_buf,
    ends_buf,
    tab_buf,
    base_buf,
    plane_buf,
    ssem,
    rsem,
):
    s, f, h = (lax.axis_index(a) for a in ("step", "frame", "head"))
    loads = [
        pltpu.make_async_copy(src, dst, ssem.at[ssem.shape[0] - 1 - n])
        for n, (src, dst) in enumerate(
            (
                (gain_hbm, gain_ref),
                (pos_hbm, pos_ref),
                (wqkv_hbm, wqkv_ref),
                (wfin_hbm, wfin_ref),
                (wproj_hbm, wproj_ref),
                (keep_hbm, keep_ref),
                (coef_hbm, coef_ref),
                (noise_hbm, noise_buf.at[f]),
                (table_hbm, table_ref),
                (win_hbm, win_ref),
            )
        )
    ]
    for copy in loads:
        copy.start()
    PL = F * H
    q_me = f * H + h
    C, rows = noise_buf.shape[1:]
    D = pos_ref.shape[1]
    N = rows * F
    R = wqkv_ref.shape[1]
    lanes = table_ref.shape[0]
    e = lax.rem(s, 2)
    e_near = 1 - e
    s_near = s + 1 - 2 * e
    s_far = lax.rem(s + 2, S)
    HZ = wqkv_ref.shape[2] // (F * 2 * HDIM)
    B = HZ * HDIM
    QK = 2 * B
    V = HZ * C

    def step_peer(d):
        return {"step": lax.rem(s + d, S)}

    def group_peer(d):
        t = lax.rem(q_me + lax.rem(d, PL), PL)
        z = s_near if d >= PL else s
        return {"step": z, "frame": t // H, "head": lax.rem(t, H)}

    frame_peer = {"frame": 1 - f}

    barrier = pltpu.get_barrier_semaphore()
    for d in range(1, S):
        pl.semaphore_signal(barrier, inc=1, device_id=step_peer(d), device_id_type=MESH)
    for d in range(1, 2 * PL):
        if d != PL:
            pl.semaphore_signal(barrier, inc=1, device_id=group_peer(d), device_id_type=MESH)

    count = [0]
    started = []

    def send(src, dst, peer):
        k = count[0]
        count[0] += 1
        copy = pltpu.make_async_remote_copy(
            src_ref=src,
            dst_ref=dst,
            send_sem=ssem.at[k],
            recv_sem=rsem.at[k],
            device_id=peer,
            device_id_type=MESH,
        )
        copy.start()
        started.append(copy)
        return copy

    for copy in loads[:2]:
        copy.wait()
    gain = gain_ref[...].reshape(1, D)
    pos = pos_ref[...]
    at_ref[...] = jnp.transpose(pos.astype(F32) * gain).astype(BF16)
    loads[2].wait()
    for i in range(F):

        @pl.when(f == i)
        def _():
            for p in range(3):
                turned = jnp.transpose(wqkv_ref[p, :, i * 2 * B : (i + 1) * 2 * B])
                for t in range(2):
                    wt_ref[t, p * B : (p + 1) * B] = turned[t * B : (t + 1) * B]

    mine = pl.ds(pl.multiple_of(s * R, R), R)
    at_mine = at_ref[mine]
    near_send[0] = dot(wt_ref[e_near, 0:QK], at_mine).astype(BF16)
    loads[3].wait()
    loads[4].wait()
    rows_of = wfin_ref[:, 0:R].astype(F32)
    for j in range(1, S):
        rows_of = jnp.where(s == j, wfin_ref[:, j * R : (j + 1) * R].astype(F32), rows_of)
    folded = dot(rows_of.astype(BF16), wproj_ref[...])
    picked = folded[:, 0 : 2 * B]
    for i in range(1, F):
        picked = jnp.where(f == i, folded[:, i * 2 * B : (i + 1) * 2 * B], picked)
    mix_buf[s] = picked.astype(BF16)
    for copy in loads[5:8]:
        copy.wait()
    row_id = lax.broadcasted_iota(jnp.int32, (8, lanes), 0)
    lane_id = lax.broadcasted_iota(jnp.int32, (1, lanes), 1)
    hot_t = jnp.where(lane_id == tidx_ref[0], 1.0, 0.0)
    hot_s = lane_id == sidx_ref[0]
    keep = jnp.sum(jnp.where(hot_s, keep_ref[...], 0.0), axis=1, keepdims=True)
    coef = jnp.sum(jnp.where(hot_s, coef_ref[...], 0.0), axis=1, keepdims=True)
    meta_buf[s] = jnp.where(row_id == 0, hot_t, jnp.where(row_id == 1, keep, coef))

    pl.semaphore_wait(barrier, S - 1 + 2 * PL - 2)
    near = [send(near_send.at[0], near_recv.at[0], {"step": s_near})]
    turn = send(at_ref.at[mine], at_peer, frame_peer)
    order = sorted(range(1, S), key=lambda d: abs(d - S / 2))
    early = [send(meta_buf.at[s], meta_buf.at[s], step_peer(d)) for d in order]
    early += [send(mix_buf.at[s], mix_buf.at[s], step_peer(d)) for d in order]
    sides = [send(noise_buf.at[f], noise_buf.at[f], frame_peer)]

    own_ref[0] = dot(wt_ref[e, 0:QK], at_mine)
    pv_ref[0, :, 0:rows] = dot(wt_ref[e, QK : QK + B], at_mine).astype(BF16)
    pv_ref[1, :, 0:rows] = dot(wt_ref[e_near, QK : QK + B], at_mine).astype(BF16)
    for copy in loads[8:]:
        copy.wait()
    w_in = win_ref[...]
    ends = jnp.concatenate([w_in, wfin_ref[...]], axis=0)
    ends_in = dot(ends, w_in, 1, 1)
    posf = pos.astype(F32)
    sq_hi, sq_lo = two(posf * posf)
    ones = jnp.ones((8, D), BF16)
    ends_buf[f, 0 : 2 * C] = dot(ends, pos, 1, 1)
    ends_buf[f, 2 * C : 2 * C + 8] = dot(ones, sq_hi, 1, 1) + dot(ones, sq_lo, 1, 1)

    far = []

    def pass_on(i, low, high):
        near[i].wait_recv()
        total = own_ref[i, low:high] + near_recv[i, low:high].astype(F32)
        far_send[i, low:high] = total.astype(BF16)
        window = pl.ds(low, high - low)
        far.append(
            send(far_send.at[i, window], far_recv.at[i, window], {"step": s_far})
        )

    pass_on(0, 0, QK)
    turn.wait_recv()
    at_other = at_peer[...]
    near_send[1] = dot(wt_ref[e_near, 0:QK], at_other).astype(BF16)
    near.append(send(near_send.at[1], near_recv.at[1], {"step": s_near}))
    own_ref[1] = dot(wt_ref[e, 0:QK], at_other)
    pv_ref[0, :, rows : 2 * rows] = dot(wt_ref[e, QK : QK + B], at_other).astype(BF16)
    pv_ref[1, :, rows : 2 * rows] = dot(wt_ref[e_near, QK : QK + B], at_other).astype(BF16)

    for copy in early:
        copy.wait_recv()
    metas = [meta_buf[j] for j in range(S)]
    hot = jnp.concatenate(
        [m[0:1] for m in metas] + [jnp.zeros((8 - S, lanes), F32)], axis=0
    ).astype(BF16)
    keeps = [jnp.concatenate([m[1:2, :rows]] * F, axis=1) for m in metas]
    coefs = [jnp.concatenate([m[2:3, :rows]] * F, axis=1) for m in metas]
    temb = dot(hot, table_ref[...])
    temb_b = temb.astype(BF16)
    ends_buf[f, 2 * C + 8 : 2 * C + 16] = dot(temb_b, pos, 1, 1)
    sides.append(send(ends_buf.at[f], ends_buf.at[f], frame_peer))
    ends_t = dot(ends, temb_b, 1, 1)
    norm_t = jnp.sum(temb * temb, axis=1, keepdims=True)
    side = jnp.concatenate(
        [w_in.astype(F32), temb, jnp.zeros((128 - C - 8, D), F32)], axis=0
    )
    side_ref[...] = jnp.transpose(side * gain).astype(BF16)
    side_mine = side_ref[mine]
    mix = mix_buf[0].astype(F32)
    for j in range(1, S):
        mix = mix + mix_buf[j].astype(F32)
    mix_lane = lax.broadcasted_iota(jnp.int32, (V, B), 1) // HDIM
    mix_row = lax.broadcasted_iota(jnp.int32, (V, B), 0) // C

    def late_rows(role, member):
        pv_ref[role, :, 2 * rows : 2 * rows + 128] = dot(
            wt_ref[member, QK : QK + B], side_mine
        ).astype(BF16)
        part = jnp.where(member == 0, mix[:, 0:B], mix[:, B : 2 * B])
        block = jnp.where(
            mix_lane == mix_row, jnp.concatenate([part] * HZ, axis=0), 0.0
        )
        block_hi, block_lo = two(block)
        values = dot(jnp.concatenate([block_hi, block_lo], axis=0), pv_ref[role])
        values = values[0:V] + values[V : 2 * V]
        turned = dot(wt_ref[member, 0:QK], side_mine)
        packs = []
        for arr in (turned, values[:, 2 * rows : 2 * rows + 128]):
            size = arr.shape[0] // 4
            packed = arr[0:size]
            for g in range(1, 4):
                packed = packed + pltpu.roll(arr[g * size : (g + 1) * size], 32 * g, 1)
            packs.append(packed)
        return jnp.concatenate(
            [values[:, 0:rows], values[:, rows : 2 * rows]] + packs, axis=0
        )

    LATE = 2 * V + (QK + V) // 4
    near_send[2, 0:LATE] = late_rows(1, e_near).astype(BF16)
    tail_rows = pl.ds(0, LATE)
    near.append(
        send(near_send.at[2, tail_rows], near_recv.at[2, tail_rows], {"step": s_near})
    )
    own_ref[2, 0:LATE] = late_rows(0, e)
    pass_on(1, 0, QK)
    pass_on(2, 0, LATE)

    scale = 1.4426950408889634 / math.sqrt(HDIM)
    qk_row = lax.broadcasted_iota(jnp.int32, (QK, 1), 0)
    row_scale = jnp.where(qk_row < B, scale, 1.0)

    def whole(i, low, high):
        return far_send[i, low:high].astype(F32) + far_recv[i, low:high].astype(F32)

    far[0].wait_recv()
    tab_buf[f, 0:QK] = whole(0, 0, QK) * row_scale
    for copy in sides:
        copy.wait_recv()
    start = jnp.concatenate([noise_buf[i] for i in range(F)], axis=1)
    ends_all = jnp.concatenate([ends_buf[i] for i in range(F)], axis=1)
    ends_pos = ends_all[0 : 2 * C]
    norm_p = ends_all[2 * C : 2 * C + 1]
    cross = ends_all[2 * C + 8 : 2 * C + 16]
    norms = [norm_p + 2.0 * cross[j : j + 1] + norm_t[j : j + 1] for j in range(S)]
    for j in range(S):
        base_buf[j] = jnp.concatenate(
            [
                2.0 * (ends_pos[0:C] + ends_t[0:C, j : j + 1]),
                ends_pos[C : 2 * C] + ends_t[C : 2 * C, j : j + 1],
            ],
            axis=0,
        )
    far[1].wait_recv()
    tab_buf[1 - f, 0:QK] = whole(1, 0, QK) * row_scale
    far[2].wait_recv()
    last = whole(2, 0, LATE)
    tab_buf[f, QK : QK + V] = last[0:V]
    tab_buf[1 - f, QK : QK + V] = last[V : 2 * V]
    packed = last[2 * V : LATE]
    size = QK // 4
    big_qk = jnp.concatenate([packed[0:size, 32 * g : 32 * g + 32] for g in range(4)], axis=0)
    big_v = jnp.concatenate([packed[size:, 32 * g : 32 * g + 32] for g in range(4)], axis=0)
    ends_hi, ends_lo = two(
        jnp.concatenate([ends_in, jnp.zeros((2 * C, 32 - C), F32)], axis=1)
    )
    big = jnp.concatenate(
        [(big_qk * row_scale).astype(BF16), big_v.astype(BF16), ends_hi, ends_lo], axis=0
    )
    tab = jnp.concatenate([tab_buf[i] for i in range(F)], axis=1)
    T = QK + V
    hot_row = lax.broadcasted_iota(jnp.int32, (32 - C, N), 0)

    def partial(x, j):
        xb = x.astype(BF16)
        pick = jnp.where(hot_row == j, 1.0, 0.0).astype(BF16)
        lin = dot(big, jnp.concatenate([xb, pick], axis=0))
        tail = lin[T : T + 2 * C] + lin[T + 2 * C : T + 4 * C]
        base = base_buf[j]
        square = jnp.sum(xb.astype(F32) * (tail[0:C] + base[0:C]), axis=0, keepdims=True)
        square = jnp.maximum(square + norms[j], 0.0)
        r = lax.rsqrt(square * (1.0 / D) + 1e-06)
        lin = (lin[0:T] + tab) * r
        out = jnp.zeros((C, N), F32)
        for n in range(HZ):
            q = lin[n * HDIM : (n + 1) * HDIM].astype(BF16)
            k = lin[B + n * HDIM : B + (n + 1) * HDIM].astype(BF16)
            v_hi, v_lo = two(lin[QK + n * C : QK + (n + 1) * C])
            scores = dot(k, q, 0, 0)
            p = jnp.exp2(scores - jnp.max(scores, axis=0, keepdims=True)).astype(BF16)
            o = dot(jnp.concatenate([v_hi, v_lo, jnp.ones((C, N), BF16)], axis=0), p)
            out = out + (o[0:C] + o[C : 2 * C]) / o[2 * C : 2 * C + 1]
        return out, tail[C : 2 * C] + base[C : 2 * C]

    keys = evals_of(S)
    state, local_eps, drift, flying = {}, {}, {}, {}

    def launch(key):
        i, j = key
        n = keys.index(key)
        x = start
        for m in range(j if i else 0):
            x = x + drift[(min(i - 1, m), m)]
        state[key] = x
        part, local_eps[key] = partial(x, j)
        own = e * PL + q_me
        plane_buf[n, own] = part.astype(BF16)
        slot = plane_buf.at[n, own]
        flying[key] = [send(slot, slot, group_peer(d)) for d in range(1, 2 * PL)]

    def land(key):
        n, j = keys.index(key), key[1]
        for copy in flying[key]:
            copy.wait_recv()
        total = local_eps[key]
        for i in range(2 * PL):
            total = total + plane_buf[n, i].astype(F32)
        drift[key] = keeps[j] * state[key] + coefs[j] * total

    for act, key in PLAN:
        {"launch": launch, "land": land}[act](key)

    old = [start] * S
    norms_out = []
    for it in range(ITERS):
        new, run = [], start
        for j in range(S):
            new.append(run)
            if j < S - 1:
                run = run + drift[(min(it, j), j)]
        square = jnp.zeros((1, 1), F32)
        for j in range(S):
            change = new[j] - old[j]
            square = square + jnp.sum(
                jnp.sum(change * change, axis=0, keepdims=True), axis=1, keepdims=True
            )
        norms_out.append(jnp.sqrt(square / (S * C * N) + 1e-06))
        old = new
    lane = lax.broadcasted_iota(jnp.int32, res_ref.shape, 1)
    res = jnp.zeros(res_ref.shape, F32)
    for it in range(ITERS):
        res = jnp.where(lane == it, norms_out[it], res)
    res_ref[...] = res
    final = jnp.zeros((C, N), F32)
    for j in range(S):
        final = jnp.where(s == j, old[j] + drift[(min(ITERS - 1, j), j)], final)
    half = final[:, 0:rows]
    for i in range(1, F):
        half = jnp.where(f == i, final[:, i * rows : (i + 1) * rows], half)
    traj_ref[0] = half
    for copy in started:
        copy.wait_send()


PLAN = (
    ("launch", (0, 0)),
    ("launch", (0, 1)),
    ("launch", (0, 2)),
    ("land", (0, 0)),
    ("launch", (1, 1)),
    ("land", (0, 1)),
    ("launch", (1, 2)),
    ("land", (1, 1)),
    ("launch", (2, 2)),
    ("land", (0, 2)),
    ("land", (1, 2)),
    ("land", (2, 2)),
    ("launch", (3, 3)),
    ("land", (3, 3)),
)


def local_heads(
    start_noise,
    position,
    time_table,
    time_index,
    sched_index,
    coef_keep,
    coef_noise,
    w_in,
    norm_gain,
    w_qkv,
    w_proj,
    w_final,
):
    S, F, H = (lax.axis_size(a) for a in ("step", "frame", "head"))
    R = w_qkv.shape[0]
    C, rows = start_noise.shape
    D = position.shape[1]
    N = rows * F
    PL = F * H
    HZ = w_qkv.shape[2] // (F * 2 * HDIM)
    B = HZ * HDIM
    QK = 2 * B
    V = HZ * C
    n_evals = len(evals_of(S))
    n_sems = 2 * (S - 1) + 3 + 6 + n_evals * (2 * PL - 1)
    vmem = pl.BlockSpec(memory_space=pltpu.VMEM)
    smem = pl.BlockSpec(memory_space=pltpu.SMEM)
    here = pl.BlockSpec(memory_space=pl.ANY)
    traj, res = pl.pallas_call(
        functools.partial(kernel, S, F, H),
        out_shape=(pltpu.VMEM((1, C, rows), F32), pltpu.VMEM((1, ITERS), F32)),
        in_specs=[here, here, here, smem, smem] + [here] * 7,
        out_specs=(vmem, vmem),
        scratch_shapes=[
            pltpu.VMEM((rows, D), BF16),
            pltpu.VMEM(time_table.shape, BF16),
            pltpu.VMEM((1, coef_keep.shape[0]), F32),
            pltpu.VMEM((1, coef_noise.shape[0]), F32),
            pltpu.VMEM(w_in.shape, BF16),
            pltpu.VMEM((D,), F32),
            pltpu.VMEM((3, R, w_qkv.shape[2]), BF16),
            pltpu.VMEM(w_proj.shape, BF16),
            pltpu.VMEM(w_final.shape, BF16),
            pltpu.VMEM((2, QK + B, R), BF16),
            pltpu.VMEM((D, rows), BF16),
            pltpu.VMEM((R, rows), BF16),
            pltpu.VMEM((D, 128), BF16),
            pltpu.VMEM((2, B, N + 128), BF16),
            pltpu.VMEM((3, QK, rows), F32),
            pltpu.VMEM((3, QK, rows), BF16),
            pltpu.VMEM((3, QK, rows), BF16),
            pltpu.VMEM((3, QK, rows), BF16),
            pltpu.VMEM((3, QK, rows), BF16),
            pltpu.VMEM((C, 2 * B), BF16),
            pltpu.VMEM((S, C, 2 * B), BF16),
            pltpu.VMEM((F, C, rows), F32),
            pltpu.VMEM((S, 8, time_table.shape[0]), F32),
            pltpu.VMEM((F, 2 * C + 16, rows), F32),
            pltpu.VMEM((F, QK + V, rows), F32),
            pltpu.VMEM((S, 2 * C, N), F32),
            pltpu.VMEM((n_evals, 2 * PL, C, N), BF16),
            pltpu.SemaphoreType.DMA((n_sems + 10,)),
            pltpu.SemaphoreType.DMA((n_sems,)),
        ],
        compiler_params=pltpu.CompilerParams(
            collective_id=0, has_side_effects=True, vmem_limit_bytes=60 * 1024 * 1024
        ),
    )(
        start_noise,
        position,
        time_table,
        time_index,
        sched_index,
        coef_keep[None],
        coef_noise[None],
        w_in,
        norm_gain,
        jnp.transpose(w_qkv, (1, 0, 2)),
        w_proj,
        w_final,
    )
    return traj, res.reshape(ITERS)


def one_head_each(mesh, start_noise, time_index, w_qkv, time_table):
    S, F, H = (mesh.shape[a] for a in ("step", "frame", "head"))
    return (
        S == ITERS
        and time_index.shape[0] == S
        and w_qkv.shape[2] == S * F * H * HDIM
        and w_qkv.shape[0] % (16 * S) == 0
        and start_noise.shape[1] % (128 * F) == 0
        and start_noise.shape[1] // F <= time_table.shape[0]
        and time_table.shape[0] % 128 == 0
    )


def solution(mesh):
    def call(*args):
        fits = one_head_each(mesh, args[0], args[3], args[9], args[2])
        return jax.shard_map(
            local_heads if fits else local_any,
            mesh=mesh,
            in_specs=(
                P("parts", "frame"),
                P("frame", None),
                P(),
                P("step"),
                P("step"),
                P(),
                P(),
                P(),
                P(),
                P("step", None, "head"),
                P("step", "head"),
                P(),
            ),
            out_specs=(P("step", "parts", "frame"), P("parts")),
            check_vma=False,
        )(*args)

    return call
```

```python
import functools
import math

import jax
import jax.numpy as jnp
from jax import lax
from jax.experimental import pallas as pl
from jax.experimental.pallas import tpu as pltpu
from jax.sharding import PartitionSpec as P

HDIM = 72
ITERS = 4


def entering(value, axis, combine, identity):
    count, here = (lax.axis_size(axis), lax.axis_index(axis))
    everything = lax.all_gather(value, axis)
    start = jnp.broadcast_to(jnp.asarray(identity, value.dtype), value.shape)

    def hop(k, before):
        reached = k < here
        new = combine(before, everything[k])
        return jnp.where(reached, new, before)

    return lax.fori_loop(0, count, hop, start)


def add_terms(first, second):
    return first + second


def local_any(
    start_noise,
    position,
    time_table,
    time_index,
    sched_index,
    coef_keep,
    coef_noise,
    w_in,
    norm_gain,
    w_qkv,
    w_proj,
    w_final,
):
    w_qkv_all, w_proj_all = (
        lax.all_gather(w_qkv, "step", axis=0, tiled=True),
        lax.all_gather(w_proj, "step", axis=0, tiled=True),
    )
    batch_steps = time_index.shape[0]
    row_count = start_noise.shape[1]
    table_rows = time_table.shape[0]
    pick_time = (time_index[:, None] == jnp.arange(table_rows)[None, :]).astype(jnp.bfloat16)
    time_embed = jnp.dot(pick_time, time_table, preferred_element_type=jnp.float32)
    pick_sched = (sched_index[:, None] == jnp.arange(table_rows)[None, :]).astype(jnp.float32)
    keep_rate = jnp.sum(pick_sched * coef_keep[None, :], axis=1)
    noise_rate = jnp.sum(pick_sched * coef_noise[None, :], axis=1)
    heads_local = w_qkv_all.shape[2] // HDIM
    cell_count = (
        batch_steps
        * lax.axis_size("step")
        * start_noise.shape[0]
        * row_count
        * lax.axis_size("frame")
    )
    states = start_noise[None]
    drift_term = jnp.zeros_like(states)
    residual_list = []
    for iteration in range(ITERS):
        latent_bf = states.astype(jnp.bfloat16)
        hidden = (
            jnp.einsum("bcr,cd->brd", latent_bf, w_in, preferred_element_type=jnp.float32)
            + position
            + time_embed[:, None, :]
        )
        normed = (
            hidden * lax.rsqrt(jnp.mean(hidden * hidden, axis=2, keepdims=True) + 1e-06) * norm_gain
        ).astype(jnp.bfloat16)
        projected = jnp.einsum(
            "brd,dkq->brkq", normed, w_qkv_all, preferred_element_type=jnp.float32
        ).astype(jnp.bfloat16)
        queries = projected[:, :, 0].reshape(batch_steps, row_count, heads_local, HDIM)
        score_scale = 1.0 / math.sqrt(HDIM)
        keys_values = projected[:, :, 1:3]
        piece = lax.all_gather(keys_values, "frame", axis=1, tiled=True)
        top_old = jnp.full((batch_steps, heads_local, row_count), -1e30, jnp.float32)
        piece_rows = piece.shape[1]
        keys_blk = piece[:, :, 0].reshape(batch_steps, piece_rows, heads_local, HDIM)
        values_blk = piece[:, :, 1].reshape(batch_steps, piece_rows, heads_local, HDIM)
        scores = (
            jnp.einsum("bqhe,bkhe->bhqk", queries, keys_blk, preferred_element_type=jnp.float32)
            * score_scale
        )
        top_new = jnp.maximum(top_old, jnp.max(scores, axis=3))
        weights_exp = jnp.exp(scores - top_new[:, :, :, None])
        total_new = jnp.sum(weights_exp, axis=3)
        update = jnp.einsum(
            "bhqk,bkhe->bqhe",
            weights_exp.astype(jnp.bfloat16),
            values_blk,
            preferred_element_type=jnp.float32,
        )
        accum = update
        top_final, total_final, accum = (top_new, total_new, accum)
        attended = accum / jnp.transpose(total_final, (0, 2, 1))[:, :, :, None]
        attn_mixed = attended.reshape(batch_steps, row_count, heads_local * HDIM).astype(
            jnp.bfloat16
        )
        partial_value = jnp.einsum(
            "brq,dq->brd", attn_mixed, w_proj_all, preferred_element_type=jnp.float32
        )
        head_total = lax.psum(partial_value, "head")
        joined = (hidden + head_total).astype(jnp.bfloat16)
        predicted = jnp.einsum("cd,brd->bcr", w_final, joined, preferred_element_type=jnp.float32)
        drift_term = keep_rate[:, None, None] * states + noise_rate[:, None, None] * predicted
        local_incl = jnp.cumsum(drift_term, axis=0)
        local_total = local_incl[-1]
        earlier = entering(local_total, "step", add_terms, jnp.zeros_like(local_total))
        before = earlier[None] + (local_incl - drift_term)
        new_states = start_noise[None] + before
        change = new_states - states
        square_sum = jnp.sum(change * change)
        summed = lax.psum(square_sum, ("step", "frame"))
        residual_list.append(jnp.sqrt(summed / cell_count + 1e-06))
        states = new_states
    residual_norms = jnp.stack(residual_list)
    trajectory = states + drift_term
    return (trajectory, residual_norms)


MESH = pl.DeviceIdType.MESH
F32 = jnp.float32
BF16 = jnp.bfloat16


def dot(a, b, ca=1, cb=0):
    return lax.dot_general(a, b, (((ca,), (cb,)), ((), ())), preferred_element_type=F32)


def dot_exact(a, b):
    return lax.dot_general(
        a, b, (((1,), (0,)), ((), ())), precision=lax.Precision.HIGHEST, preferred_element_type=F32
    )


def two(a):
    high = a.astype(BF16)
    return high, (a - high.astype(F32)).astype(BF16)


def evals_of(steps):
    return [(i, j) for j in range(steps - 1) for i in range(min(j, ITERS - 1) + 1)] + [
        (min(ITERS, steps) - 1, steps - 1)
    ]


def kernel(
    S,
    F,
    H,
    noise_hbm,
    pos_hbm,
    table_hbm,
    tidx_ref,
    sidx_ref,
    keep_hbm,
    coef_hbm,
    win_hbm,
    gain_hbm,
    wqkv_hbm,
    wproj_hbm,
    wfin_hbm,
    traj_ref,
    res_ref,
    pos_ref,
    table_ref,
    keep_ref,
    coef_ref,
    win_ref,
    gain_ref,
    wqkv_ref,
    wproj_ref,
    wfin_ref,
    wt_ref,
    at_ref,
    at_peer,
    side_ref,
    side_cut,
    pv_ref,
    own_ref,
    near_send,
    near_recv,
    far_send,
    far_recv,
    mix_buf,
    noise_buf,
    meta_buf,
    ends_buf,
    tab_buf,
    base_buf,
    plane_buf,
    ssem,
    rsem,
):
    s, f, h = (lax.axis_index(a) for a in ("step", "frame", "head"))
    loads = [
        pltpu.make_async_copy(src, dst, ssem.at[ssem.shape[0] - 1 - n])
        for n, (src, dst) in enumerate(
            (
                (keep_hbm, keep_ref),
                (coef_hbm, coef_ref),
                (gain_hbm, gain_ref),
                (pos_hbm, pos_ref),
                (wqkv_hbm, wqkv_ref),
                (wfin_hbm, wfin_ref),
                (wproj_hbm, wproj_ref),
                (noise_hbm, noise_buf.at[f]),
                (table_hbm, table_ref),
                (win_hbm, win_ref),
            )
        )
    ]
    for copy in loads:
        copy.start()
    PL = F * H
    q_me = f * H + h
    C, rows = noise_buf.shape[1:]
    D = pos_ref.shape[1]
    N = rows * F
    R = wqkv_ref.shape[1]
    lanes = table_ref.shape[0]
    e = lax.rem(s, 2)
    e_near = 1 - e
    s_near = s + 1 - 2 * e
    s_far = lax.rem(s + 2, S)
    HZ = wqkv_ref.shape[2] // (F * 2 * HDIM)
    B = HZ * HDIM
    QK = 2 * B
    V = HZ * C

    def step_peer(d):
        return {"step": lax.rem(s + d, S)}

    def group_peer(d):
        t = lax.rem(q_me + lax.rem(d, PL), PL)
        z = s_near if d >= PL else s
        return {"step": z, "frame": t // H, "head": lax.rem(t, H)}

    frame_peer = {"frame": 1 - f}

    barrier = pltpu.get_barrier_semaphore()
    for d in range(1, PL):
        pl.semaphore_signal(barrier, inc=1, device_id=group_peer(d), device_id_type=MESH)
    for d in range(1, S):
        pl.semaphore_signal(barrier, inc=1, device_id=step_peer(d), device_id_type=MESH)

    count = [0]
    started = []

    def send(src, dst, peer):
        k = count[0]
        count[0] += 1
        copy = pltpu.make_async_remote_copy(
            src_ref=src,
            dst_ref=dst,
            send_sem=ssem.at[k],
            recv_sem=rsem.at[k],
            device_id=peer,
            device_id_type=MESH,
        )
        copy.start()
        started.append(copy)
        return copy

    for copy in loads[:3]:
        copy.wait()
    row_id = lax.broadcasted_iota(jnp.int32, (8, lanes), 0)
    lane_id = lax.broadcasted_iota(jnp.int32, (1, lanes), 1)
    hot_t = jnp.where(lane_id == tidx_ref[0], 1.0, 0.0)
    hot_s = lane_id == sidx_ref[0]
    keep = jnp.sum(jnp.where(hot_s, keep_ref[...], 0.0), axis=1, keepdims=True)
    coef = jnp.sum(jnp.where(hot_s, coef_ref[...], 0.0), axis=1, keepdims=True)
    meta_buf[s] = jnp.where(row_id == 0, hot_t, jnp.where(row_id == 1, keep, coef))
    for copy in loads[3:5]:
        copy.wait()
    gain = gain_ref[...].reshape(1, D)
    pos = pos_ref[...]
    at_ref[...] = jnp.transpose(pos.astype(F32) * gain).astype(BF16)
    for i in range(F):

        @pl.when(f == i)
        def _():
            for p in range(3):
                turned = jnp.transpose(wqkv_ref[p, :, i * 2 * B : (i + 1) * 2 * B])
                for t in range(2):
                    wt_ref[t, p * B : (p + 1) * B] = turned[t * B : (t + 1) * B]

    mine = pl.ds(pl.multiple_of(s * R, R), R)
    at_mine = at_ref[mine]
    near_send[0] = dot(wt_ref[e_near, 0:QK], at_mine).astype(BF16)
    pl.semaphore_wait(barrier, S - 1 + PL - 1)
    to_near, to_far = {"step": s_near}, {"step": s_far}
    near, far = {}, {}

    def send_near(i, low, high):
        window = pl.ds(low, high - low)
        near[i, low] = send(near_send.at[i, window], near_recv.at[i, window], to_near)

    pieces = [(low, low + QK // 3) for low in range(0, QK, QK // 3)]
    order = sorted(range(1, S), key=lambda d: abs(d - S / 2))
    early = [send(meta_buf.at[s], meta_buf.at[s], step_peer(d)) for d in order]
    send_near(0, *pieces[0])
    turn = send(at_ref.at[mine], at_peer, frame_peer)
    for piece in pieces[1:]:
        send_near(0, *piece)
    for copy in loads[5:7]:
        copy.wait()
    rows_of = wfin_ref[:, 0:R].astype(F32)
    for j in range(1, S):
        rows_of = jnp.where(s == j, wfin_ref[:, j * R : (j + 1) * R].astype(F32), rows_of)
    folded = dot(rows_of.astype(BF16), wproj_ref[...])
    picked = folded[:, 0 : 2 * B]
    for i in range(1, F):
        picked = jnp.where(f == i, folded[:, i * 2 * B : (i + 1) * 2 * B], picked)
    mix_buf[s] = picked.astype(BF16)
    early += [send(mix_buf.at[s], mix_buf.at[s], step_peer(d)) for d in order]
    loads[7].wait()
    sides = [send(noise_buf.at[f], noise_buf.at[f], frame_peer)]
    own_ref[0] = dot(wt_ref[e, 0:QK], at_mine)

    def pass_on(i, low, high):
        near[i, low].wait_recv()
        total = own_ref[i, low:high] + near_recv[i, low:high].astype(F32)
        far_send[i, low:high] = total.astype(BF16)
        window = pl.ds(low, high - low)
        far[i, low] = send(far_send.at[i, window], far_recv.at[i, window], to_far)

    for piece in pieces:
        pass_on(0, *piece)
    pv_ref[0, :, 0:rows] = dot(wt_ref[e, QK : QK + B], at_mine).astype(BF16)
    pv_ref[1, :, 0:rows] = dot(wt_ref[e_near, QK : QK + B], at_mine).astype(BF16)
    for copy in loads[8:]:
        copy.wait()
    w_in = win_ref[...]
    ends = jnp.concatenate([w_in, wfin_ref[...]], axis=0)
    ends_in = dot(ends, w_in, 1, 1)
    posf = pos.astype(F32)
    sq_hi, sq_lo = two(posf * posf)
    ones = jnp.ones((8, D), BF16)
    ends_buf[f, 0 : 2 * C] = dot(ends, pos, 1, 1)
    ends_buf[f, 2 * C : 2 * C + 8] = dot(ones, sq_hi, 1, 1) + dot(ones, sq_lo, 1, 1)

    turn.wait_recv()
    at_other = at_peer[...]
    near_send[1] = dot(wt_ref[e_near, 0:QK], at_other).astype(BF16)
    for piece in pieces:
        send_near(1, *piece)
    own_ref[1] = dot(wt_ref[e, 0:QK], at_other)
    pv_ref[0, :, rows : 2 * rows] = dot(wt_ref[e, QK : QK + B], at_other).astype(BF16)
    pv_ref[1, :, rows : 2 * rows] = dot(wt_ref[e_near, QK : QK + B], at_other).astype(BF16)

    side_ref[0:C] = w_in.astype(F32)
    for copy in early:
        copy.wait_recv()
    metas = [meta_buf[j] for j in range(S)]
    hot = jnp.concatenate(
        [m[0:1] for m in metas] + [jnp.zeros((8 - S, lanes), F32)], axis=0
    ).astype(BF16)
    keeps = [jnp.concatenate([m[1:2, :rows]] * F, axis=1) for m in metas]
    coefs = [jnp.concatenate([m[2:3, :rows]] * F, axis=1) for m in metas]
    temb = dot(hot, table_ref[...])
    side_ref[C : C + 8] = temb
    side_ref[C + 8 :] = jnp.zeros((32 - C - 8, D), F32)
    for j in range(S):

        @pl.when(s == j)
        def _():
            cut = slice(j * R, (j + 1) * R)
            side_cut[...] = (side_ref[:, cut] * gain[:, cut]).astype(BF16)

    side_mine = side_cut[...]
    mix = mix_buf[0].astype(F32)
    for j in range(1, S):
        mix = mix + mix_buf[j].astype(F32)
    mix_lane = lax.broadcasted_iota(jnp.int32, (V, B), 1) // HDIM
    mix_row = lax.broadcasted_iota(jnp.int32, (V, B), 0) // C

    def late_rows(role, member):
        turned = dot(wt_ref[member], side_mine, 1, 1)
        pv_ref[role, :, 2 * rows : 2 * rows + 32] = turned[QK:].astype(BF16)
        part = jnp.where(member == 0, mix[:, 0:B], mix[:, B : 2 * B])
        block = jnp.where(
            mix_lane == mix_row, jnp.concatenate([part] * HZ, axis=0), 0.0
        )
        block_hi, block_lo = two(block)
        values = dot(jnp.concatenate([block_hi, block_lo], axis=0), pv_ref[role])
        values = values[0:V] + values[V : 2 * V]
        packs = []
        for arr in (turned[0:QK], values[:, 2 * rows : 2 * rows + 32]):
            size = arr.shape[0] // 4
            packs.append(
                jnp.concatenate([arr[g * size : (g + 1) * size] for g in range(4)], axis=1)
            )
        return jnp.concatenate(
            [values[:, 0:rows], values[:, rows : 2 * rows]] + packs, axis=0
        )

    LATE = 2 * V + (QK + V) // 4
    near_send[2, 0:LATE] = late_rows(1, e_near).astype(BF16)
    send_near(2, 0, LATE)
    own_ref[2, 0:LATE] = late_rows(0, e)
    temb_b = temb.astype(BF16)
    ends_buf[f, 2 * C + 8 : 2 * C + 16] = dot(temb_b, pos, 1, 1)
    sides.append(send(ends_buf.at[f], ends_buf.at[f], frame_peer))
    ends_t = dot(ends, temb_b, 1, 1)
    norm_t = jnp.sum(temb * temb, axis=1, keepdims=True)
    for piece in pieces:
        pass_on(1, *piece)
    pass_on(2, 0, LATE)

    scale = 1.4426950408889634 / math.sqrt(HDIM)
    qk_row = lax.broadcasted_iota(jnp.int32, (QK, 1), 0)
    row_scale = jnp.where(qk_row < B, scale, 1.0)

    def whole(i, low, high):
        return far_send[i, low:high].astype(F32) + far_recv[i, low:high].astype(F32)

    for low, _ in pieces:
        far[0, low].wait_recv()
    tab_buf[f, 0:QK] = whole(0, 0, QK) * row_scale
    for copy in sides:
        copy.wait_recv()
    start = jnp.concatenate([noise_buf[i] for i in range(F)], axis=1)
    ends_all = jnp.concatenate([ends_buf[i] for i in range(F)], axis=1)
    ends_pos = ends_all[0 : 2 * C]
    norm_p = ends_all[2 * C : 2 * C + 1]
    cross = ends_all[2 * C + 8 : 2 * C + 16]
    norms = [norm_p + 2.0 * cross[j : j + 1] + norm_t[j : j + 1] for j in range(S)]
    for j in range(S):
        base_buf[j] = jnp.concatenate(
            [
                2.0 * (ends_pos[0:C] + ends_t[0:C, j : j + 1]),
                ends_pos[C : 2 * C] + ends_t[C : 2 * C, j : j + 1],
            ],
            axis=0,
        )
    for low, _ in pieces:
        far[1, low].wait_recv()
    tab_buf[1 - f, 0:QK] = whole(1, 0, QK) * row_scale
    far[2, 0].wait_recv()
    last = whole(2, 0, LATE)
    tab_buf[f, QK : QK + V] = last[0:V]
    tab_buf[1 - f, QK : QK + V] = last[V : 2 * V]
    packed = last[2 * V : LATE]
    size = QK // 4
    big_qk = jnp.concatenate([packed[0:size, 32 * g : 32 * g + 32] for g in range(4)], axis=0)
    big_v = jnp.concatenate([packed[size:, 32 * g : 32 * g + 32] for g in range(4)], axis=0)
    ends_hi, ends_lo = two(
        jnp.concatenate([ends_in, jnp.zeros((2 * C, 32 - C), F32)], axis=1)
    )
    big = jnp.concatenate(
        [ends_hi, ends_lo, (big_qk * row_scale).astype(BF16), big_v.astype(BF16)], axis=0
    )
    tab = jnp.concatenate([tab_buf[i] for i in range(F)], axis=1)
    hot_row = lax.broadcasted_iota(jnp.int32, (32 - C, N), 0)

    def partial(x, j):
        xb = x.astype(BF16)
        pick = jnp.where(hot_row == j, 1.0, 0.0).astype(BF16)
        lin = dot(big, jnp.concatenate([xb, pick], axis=0))
        tail = lin[0 : 2 * C] + lin[2 * C : 4 * C]
        base = base_buf[j]
        square = jnp.sum(xb.astype(F32) * (tail[0:C] + base[0:C]), axis=0, keepdims=True)
        square = jnp.maximum(square + norms[j], 0.0)
        r = lax.rsqrt(square * (1.0 / D) + 1e-06)
        lin = (lin[4 * C :] + tab) * r
        out = jnp.zeros((C, N), F32)
        for n in range(HZ):
            q = lin[n * HDIM : (n + 1) * HDIM].astype(BF16)
            k = lin[B + n * HDIM : B + (n + 1) * HDIM].astype(BF16)
            v_hi, v_lo = two(lin[QK + n * C : QK + (n + 1) * C])
            scores = dot(k, q, 0, 0)
            p = jnp.exp2(scores - jnp.max(scores, axis=0, keepdims=True)).astype(BF16)
            o = dot(jnp.concatenate([v_hi, v_lo, jnp.ones((C, N), BF16)], axis=0), p)
            out = out + (o[0:C] + o[C : 2 * C]) / o[2 * C : 2 * C + 1]
        return out, tail[C : 2 * C] + base[C : 2 * C]

    keys = evals_of(S)
    state, local_eps, drift, flying = {}, {}, {}, {}

    def launch(key):
        i, j = key
        n = keys.index(key)
        x = start
        for m in range(j if i else 0):
            x = x + drift[(min(i - 1, m), m)]
        state[key] = x
        part, local_eps[key] = partial(x, j)
        own = e * PL + q_me
        plane_buf[n, own] = part.astype(BF16)
        slot = plane_buf.at[n, own]
        k = count[0]
        count[0] += 1
        for d in range(1, 2 * PL):
            pltpu.make_async_remote_copy(
                src_ref=slot,
                dst_ref=slot,
                send_sem=ssem.at[k],
                recv_sem=rsem.at[k],
                device_id=group_peer(d),
                device_id_type=MESH,
            ).start()
        flying[key] = k

    def settle(n, sem):
        others = plane_buf.at[n, pl.ds(0, 2 * PL - 1)]
        pltpu.make_async_copy(others, others, sem).wait()

    def land(key):
        n, j, k = keys.index(key), key[1], flying[key]
        settle(n, rsem.at[k])
        total = local_eps[key]
        for i in range(2 * PL):
            total = total + plane_buf[n, i].astype(F32)
        drift[key] = keeps[j] * state[key] + coefs[j] * total
        settle(n, ssem.at[k])

    for act, key in PLAN[:-1]:
        if act == "land" and started:
            for copy in started:
                copy.wait_send()
            started.clear()
        {"launch": launch, "land": land}[act](key)

    old = [start] * S
    norms_out = []
    for it in range(ITERS):
        new, run = [], start
        for j in range(S):
            new.append(run)
            if j < S - 1:
                run = run + drift[(min(it, j), j)]
        square = jnp.zeros((1, 1), F32)
        for j in range(S):
            change = new[j] - old[j]
            square = square + jnp.sum(
                jnp.sum(change * change, axis=0, keepdims=True), axis=1, keepdims=True
            )
        norms_out.append(jnp.sqrt(square / (S * C * N) + 1e-06))
        old = new
    lane = lax.broadcasted_iota(jnp.int32, res_ref.shape, 1)
    res = jnp.zeros(res_ref.shape, F32)
    for it in range(ITERS):
        res = jnp.where(lane == it, norms_out[it], res)
    res_ref[...] = res
    land(PLAN[-1][1])
    final = jnp.zeros((C, N), F32)
    for j in range(S):
        final = jnp.where(s == j, old[j] + drift[(min(ITERS - 1, j), j)], final)
    half = final[:, 0:rows]
    for i in range(1, F):
        half = jnp.where(f == i, final[:, i * rows : (i + 1) * rows], half)
    traj_ref[0] = half


PLAN = (
    ("launch", (0, 0)),
    ("launch", (0, 1)),
    ("launch", (0, 2)),
    ("land", (0, 0)),
    ("launch", (1, 1)),
    ("land", (0, 1)),
    ("launch", (1, 2)),
    ("land", (1, 1)),
    ("launch", (2, 2)),
    ("land", (0, 2)),
    ("land", (1, 2)),
    ("land", (2, 2)),
    ("launch", (3, 3)),
    ("land", (3, 3)),
)


def local_heads(
    start_noise,
    position,
    time_table,
    time_index,
    sched_index,
    coef_keep,
    coef_noise,
    w_in,
    norm_gain,
    w_qkv,
    w_proj,
    w_final,
):
    S, F, H = (lax.axis_size(a) for a in ("step", "frame", "head"))
    R = w_qkv.shape[0]
    C, rows = start_noise.shape
    D = position.shape[1]
    N = rows * F
    PL = F * H
    HZ = w_qkv.shape[2] // (F * 2 * HDIM)
    B = HZ * HDIM
    QK = 2 * B
    V = HZ * C
    n_evals = len(evals_of(S))
    n_sems = 2 * (S - 1) + 3 + 2 * 7 + n_evals
    vmem = pl.BlockSpec(memory_space=pltpu.VMEM)
    smem = pl.BlockSpec(memory_space=pltpu.SMEM)
    here = pl.BlockSpec(memory_space=pl.ANY)
    traj, res = pl.pallas_call(
        functools.partial(kernel, S, F, H),
        out_shape=(pltpu.VMEM((1, C, rows), F32), pltpu.VMEM((1, ITERS), F32)),
        in_specs=[here, here, here, smem, smem] + [here] * 7,
        out_specs=(vmem, vmem),
        scratch_shapes=[
            pltpu.VMEM((rows, D), BF16),
            pltpu.VMEM(time_table.shape, BF16),
            pltpu.VMEM((1, coef_keep.shape[0]), F32),
            pltpu.VMEM((1, coef_noise.shape[0]), F32),
            pltpu.VMEM(w_in.shape, BF16),
            pltpu.VMEM((D,), F32),
            pltpu.VMEM((3, R, w_qkv.shape[2]), BF16),
            pltpu.VMEM(w_proj.shape, BF16),
            pltpu.VMEM(w_final.shape, BF16),
            pltpu.VMEM((2, QK + B, R), BF16),
            pltpu.VMEM((D, rows), BF16),
            pltpu.VMEM((R, rows), BF16),
            pltpu.VMEM((32, D), F32),
            pltpu.VMEM((32, R), BF16),
            pltpu.VMEM((2, B, N + 32), BF16),
            pltpu.VMEM((3, QK, rows), F32),
            pltpu.VMEM((3, QK, rows), BF16),
            pltpu.VMEM((3, QK, rows), BF16),
            pltpu.VMEM((3, QK, rows), BF16),
            pltpu.VMEM((3, QK, rows), BF16),
            pltpu.VMEM((S, C, 2 * B), BF16),
            pltpu.VMEM((F, C, rows), F32),
            pltpu.VMEM((S, 8, time_table.shape[0]), F32),
            pltpu.VMEM((F, 2 * C + 16, rows), F32),
            pltpu.VMEM((F, QK + V, rows), F32),
            pltpu.VMEM((S, 2 * C, N), F32),
            pltpu.VMEM((n_evals, 2 * PL, C, N), BF16),
            pltpu.SemaphoreType.DMA((n_sems + 10,)),
            pltpu.SemaphoreType.DMA((n_sems,)),
        ],
        compiler_params=pltpu.CompilerParams(
            collective_id=0, has_side_effects=True, vmem_limit_bytes=60 * 1024 * 1024
        ),
    )(
        start_noise,
        position,
        time_table,
        time_index,
        sched_index,
        coef_keep[None],
        coef_noise[None],
        w_in,
        norm_gain,
        jnp.transpose(w_qkv, (1, 0, 2)),
        w_proj,
        w_final,
    )
    return traj, res.reshape(ITERS)


def one_head_each(mesh, start_noise, time_index, w_qkv, time_table):
    S, F, H = (mesh.shape[a] for a in ("step", "frame", "head"))
    return (
        S == ITERS
        and time_index.shape[0] == S
        and w_qkv.shape[2] == S * F * H * HDIM
        and w_qkv.shape[0] % (16 * S) == 0
        and start_noise.shape[1] % (128 * F) == 0
        and start_noise.shape[1] // F <= time_table.shape[0]
        and time_table.shape[0] % 128 == 0
    )


def solution(mesh):
    def call(*args):
        fits = one_head_each(mesh, args[0], args[3], args[9], args[2])
        return jax.shard_map(
            local_heads if fits else local_any,
            mesh=mesh,
            in_specs=(
                P("parts", "frame"),
                P("frame", None),
                P(),
                P("step"),
                P("step"),
                P(),
                P(),
                P(),
                P(),
                P("step", None, "head"),
                P("step", "head"),
                P(),
            ),
            out_specs=(P("step", "parts", "frame"), P("parts")),
            check_vma=False,
        )(*args)

    return call
```

```python
import functools
import math

import jax
import jax.numpy as jnp
from jax import lax
from jax.experimental import pallas as pl
from jax.experimental.pallas import tpu as pltpu
from jax.sharding import PartitionSpec as P

HDIM = 72
ITERS = 4


def entering(value, axis, combine, identity):
    count, here = (lax.axis_size(axis), lax.axis_index(axis))
    everything = lax.all_gather(value, axis)
    start = jnp.broadcast_to(jnp.asarray(identity, value.dtype), value.shape)

    def hop(k, before):
        reached = k < here
        new = combine(before, everything[k])
        return jnp.where(reached, new, before)

    return lax.fori_loop(0, count, hop, start)


def add_terms(first, second):
    return first + second


def local_any(
    start_noise,
    position,
    time_table,
    time_index,
    sched_index,
    coef_keep,
    coef_noise,
    w_in,
    norm_gain,
    w_qkv,
    w_proj,
    w_final,
):
    w_qkv_all, w_proj_all = (
        lax.all_gather(w_qkv, "step", axis=0, tiled=True),
        lax.all_gather(w_proj, "step", axis=0, tiled=True),
    )
    batch_steps = time_index.shape[0]
    row_count = start_noise.shape[1]
    table_rows = time_table.shape[0]
    pick_time = (time_index[:, None] == jnp.arange(table_rows)[None, :]).astype(jnp.bfloat16)
    time_embed = jnp.dot(pick_time, time_table, preferred_element_type=jnp.float32)
    pick_sched = (sched_index[:, None] == jnp.arange(table_rows)[None, :]).astype(jnp.float32)
    keep_rate = jnp.sum(pick_sched * coef_keep[None, :], axis=1)
    noise_rate = jnp.sum(pick_sched * coef_noise[None, :], axis=1)
    heads_local = w_qkv_all.shape[2] // HDIM
    cell_count = (
        batch_steps
        * lax.axis_size("step")
        * start_noise.shape[0]
        * row_count
        * lax.axis_size("frame")
    )
    states = start_noise[None]
    drift_term = jnp.zeros_like(states)
    residual_list = []
    for iteration in range(ITERS):
        latent_bf = states.astype(jnp.bfloat16)
        hidden = (
            jnp.einsum("bcr,cd->brd", latent_bf, w_in, preferred_element_type=jnp.float32)
            + position
            + time_embed[:, None, :]
        )
        normed = (
            hidden * lax.rsqrt(jnp.mean(hidden * hidden, axis=2, keepdims=True) + 1e-06) * norm_gain
        ).astype(jnp.bfloat16)
        projected = jnp.einsum(
            "brd,dkq->brkq", normed, w_qkv_all, preferred_element_type=jnp.float32
        ).astype(jnp.bfloat16)
        queries = projected[:, :, 0].reshape(batch_steps, row_count, heads_local, HDIM)
        score_scale = 1.0 / math.sqrt(HDIM)
        keys_values = projected[:, :, 1:3]
        piece = lax.all_gather(keys_values, "frame", axis=1, tiled=True)
        top_old = jnp.full((batch_steps, heads_local, row_count), -1e30, jnp.float32)
        piece_rows = piece.shape[1]
        keys_blk = piece[:, :, 0].reshape(batch_steps, piece_rows, heads_local, HDIM)
        values_blk = piece[:, :, 1].reshape(batch_steps, piece_rows, heads_local, HDIM)
        scores = (
            jnp.einsum("bqhe,bkhe->bhqk", queries, keys_blk, preferred_element_type=jnp.float32)
            * score_scale
        )
        top_new = jnp.maximum(top_old, jnp.max(scores, axis=3))
        weights_exp = jnp.exp(scores - top_new[:, :, :, None])
        total_new = jnp.sum(weights_exp, axis=3)
        update = jnp.einsum(
            "bhqk,bkhe->bqhe",
            weights_exp.astype(jnp.bfloat16),
            values_blk,
            preferred_element_type=jnp.float32,
        )
        accum = update
        top_final, total_final, accum = (top_new, total_new, accum)
        attended = accum / jnp.transpose(total_final, (0, 2, 1))[:, :, :, None]
        attn_mixed = attended.reshape(batch_steps, row_count, heads_local * HDIM).astype(
            jnp.bfloat16
        )
        partial_value = jnp.einsum(
            "brq,dq->brd", attn_mixed, w_proj_all, preferred_element_type=jnp.float32
        )
        head_total = lax.psum(partial_value, "head")
        joined = (hidden + head_total).astype(jnp.bfloat16)
        predicted = jnp.einsum("cd,brd->bcr", w_final, joined, preferred_element_type=jnp.float32)
        drift_term = keep_rate[:, None, None] * states + noise_rate[:, None, None] * predicted
        local_incl = jnp.cumsum(drift_term, axis=0)
        local_total = local_incl[-1]
        earlier = entering(local_total, "step", add_terms, jnp.zeros_like(local_total))
        before = earlier[None] + (local_incl - drift_term)
        new_states = start_noise[None] + before
        change = new_states - states
        square_sum = jnp.sum(change * change)
        summed = lax.psum(square_sum, ("step", "frame"))
        residual_list.append(jnp.sqrt(summed / cell_count + 1e-06))
        states = new_states
    residual_norms = jnp.stack(residual_list)
    trajectory = states + drift_term
    return (trajectory, residual_norms)


MESH = pl.DeviceIdType.MESH
F32 = jnp.float32
BF16 = jnp.bfloat16


def dot(a, b, ca=1, cb=0):
    return lax.dot_general(a, b, (((ca,), (cb,)), ((), ())), preferred_element_type=F32)


def dot_exact(a, b):
    return lax.dot_general(
        a, b, (((1,), (0,)), ((), ())), precision=lax.Precision.HIGHEST, preferred_element_type=F32
    )


def two(a):
    high = a.astype(BF16)
    return high, (a - high.astype(F32)).astype(BF16)


def kernel(
    S,
    F,
    H,
    noise_hbm,
    pos_hbm,
    table_hbm,
    tidx_ref,
    sidx_ref,
    keep_hbm,
    coef_hbm,
    win_hbm,
    gain_hbm,
    wqkv_hbm,
    wproj_hbm,
    wfin_hbm,
    traj_ref,
    res_ref,
    pos_ref,
    table_ref,
    keep_ref,
    coef_ref,
    win_ref,
    gain_ref,
    wqkv_ref,
    wproj_ref,
    wfin_ref,
    wt_ref,
    at_ref,
    at_peer,
    side_ref,
    side_cut,
    pv_ref,
    own_ref,
    near_send,
    near_recv,
    far_send,
    far_recv,
    mix_buf,
    noise_buf,
    meta_buf,
    ends_buf,
    fin_qk,
    fin_late,
    big_buf,
    tab_buf,
    base_buf,
    plane_buf,
    chip_buf,
    ssem,
    rsem,
):
    s, f, h = (lax.axis_index(a) for a in ("step", "frame", "head"))
    loads = [
        pltpu.make_async_copy(src, dst, ssem.at[ssem.shape[0] - 1 - n])
        for n, (src, dst) in enumerate(
            (
                (keep_hbm, keep_ref),
                (coef_hbm, coef_ref),
                (gain_hbm, gain_ref),
                (pos_hbm, pos_ref),
                (wqkv_hbm, wqkv_ref),
                (wfin_hbm, wfin_ref),
                (wproj_hbm, wproj_ref),
                (noise_hbm, noise_buf.at[f]),
                (table_hbm, table_ref),
                (win_hbm, win_ref),
            )
        )
    ]
    for copy in loads:
        copy.start()
    PL = F * H
    q_me = f * H + h
    C, rows = noise_buf.shape[1:]
    D = pos_ref.shape[1]
    N = rows * F
    R = wqkv_ref.shape[1]
    lanes = table_ref.shape[0]
    e = lax.rem(s, 2)
    e_near = 1 - e
    s_near = s + 1 - 2 * e
    s_far = lax.rem(s + 2, S)
    HZ = wqkv_ref.shape[2] // (F * 2 * HDIM)
    B = HZ * HDIM
    QK = 2 * B
    V = HZ * C

    def step_peer(d):
        return {"step": lax.rem(s + d, S)}

    def group_peer(d):
        dz, df, dh = d // PL, d % PL // H, d % H
        return {
            "step": s_near if dz else s,
            "frame": lax.rem(f + df, F),
            "head": lax.rem(h + dh, H),
        }

    frame_peer = {"frame": 1 - f}

    barrier = pltpu.get_barrier_semaphore()
    for d in range(1, PL):
        pl.semaphore_signal(barrier, inc=1, device_id=group_peer(d), device_id_type=MESH)
    for d in range(1, S):
        pl.semaphore_signal(barrier, inc=1, device_id=step_peer(d), device_id_type=MESH)

    count = [0]
    started = []

    def send(src, dst, peer):
        k = count[0]
        count[0] += 1
        copy = pltpu.make_async_remote_copy(
            src_ref=src,
            dst_ref=dst,
            send_sem=ssem.at[k],
            recv_sem=rsem.at[k],
            device_id=peer,
            device_id_type=MESH,
        )
        copy.start()
        started.append(copy)
        return copy

    for copy in loads[:3]:
        copy.wait()
    row_id = lax.broadcasted_iota(jnp.int32, (8, lanes), 0)
    lane_id = lax.broadcasted_iota(jnp.int32, (1, lanes), 1)
    hot_t = jnp.where(lane_id == tidx_ref[0], 1.0, 0.0)
    hot_s = lane_id == sidx_ref[0]
    keep = jnp.sum(jnp.where(hot_s, keep_ref[...], 0.0), axis=1, keepdims=True)
    coef = jnp.sum(jnp.where(hot_s, coef_ref[...], 0.0), axis=1, keepdims=True)
    meta_buf[s] = jnp.where(row_id == 0, hot_t, jnp.where(row_id == 1, keep, coef))
    for copy in loads[3:5]:
        copy.wait()
    gain = gain_ref[...].reshape(1, D)
    pos = pos_ref[...]
    at_ref[...] = jnp.transpose(pos.astype(F32) * gain).astype(BF16)

    def turn_weights(parts):
        for i in range(F):

            @pl.when(f == i)
            def _():
                for p in parts:
                    turned = jnp.transpose(wqkv_ref[p, :, i * 2 * B : (i + 1) * 2 * B])
                    for t in range(2):
                        wt_ref[t, p * B : (p + 1) * B] = turned[t * B : (t + 1) * B]

    turn_weights((0, 1))
    mine = pl.ds(pl.multiple_of(s * R, R), R)
    at_mine = at_ref[mine]
    near_send[0] = dot(wt_ref[e_near, 0:QK], at_mine).astype(BF16)
    pl.semaphore_wait(barrier, S - 1 + PL - 1)
    to_near, to_far = {"step": s_near}, {"step": s_far}
    near, far = {}, {}

    def send_near(i, low, high):
        window = pl.ds(low, high - low)
        near[i, low] = send(near_send.at[i, window], near_recv.at[i, window], to_near)

    pieces = [(low, low + QK // 3) for low in range(0, QK, QK // 3)]
    order = sorted(range(1, S), key=lambda d: abs(d - S / 2))
    early = [send(meta_buf.at[s], meta_buf.at[s], step_peer(d)) for d in order]
    send_near(0, *pieces[0])
    turn = send(at_ref.at[mine], at_peer, frame_peer)
    for piece in pieces[1:]:
        send_near(0, *piece)
    for copy in loads[5:7]:
        copy.wait()
    rows_of = wfin_ref[:, 0:R].astype(F32)
    for j in range(1, S):
        rows_of = jnp.where(s == j, wfin_ref[:, j * R : (j + 1) * R].astype(F32), rows_of)
    folded = dot(rows_of.astype(BF16), wproj_ref[...])
    picked = folded[:, 0 : 2 * B]
    for i in range(1, F):
        picked = jnp.where(f == i, folded[:, i * 2 * B : (i + 1) * 2 * B], picked)
    mix_buf[s] = picked.astype(BF16)
    early += [send(mix_buf.at[s], mix_buf.at[s], step_peer(d)) for d in order]
    loads[7].wait()
    sides = [send(noise_buf.at[f], noise_buf.at[f], frame_peer)]
    own_ref[0] = dot(wt_ref[e, 0:QK], at_mine)
    turn_weights((2,))

    def pass_on(i, low, high):
        near[i, low].wait_recv()
        total = own_ref[i, low:high] + near_recv[i, low:high].astype(F32)
        far_send[i, low:high] = total.astype(BF16)
        window = pl.ds(low, high - low)
        far[i, low] = send(far_send.at[i, window], far_recv.at[i, window], to_far)

    for piece in pieces:
        pass_on(0, *piece)
    pv_ref[0, :, 0:rows] = dot(wt_ref[e, QK : QK + B], at_mine).astype(BF16)
    pv_ref[1, :, 0:rows] = dot(wt_ref[e_near, QK : QK + B], at_mine).astype(BF16)
    for copy in loads[8:]:
        copy.wait()
    w_in = win_ref[...]
    ends = jnp.concatenate([w_in, wfin_ref[...]], axis=0)
    ends_in = dot(ends, w_in, 1, 1)
    posf = pos.astype(F32)
    sq_hi, sq_lo = two(posf * posf)
    ones = jnp.ones((8, D), BF16)
    ends_buf[f, 0 : 2 * C] = dot(ends, pos, 1, 1)
    ends_buf[f, 2 * C : 2 * C + 8] = dot(ones, sq_hi, 1, 1) + dot(ones, sq_lo, 1, 1)

    turn.wait_recv()
    at_other = at_peer[...]
    near_send[1] = dot(wt_ref[e_near, 0:QK], at_other).astype(BF16)
    for piece in pieces:
        send_near(1, *piece)
    own_ref[1] = dot(wt_ref[e, 0:QK], at_other)
    pv_ref[0, :, rows : 2 * rows] = dot(wt_ref[e, QK : QK + B], at_other).astype(BF16)
    pv_ref[1, :, rows : 2 * rows] = dot(wt_ref[e_near, QK : QK + B], at_other).astype(BF16)

    side_ref[0:C] = w_in.astype(F32)
    for copy in early:
        copy.wait_recv()
    metas = [meta_buf[j] for j in range(S)]
    hot = jnp.concatenate(
        [m[0:1] for m in metas] + [jnp.zeros((8 - S, lanes), F32)], axis=0
    ).astype(BF16)
    keeps = [jnp.concatenate([m[1:2, :rows]] * F, axis=1) for m in metas]
    coefs = [jnp.concatenate([m[2:3, :rows]] * F, axis=1) for m in metas]
    temb = dot(hot, table_ref[...])
    side_ref[C : C + 8] = temb
    side_ref[C + 8 :] = jnp.zeros((32 - C - 8, D), F32)
    for j in range(S):

        @pl.when(s == j)
        def _():
            cut = slice(j * R, (j + 1) * R)
            side_cut[...] = (side_ref[:, cut] * gain[:, cut]).astype(BF16)

    side_mine = side_cut[...]
    mix = mix_buf[0].astype(F32)
    for j in range(1, S):
        mix = mix + mix_buf[j].astype(F32)
    mix_lane = lax.broadcasted_iota(jnp.int32, (V, B), 1) // HDIM
    mix_row = lax.broadcasted_iota(jnp.int32, (V, B), 0) // C

    def late_rows(role, member):
        turned = dot(wt_ref[member], side_mine, 1, 1)
        pv_ref[role, :, 2 * rows : 2 * rows + 32] = turned[QK:].astype(BF16)
        part = jnp.where(member == 0, mix[:, 0:B], mix[:, B : 2 * B])
        block = jnp.where(
            mix_lane == mix_row, jnp.concatenate([part] * HZ, axis=0), 0.0
        )
        block_hi, block_lo = two(block)
        values = dot(jnp.concatenate([block_hi, block_lo], axis=0), pv_ref[role])
        values = values[0:V] + values[V : 2 * V]
        packs = []
        for arr in (turned[0:QK], values[:, 2 * rows : 2 * rows + 32]):
            size = arr.shape[0] // 4
            packs.append(
                jnp.concatenate([arr[g * size : (g + 1) * size] for g in range(4)], axis=1)
            )
        return jnp.concatenate(
            [values[:, 0:rows], values[:, rows : 2 * rows]] + packs, axis=0
        )

    LATE = 2 * V + (QK + V) // 4
    near_send[2, 0:LATE] = late_rows(1, e_near).astype(BF16)
    send_near(2, 0, LATE)
    own_ref[2, 0:LATE] = late_rows(0, e)
    temb_b = temb.astype(BF16)
    ends_buf[f, 2 * C + 8 : 2 * C + 16] = dot(temb_b, pos, 1, 1)
    sides.append(send(ends_buf.at[f], ends_buf.at[f], frame_peer))
    ends_t = dot(ends, temb_b, 1, 1)
    norm_t = jnp.sum(temb * temb, axis=1, keepdims=True)
    for piece in pieces:
        pass_on(1, *piece)

    scale = 1.4426950408889634 / math.sqrt(HDIM)
    qk_row = lax.broadcasted_iota(jnp.int32, (QK, 1), 0)
    row_scale = jnp.where(qk_row < B, scale, 1.0)
    set_own, set_near = 2 * f + e, 2 * f + e_near
    halves = (f, 1 - f)

    def whole(i, low, high):
        far[i, low].wait_recv()
        total = far_send[i, low:high].astype(F32) + far_recv[i, low:high].astype(F32)
        return total.astype(BF16)

    def finish(i, low, high):
        total = whole(i, low, high)
        window = pl.ds(low, high - low)
        if i < 2:
            fin_qk[set_own, halves[i], low:high] = total
            ref = fin_qk.at[set_own, halves[i], window]
            twin = fin_qk.at[set_near, halves[i], window]
        else:
            fin_late[set_own] = total
            ref = fin_late.at[set_own]
            twin = fin_late.at[set_near]
        return ref, twin

    across, shared, passed = [], [], []

    def cross_over(refs):
        across.append(send(refs[0], refs[0], frame_peer))

    def share(refs):
        shared.append((send(refs[0], refs[0], to_near), refs[1]))

    def forward(number):
        for _ in range(number):
            copy, twin = shared.pop(0)
            copy.wait_recv()
            passed.append(send(twin, twin, frame_peer))

    ready = [finish(0, *piece) for piece in pieces]
    pass_on(2, 0, LATE)
    for refs in ready:
        cross_over(refs)
        share(refs)
    for copy in sides:
        copy.wait_recv()
    start = jnp.concatenate([noise_buf[i] for i in range(F)], axis=1)
    ends_all = jnp.concatenate([ends_buf[i] for i in range(F)], axis=1)
    ends_pos = ends_all[0 : 2 * C]
    norm_p = ends_all[2 * C : 2 * C + 1]
    cross = ends_all[2 * C + 8 : 2 * C + 16]
    norms = [norm_p + 2.0 * cross[j : j + 1] + norm_t[j : j + 1] for j in range(S)]
    for j in range(S):
        base_buf[j] = jnp.concatenate(
            [
                2.0 * (ends_pos[0:C] + ends_t[0:C, j : j + 1]),
                ends_pos[C : 2 * C] + ends_t[C : 2 * C, j : j + 1],
            ],
            axis=0,
        )
    ends_hi, ends_lo = two(
        jnp.concatenate([ends_in, jnp.zeros((2 * C, 32 - C), F32)], axis=1)
    )
    ends_big = jnp.concatenate([ends_hi, ends_lo], axis=0)
    size = QK // 4

    def build(slot, group, frame):
        last = fin_late[group].astype(F32)
        one, other = last[0:V], last[V : 2 * V]
        packed = last[2 * V : LATE]
        big_qk = jnp.concatenate(
            [packed[0:size, 32 * g : 32 * g + 32] for g in range(4)], axis=0
        )
        big_v = jnp.concatenate(
            [packed[size:, 32 * g : 32 * g + 32] for g in range(4)], axis=0
        )
        big_buf[slot, 0:QK] = (big_qk * row_scale).astype(BF16)
        big_buf[slot, QK:] = big_v.astype(BF16)
        for i in range(F):
            cut = slice(i * rows, (i + 1) * rows)
            tab_buf[slot, 0:QK, cut] = fin_qk[group, i].astype(F32) * row_scale
            tab_buf[slot, QK:, cut] = jnp.where(frame == i, one, other)

    ready = [finish(1, *piece) for piece in pieces]
    for refs in ready:
        cross_over(refs)
        share(refs)
    ready = finish(2, 0, LATE)
    build(4, set_own, f)

    def share_rest(_):
        cross_over(ready)
        share(ready)

    hot_row = lax.broadcasted_iota(jnp.int32, (32 - C, N), 0)
    ones_rows = jnp.ones((C, N), BF16)

    def evaluate(x, j, slots):
        xb = x.astype(BF16)
        pick = jnp.where(hot_row == j, 1.0, 0.0).astype(BF16)
        x_in = jnp.concatenate([xb, pick], axis=0)
        base = base_buf[j]
        out = jnp.zeros((C, N), F32)
        items, scores, r, eps = {}, {}, None, None
        G = len(slots)
        for g in range(G + 2):
            if g < G:
                big = big_buf[slots[g]]
                if g == 0:
                    lin = dot(jnp.concatenate([ends_big, big], axis=0), x_in)
                    tail = lin[0 : 2 * C] + lin[2 * C : 4 * C]
                    lin = lin[4 * C :]
                    square = jnp.sum(
                        xb.astype(F32) * (tail[0:C] + base[0:C]), axis=0, keepdims=True
                    )
                    square = jnp.maximum(square + norms[j], 0.0)
                    r = lax.rsqrt(square * (1.0 / D) + 1e-06)
                    eps = tail[C : 2 * C] + base[C : 2 * C]
                else:
                    lin = dot(big, x_in)
                lin = (lin + tab_buf[slots[g]]) * r
                for n in range(HZ):
                    q = lin[n * HDIM : (n + 1) * HDIM].astype(BF16)
                    k = lin[B + n * HDIM : B + (n + 1) * HDIM].astype(BF16)
                    v_hi, v_lo = two(lin[QK + n * C : QK + (n + 1) * C])
                    items[g, n] = q, k, jnp.concatenate([v_hi, v_lo, ones_rows], axis=0)
            if 0 <= g - 1 < G:
                for n in range(HZ):
                    q, k, _ = items[g - 1, n]
                    scores[g - 1, n] = dot(k, q, 0, 0)
            if 0 <= g - 2 < G:
                for n in range(HZ):
                    block = scores.pop((g - 2, n))
                    top = jnp.max(block, axis=0, keepdims=True)
                    p = jnp.exp2(block - top).astype(BF16)
                    o = dot(items[g - 2, n][2], p)
                    out = out + (o[0:C] + o[C : 2 * C]) / o[2 * C : 2 * C + 1]
        return out, eps

    spread = [key for act, key in PLAN if act == "spread"]
    local = [key for act, key in PLAN if act == "local"]
    state, local_eps, drift, flying = {}, {}, {}, {}
    outward = sorted(
        range(1, 2 * PL), key=lambda d: (-(d // PL + (d % PL // H > 0)), -(d // PL))
    )

    def launch(key, slots):
        i, j = key
        x = start
        for m in range(j if i else 0):
            x = x + drift[(min(i - 1, m), m)]
        state[key] = x
        part, local_eps[key] = evaluate(x, j, slots)
        k = count[0]
        count[0] += 1
        if key in spread:
            slot = plane_buf.at[spread.index(key), e * PL + q_me]
            slot[...] = part.astype(BF16)
            peers = [group_peer(d) for d in outward]
        else:
            slot = chip_buf.at[local.index(key), h]
            slot[...] = part
            peers = [{"head": 1 - h}]
        for peer in peers:
            pltpu.make_async_remote_copy(
                src_ref=slot,
                dst_ref=slot,
                send_sem=ssem.at[k],
                recv_sem=rsem.at[k],
                device_id=peer,
                device_id_type=MESH,
            ).start()
        flying[key] = k

    def settle(key, sem):
        if key in spread:
            others = plane_buf.at[spread.index(key), pl.ds(0, 2 * PL - 1)]
        else:
            others = chip_buf.at[local.index(key), 0]
        pltpu.make_async_copy(others, others, sem).wait()

    def land(key):
        j, k = key[1], flying[key]
        settle(key, rsem.at[k])
        total = local_eps[key]
        if key in spread:
            for i in range(2 * PL):
                total = total + plane_buf[spread.index(key), i].astype(F32)
        else:
            for i in range(H):
                total = total + chip_buf[local.index(key), i]
        drift[key] = keeps[j] * state[key] + coefs[j] * total
        settle(key, ssem.at[k])

    def clear(_):
        for copy in started:
            copy.wait_send()
        started.clear()

    def gather(_):
        for copy in across + passed:
            copy.wait_recv()
        for g in range(2 * F):
            build(g, g, g // 2)

    def norms_now(_):
        lane = lax.broadcasted_iota(jnp.int32, res_ref.shape, 1)
        res = jnp.zeros(res_ref.shape, F32)
        old = [start] * S
        for it in range(ITERS):
            new, run = [], start
            for j in range(S):
                new.append(run)
                if j < S - 1:
                    run = run + drift[(min(it, j), j)]
            square = jnp.zeros((C, N), F32)
            for j in range(1, S):
                change = new[j] - old[j]
                square = square + change * change
            square = jnp.sum(
                jnp.sum(square, axis=0, keepdims=True), axis=1, keepdims=True
            )
            res = jnp.where(lane == it, jnp.sqrt(square / (S * C * N) + 1e-06), res)
            old = new
        res_ref[...] = res

    acts = {
        "clear": clear,
        "share": share_rest,
        "forward": forward,
        "gather": gather,
        "land": land,
        "norms": norms_now,
        "spread": lambda key: launch(key, [2 * F]),
        "local": lambda key: launch(key, list(range(2 * F))),
    }
    for act, key in PLAN:
        acts[act](key)
    final = jnp.zeros((C, N), F32)
    for j in range(S):
        final = jnp.where(s == j, state[(j, j)] + drift[(j, j)], final)
    half = final[:, 0:rows]
    for i in range(1, F):
        half = jnp.where(f == i, final[:, i * rows : (i + 1) * rows], half)
    traj_ref[0] = half


PLAN = (
    ("spread", (0, 0)),
    ("share", None),
    ("forward", 6),
    ("spread", (0, 1)),
    ("land", (0, 0)),
    ("spread", (1, 1)),
    ("forward", 1),
    ("land", (0, 1)),
    ("spread", (0, 2)),
    ("spread", (1, 2)),
    ("gather", None),
    ("clear", None),
    ("land", (1, 1)),
    ("local", (2, 2)),
    ("land", (2, 2)),
    ("local", (3, 3)),
    ("land", (0, 2)),
    ("land", (1, 2)),
    ("norms", None),
    ("land", (3, 3)),
)


def local_heads(
    start_noise,
    position,
    time_table,
    time_index,
    sched_index,
    coef_keep,
    coef_noise,
    w_in,
    norm_gain,
    w_qkv,
    w_proj,
    w_final,
):
    S, F, H = (lax.axis_size(a) for a in ("step", "frame", "head"))
    R = w_qkv.shape[0]
    C, rows = start_noise.shape
    D = position.shape[1]
    N = rows * F
    PL = F * H
    HZ = w_qkv.shape[2] // (F * 2 * HDIM)
    B = HZ * HDIM
    QK = 2 * B
    V = HZ * C
    late = 2 * V + (QK + V) // 4
    n_spread = sum(act == "spread" for act, _ in PLAN)
    n_local = sum(act == "local" for act, _ in PLAN)
    n_sems = 2 * (S - 1) + 3 + 5 * 7 + n_spread + n_local
    vmem = pl.BlockSpec(memory_space=pltpu.VMEM)
    smem = pl.BlockSpec(memory_space=pltpu.SMEM)
    here = pl.BlockSpec(memory_space=pl.ANY)
    traj, res = pl.pallas_call(
        functools.partial(kernel, S, F, H),
        out_shape=(pltpu.VMEM((1, C, rows), F32), pltpu.VMEM((1, ITERS), F32)),
        in_specs=[here, here, here, smem, smem] + [here] * 7,
        out_specs=(vmem, vmem),
        scratch_shapes=[
            pltpu.VMEM((rows, D), BF16),
            pltpu.VMEM(time_table.shape, BF16),
            pltpu.VMEM((1, coef_keep.shape[0]), F32),
            pltpu.VMEM((1, coef_noise.shape[0]), F32),
            pltpu.VMEM(w_in.shape, BF16),
            pltpu.VMEM((D,), F32),
            pltpu.VMEM((3, R, w_qkv.shape[2]), BF16),
            pltpu.VMEM(w_proj.shape, BF16),
            pltpu.VMEM(w_final.shape, BF16),
            pltpu.VMEM((2, QK + B, R), BF16),
            pltpu.VMEM((D, rows), BF16),
            pltpu.VMEM((R, rows), BF16),
            pltpu.VMEM((32, D), F32),
            pltpu.VMEM((32, R), BF16),
            pltpu.VMEM((2, B, N + 32), BF16),
            pltpu.VMEM((3, QK, rows), F32),
            pltpu.VMEM((3, QK, rows), BF16),
            pltpu.VMEM((3, QK, rows), BF16),
            pltpu.VMEM((3, QK, rows), BF16),
            pltpu.VMEM((3, QK, rows), BF16),
            pltpu.VMEM((S, C, 2 * B), BF16),
            pltpu.VMEM((F, C, rows), F32),
            pltpu.VMEM((S, 8, time_table.shape[0]), F32),
            pltpu.VMEM((F, 2 * C + 16, rows), F32),
            pltpu.VMEM((2 * F, F, QK, rows), BF16),
            pltpu.VMEM((2 * F, late, rows), BF16),
            pltpu.VMEM((2 * F + 1, QK + V, 32), BF16),
            pltpu.VMEM((2 * F + 1, QK + V, N), F32),
            pltpu.VMEM((S, 2 * C, N), F32),
            pltpu.VMEM((n_spread, 2 * PL, C, N), BF16),
            pltpu.VMEM((n_local, H, C, N), F32),
            pltpu.SemaphoreType.DMA((n_sems + 10,)),
            pltpu.SemaphoreType.DMA((n_sems,)),
        ],
        compiler_params=pltpu.CompilerParams(
            collective_id=0, has_side_effects=True, vmem_limit_bytes=60 * 1024 * 1024
        ),
    )(
        start_noise,
        position,
        time_table,
        time_index,
        sched_index,
        coef_keep[None],
        coef_noise[None],
        w_in,
        norm_gain,
        jnp.transpose(w_qkv, (1, 0, 2)),
        w_proj,
        w_final,
    )
    return traj, res.reshape(ITERS)


def one_head_each(mesh, start_noise, time_index, w_qkv, time_table):
    S, F, H = (mesh.shape[a] for a in ("step", "frame", "head"))
    return (
        S == ITERS
        and time_index.shape[0] == S
        and w_qkv.shape[2] == S * F * H * HDIM
        and w_qkv.shape[0] % (16 * S) == 0
        and start_noise.shape[1] % (128 * F) == 0
        and start_noise.shape[1] // F <= time_table.shape[0]
        and time_table.shape[0] % 128 == 0
    )


def solution(mesh):
    def call(*args):
        fits = one_head_each(mesh, args[0], args[3], args[9], args[2])
        return jax.shard_map(
            local_heads if fits else local_any,
            mesh=mesh,
            in_specs=(
                P("parts", "frame"),
                P("frame", None),
                P(),
                P("step"),
                P("step"),
                P(),
                P(),
                P(),
                P(),
                P("step", None, "head"),
                P("step", "head"),
                P(),
            ),
            out_specs=(P("step", "parts", "frame"), P("parts")),
            check_vma=False,
        )(*args)

    return call
```

```python
import functools
import math

import jax
import jax.numpy as jnp
from jax import lax
from jax.experimental import pallas as pl
from jax.experimental.pallas import tpu as pltpu
from jax.sharding import PartitionSpec as P

HDIM = 72
ITERS = 4


def entering(value, axis, combine, identity):
    count, here = (lax.axis_size(axis), lax.axis_index(axis))
    everything = lax.all_gather(value, axis)
    start = jnp.broadcast_to(jnp.asarray(identity, value.dtype), value.shape)

    def hop(k, before):
        reached = k < here
        new = combine(before, everything[k])
        return jnp.where(reached, new, before)

    return lax.fori_loop(0, count, hop, start)


def add_terms(first, second):
    return first + second


def local_any(
    start_noise,
    position,
    time_table,
    time_index,
    sched_index,
    coef_keep,
    coef_noise,
    w_in,
    norm_gain,
    w_qkv,
    w_proj,
    w_final,
):
    w_qkv_all, w_proj_all = (
        lax.all_gather(w_qkv, "step", axis=0, tiled=True),
        lax.all_gather(w_proj, "step", axis=0, tiled=True),
    )
    batch_steps = time_index.shape[0]
    row_count = start_noise.shape[1]
    table_rows = time_table.shape[0]
    pick_time = (time_index[:, None] == jnp.arange(table_rows)[None, :]).astype(jnp.bfloat16)
    time_embed = jnp.dot(pick_time, time_table, preferred_element_type=jnp.float32)
    pick_sched = (sched_index[:, None] == jnp.arange(table_rows)[None, :]).astype(jnp.float32)
    keep_rate = jnp.sum(pick_sched * coef_keep[None, :], axis=1)
    noise_rate = jnp.sum(pick_sched * coef_noise[None, :], axis=1)
    heads_local = w_qkv_all.shape[2] // HDIM
    cell_count = (
        batch_steps
        * lax.axis_size("step")
        * start_noise.shape[0]
        * row_count
        * lax.axis_size("frame")
    )
    states = start_noise[None]
    drift_term = jnp.zeros_like(states)
    residual_list = []
    for iteration in range(ITERS):
        latent_bf = states.astype(jnp.bfloat16)
        hidden = (
            jnp.einsum("bcr,cd->brd", latent_bf, w_in, preferred_element_type=jnp.float32)
            + position
            + time_embed[:, None, :]
        )
        normed = (
            hidden * lax.rsqrt(jnp.mean(hidden * hidden, axis=2, keepdims=True) + 1e-06) * norm_gain
        ).astype(jnp.bfloat16)
        projected = jnp.einsum(
            "brd,dkq->brkq", normed, w_qkv_all, preferred_element_type=jnp.float32
        ).astype(jnp.bfloat16)
        queries = projected[:, :, 0].reshape(batch_steps, row_count, heads_local, HDIM)
        score_scale = 1.0 / math.sqrt(HDIM)
        keys_values = projected[:, :, 1:3]
        piece = lax.all_gather(keys_values, "frame", axis=1, tiled=True)
        top_old = jnp.full((batch_steps, heads_local, row_count), -1e30, jnp.float32)
        piece_rows = piece.shape[1]
        keys_blk = piece[:, :, 0].reshape(batch_steps, piece_rows, heads_local, HDIM)
        values_blk = piece[:, :, 1].reshape(batch_steps, piece_rows, heads_local, HDIM)
        scores = (
            jnp.einsum("bqhe,bkhe->bhqk", queries, keys_blk, preferred_element_type=jnp.float32)
            * score_scale
        )
        top_new = jnp.maximum(top_old, jnp.max(scores, axis=3))
        weights_exp = jnp.exp(scores - top_new[:, :, :, None])
        total_new = jnp.sum(weights_exp, axis=3)
        update = jnp.einsum(
            "bhqk,bkhe->bqhe",
            weights_exp.astype(jnp.bfloat16),
            values_blk,
            preferred_element_type=jnp.float32,
        )
        accum = update
        top_final, total_final, accum = (top_new, total_new, accum)
        attended = accum / jnp.transpose(total_final, (0, 2, 1))[:, :, :, None]
        attn_mixed = attended.reshape(batch_steps, row_count, heads_local * HDIM).astype(
            jnp.bfloat16
        )
        partial_value = jnp.einsum(
            "brq,dq->brd", attn_mixed, w_proj_all, preferred_element_type=jnp.float32
        )
        head_total = lax.psum(partial_value, "head")
        joined = (hidden + head_total).astype(jnp.bfloat16)
        predicted = jnp.einsum("cd,brd->bcr", w_final, joined, preferred_element_type=jnp.float32)
        drift_term = keep_rate[:, None, None] * states + noise_rate[:, None, None] * predicted
        local_incl = jnp.cumsum(drift_term, axis=0)
        local_total = local_incl[-1]
        earlier = entering(local_total, "step", add_terms, jnp.zeros_like(local_total))
        before = earlier[None] + (local_incl - drift_term)
        new_states = start_noise[None] + before
        change = new_states - states
        square_sum = jnp.sum(change * change)
        summed = lax.psum(square_sum, ("step", "frame"))
        residual_list.append(jnp.sqrt(summed / cell_count + 1e-06))
        states = new_states
    residual_norms = jnp.stack(residual_list)
    trajectory = states + drift_term
    return (trajectory, residual_norms)


MESH = pl.DeviceIdType.MESH
F32 = jnp.float32
BF16 = jnp.bfloat16


def dot(a, b, ca=1, cb=0):
    return lax.dot_general(a, b, (((ca,), (cb,)), ((), ())), preferred_element_type=F32)


def dot_exact(a, b):
    return lax.dot_general(
        a, b, (((1,), (0,)), ((), ())), precision=lax.Precision.HIGHEST, preferred_element_type=F32
    )


def two(a):
    high = a.astype(BF16)
    return high, (a - high.astype(F32)).astype(BF16)


def kernel(
    S,
    F,
    H,
    noise_hbm,
    pos_hbm,
    table_hbm,
    tidx_ref,
    sidx_ref,
    keep_hbm,
    coef_hbm,
    win_hbm,
    gain_hbm,
    wqkv_hbm,
    wproj_hbm,
    wfin_hbm,
    traj_ref,
    res_ref,
    pos_ref,
    table_ref,
    keep_ref,
    coef_ref,
    win_ref,
    gain_ref,
    wqkv_ref,
    wproj_ref,
    wfin_ref,
    wt_ref,
    at_ref,
    at_peer,
    side_ref,
    side_cut,
    pv_ref,
    own_ref,
    near_send,
    near_recv,
    far_send,
    far_recv,
    mix_buf,
    noise_buf,
    meta_buf,
    ends_buf,
    fin_qk,
    fin_late,
    big_buf,
    tab_buf,
    base_buf,
    plane_buf,
    chip_buf,
    ssem,
    rsem,
):
    s, f, h = (lax.axis_index(a) for a in ("step", "frame", "head"))
    loads = [
        pltpu.make_async_copy(src, dst, ssem.at[ssem.shape[0] - 1 - n])
        for n, (src, dst) in enumerate(
            (
                (keep_hbm, keep_ref),
                (coef_hbm, coef_ref),
                (gain_hbm, gain_ref),
                (pos_hbm, pos_ref),
                (wqkv_hbm.at[0], wqkv_ref.at[0]),
                (wqkv_hbm.at[1], wqkv_ref.at[1]),
                (wqkv_hbm.at[2], wqkv_ref.at[2]),
                (wfin_hbm, wfin_ref),
                (wproj_hbm, wproj_ref),
                (noise_hbm, noise_buf.at[f]),
                (table_hbm, table_ref),
                (win_hbm, win_ref),
            )
        )
    ]
    for copy in loads:
        copy.start()
    PL = F * H
    q_me = f * H + h
    C, rows = noise_buf.shape[1:]
    D = pos_ref.shape[1]
    N = rows * F
    R = wqkv_ref.shape[1]
    lanes = table_ref.shape[0]
    e = lax.rem(s, 2)
    e_near = 1 - e
    s_near = s + 1 - 2 * e
    s_far = lax.rem(s + 2, S)
    HZ = wqkv_ref.shape[2] // (F * 2 * HDIM)
    B = HZ * HDIM
    QK = 2 * B
    V = HZ * C

    def step_peer(d):
        return {"step": lax.rem(s + d, S)}

    def group_peer(d):
        dz, df, dh = d // PL, d % PL // H, d % H
        return {
            "step": s_near if dz else s,
            "frame": lax.rem(f + df, F),
            "head": lax.rem(h + dh, H),
        }

    frame_peer = {"frame": 1 - f}

    barrier = pltpu.get_barrier_semaphore()
    for d in range(1, PL):
        pl.semaphore_signal(barrier, inc=1, device_id=group_peer(d), device_id_type=MESH)
    for d in range(1, S):
        pl.semaphore_signal(barrier, inc=1, device_id=step_peer(d), device_id_type=MESH)

    count = [0]
    started = []

    def send(src, dst, peer):
        k = count[0]
        count[0] += 1
        copy = pltpu.make_async_remote_copy(
            src_ref=src,
            dst_ref=dst,
            send_sem=ssem.at[k],
            recv_sem=rsem.at[k],
            device_id=peer,
            device_id_type=MESH,
        )
        copy.start()
        started.append(copy)
        return copy

    for copy in loads[:3]:
        copy.wait()
    row_id = lax.broadcasted_iota(jnp.int32, (8, lanes), 0)
    lane_id = lax.broadcasted_iota(jnp.int32, (1, lanes), 1)
    hot_t = jnp.where(lane_id == tidx_ref[0], 1.0, 0.0)
    hot_s = lane_id == sidx_ref[0]
    keep = jnp.sum(jnp.where(hot_s, keep_ref[...], 0.0), axis=1, keepdims=True)
    coef = jnp.sum(jnp.where(hot_s, coef_ref[...], 0.0), axis=1, keepdims=True)
    meta_buf[s] = jnp.where(row_id == 0, hot_t, jnp.where(row_id == 1, keep, coef))
    loads[3].wait()
    gain = gain_ref[...].reshape(1, D)
    pos = pos_ref[...]
    at_ref[...] = jnp.transpose(pos.astype(F32) * gain).astype(BF16)

    def turn_weights(parts):
        for i in range(F):

            @pl.when(f == i)
            def _():
                for p in parts:
                    turned = jnp.transpose(wqkv_ref[p, :, i * 2 * B : (i + 1) * 2 * B])
                    for t in range(2):
                        wt_ref[t, p * B : (p + 1) * B] = turned[t * B : (t + 1) * B]

    for p in range(2):
        loads[4 + p].wait()
    turn_weights((0, 1))
    mine = pl.ds(pl.multiple_of(s * R, R), R)
    at_mine = at_ref[mine]
    near_send[0] = dot(wt_ref[e_near, 0:QK], at_mine).astype(BF16)
    pl.semaphore_wait(barrier, S - 1 + PL - 1)
    to_near, to_far = {"step": s_near}, {"step": s_far}
    near, far = {}, {}

    def send_near(i, low, high):
        window = pl.ds(low, high - low)
        near[i, low] = send(near_send.at[i, window], near_recv.at[i, window], to_near)

    pieces = [(low, low + QK // 3) for low in range(0, QK, QK // 3)]
    order = sorted(range(1, S), key=lambda d: abs(d - S / 2))
    early = [send(meta_buf.at[s], meta_buf.at[s], step_peer(d)) for d in order]
    send_near(0, *pieces[0])
    turn = send(at_ref.at[mine], at_peer, frame_peer)
    for piece in pieces[1:]:
        send_near(0, *piece)
    for copy in loads[7:9]:
        copy.wait()
    rows_of = wfin_ref[:, 0:R].astype(F32)
    for j in range(1, S):
        rows_of = jnp.where(s == j, wfin_ref[:, j * R : (j + 1) * R].astype(F32), rows_of)
    folded = dot(rows_of.astype(BF16), wproj_ref[...])
    picked = folded[:, 0 : 2 * B]
    for i in range(1, F):
        picked = jnp.where(f == i, folded[:, i * 2 * B : (i + 1) * 2 * B], picked)
    mix_buf[s] = picked.astype(BF16)
    early += [send(mix_buf.at[s], mix_buf.at[s], step_peer(d)) for d in order]
    loads[9].wait()
    sides = [send(noise_buf.at[f], noise_buf.at[f], frame_peer)]
    own_ref[0] = dot(wt_ref[e, 0:QK], at_mine)
    loads[6].wait()
    turn_weights((2,))

    def pass_on(i, low, high):
        near[i, low].wait_recv()
        total = own_ref[i, low:high] + near_recv[i, low:high].astype(F32)
        far_send[i, low:high] = total.astype(BF16)
        window = pl.ds(low, high - low)
        far[i, low] = send(far_send.at[i, window], far_recv.at[i, window], to_far)

    pv_ref[0, :, 0:rows] = dot(wt_ref[e, QK : QK + B], at_mine).astype(BF16)
    pv_ref[1, :, 0:rows] = dot(wt_ref[e_near, QK : QK + B], at_mine).astype(BF16)
    for copy in loads[10:]:
        copy.wait()
    w_in = win_ref[...]
    ends = jnp.concatenate([w_in, wfin_ref[...]], axis=0)
    ends_in = dot(ends, w_in, 1, 1)
    posf = pos.astype(F32)
    sq_hi, sq_lo = two(posf * posf)
    ones = jnp.ones((8, D), BF16)
    ends_buf[f, 0 : 2 * C] = dot(ends, pos, 1, 1)
    ends_buf[f, 2 * C : 2 * C + 8] = dot(ones, sq_hi, 1, 1) + dot(ones, sq_lo, 1, 1)

    for piece in pieces:
        pass_on(0, *piece)
    turn.wait_recv()
    at_other = at_peer[...]
    near_send[1] = dot(wt_ref[e_near, 0:QK], at_other).astype(BF16)
    for piece in pieces:
        send_near(1, *piece)
    own_ref[1] = dot(wt_ref[e, 0:QK], at_other)
    pv_ref[0, :, rows : 2 * rows] = dot(wt_ref[e, QK : QK + B], at_other).astype(BF16)
    pv_ref[1, :, rows : 2 * rows] = dot(wt_ref[e_near, QK : QK + B], at_other).astype(BF16)

    side_ref[0:C] = w_in.astype(F32)
    for copy in early:
        copy.wait_recv()
    metas = [meta_buf[j] for j in range(S)]
    hot = jnp.concatenate(
        [m[0:1] for m in metas] + [jnp.zeros((8 - S, lanes), F32)], axis=0
    ).astype(BF16)
    keeps = [jnp.concatenate([m[1:2, :rows]] * F, axis=1) for m in metas]
    coefs = [jnp.concatenate([m[2:3, :rows]] * F, axis=1) for m in metas]
    temb = dot(hot, table_ref[...])
    side_ref[C : C + 8] = temb
    side_ref[C + 8 :] = jnp.zeros((32 - C - 8, D), F32)
    for j in range(S):

        @pl.when(s == j)
        def _():
            cut = slice(j * R, (j + 1) * R)
            side_cut[...] = (side_ref[:, cut] * gain[:, cut]).astype(BF16)

    side_mine = side_cut[...]
    mix = mix_buf[0].astype(F32)
    for j in range(1, S):
        mix = mix + mix_buf[j].astype(F32)
    mix_lane = lax.broadcasted_iota(jnp.int32, (V, B), 1) // HDIM
    mix_row = lax.broadcasted_iota(jnp.int32, (V, B), 0) // C

    def late_rows(role, member):
        turned = dot(wt_ref[member], side_mine, 1, 1)
        pv_ref[role, :, 2 * rows : 2 * rows + 32] = turned[QK:].astype(BF16)
        part = jnp.where(member == 0, mix[:, 0:B], mix[:, B : 2 * B])
        block = jnp.where(
            mix_lane == mix_row, jnp.concatenate([part] * HZ, axis=0), 0.0
        )
        block_hi, block_lo = two(block)
        values = dot(jnp.concatenate([block_hi, block_lo], axis=0), pv_ref[role])
        values = values[0:V] + values[V : 2 * V]
        packs = []
        for arr in (turned[0:QK], values[:, 2 * rows : 2 * rows + 32]):
            size = arr.shape[0] // 4
            packs.append(
                jnp.concatenate([arr[g * size : (g + 1) * size] for g in range(4)], axis=1)
            )
        return jnp.concatenate(
            [values[:, 0:rows], values[:, rows : 2 * rows]] + packs, axis=0
        )

    LATE = 2 * V + (QK + V) // 4
    near_send[2, 0:LATE] = late_rows(1, e_near).astype(BF16)
    send_near(2, 0, LATE)
    own_ref[2, 0:LATE] = late_rows(0, e)
    temb_b = temb.astype(BF16)
    ends_buf[f, 2 * C + 8 : 2 * C + 16] = dot(temb_b, pos, 1, 1)
    sides.append(send(ends_buf.at[f], ends_buf.at[f], frame_peer))
    ends_t = dot(ends, temb_b, 1, 1)
    norm_t = jnp.sum(temb * temb, axis=1, keepdims=True)
    for piece in pieces:
        pass_on(1, *piece)

    scale = 1.4426950408889634 / math.sqrt(HDIM)
    qk_row = lax.broadcasted_iota(jnp.int32, (QK, 1), 0)
    row_scale = jnp.where(qk_row < B, scale, 1.0)
    set_own, set_near = 2 * f + e, 2 * f + e_near
    halves = (f, 1 - f)

    def whole(i, low, high):
        far[i, low].wait_recv()
        total = far_send[i, low:high].astype(F32) + far_recv[i, low:high].astype(F32)
        return total.astype(BF16)

    def finish(i, low, high):
        total = whole(i, low, high)
        window = pl.ds(low, high - low)
        if i < 2:
            fin_qk[set_own, halves[i], low:high] = total
            ref = fin_qk.at[set_own, halves[i], window]
            twin = fin_qk.at[set_near, halves[i], window]
        else:
            fin_late[set_own] = total
            ref = fin_late.at[set_own]
            twin = fin_late.at[set_near]
        return ref, twin

    across, shared, passed = [], [], []

    def cross_over(refs):
        across.append(send(refs[0], refs[0], frame_peer))

    def share(refs):
        shared.append((send(refs[0], refs[0], to_near), refs[1]))

    def forward(number):
        for _ in range(number):
            copy, twin = shared.pop(0)
            copy.wait_recv()
            passed.append(send(twin, twin, frame_peer))

    ready = [finish(0, *piece) for piece in pieces]
    pass_on(2, 0, LATE)
    for refs in ready:
        cross_over(refs)
        share(refs)
    for copy in sides:
        copy.wait_recv()
    start = jnp.concatenate([noise_buf[i] for i in range(F)], axis=1)
    ends_all = jnp.concatenate([ends_buf[i] for i in range(F)], axis=1)
    ends_pos = ends_all[0 : 2 * C]
    norm_p = ends_all[2 * C : 2 * C + 1]
    cross = ends_all[2 * C + 8 : 2 * C + 16]
    norms = [norm_p + 2.0 * cross[j : j + 1] + norm_t[j : j + 1] for j in range(S)]
    for j in range(S):
        base_buf[j] = jnp.concatenate(
            [
                2.0 * (ends_pos[0:C] + ends_t[0:C, j : j + 1]),
                ends_pos[C : 2 * C] + ends_t[C : 2 * C, j : j + 1],
            ],
            axis=0,
        )
    ends_hi, ends_lo = two(
        jnp.concatenate([ends_in, jnp.zeros((2 * C, 32 - C), F32)], axis=1)
    )
    ends_big = jnp.concatenate([ends_hi, ends_lo], axis=0)
    size = QK // 4

    def build(slot, group, frame):
        last = fin_late[group].astype(F32)
        one, other = last[0:V], last[V : 2 * V]
        packed = last[2 * V : LATE]
        big_qk = jnp.concatenate(
            [packed[0:size, 32 * g : 32 * g + 32] for g in range(4)], axis=0
        )
        big_v = jnp.concatenate(
            [packed[size:, 32 * g : 32 * g + 32] for g in range(4)], axis=0
        )
        big_buf[slot, 0:QK] = (big_qk * row_scale).astype(BF16)
        big_buf[slot, QK:] = big_v.astype(BF16)
        for i in range(F):
            cut = slice(i * rows, (i + 1) * rows)
            tab_buf[slot, 0:QK, cut] = fin_qk[group, i].astype(F32) * row_scale
            tab_buf[slot, QK:, cut] = jnp.where(frame == i, one, other)

    ready = [finish(1, *piece) for piece in pieces]
    for refs in ready:
        cross_over(refs)
        share(refs)
    ready = finish(2, 0, LATE)
    build(4, set_own, f)

    def share_rest(_):
        cross_over(ready)
        share(ready)

    hot_row = lax.broadcasted_iota(jnp.int32, (32 - C, N), 0)
    ones_rows = jnp.ones((C, N), BF16)

    def evaluate(x, j, slots):
        xb = x.astype(BF16)
        pick = jnp.where(hot_row == j, 1.0, 0.0).astype(BF16)
        x_in = jnp.concatenate([xb, pick], axis=0)
        base = base_buf[j]
        out = jnp.zeros((C, N), F32)
        items, scores, r, eps = {}, {}, None, None
        G = len(slots)
        for g in range(G + 2):
            if g < G:
                big = big_buf[slots[g]]
                if g == 0:
                    lin = dot(jnp.concatenate([ends_big, big], axis=0), x_in)
                    tail = lin[0 : 2 * C] + lin[2 * C : 4 * C]
                    lin = lin[4 * C :]
                    square = jnp.sum(
                        xb.astype(F32) * (tail[0:C] + base[0:C]), axis=0, keepdims=True
                    )
                    square = jnp.maximum(square + norms[j], 0.0)
                    r = lax.rsqrt(square * (1.0 / D) + 1e-06)
                    eps = tail[C : 2 * C] + base[C : 2 * C]
                else:
                    lin = dot(big, x_in)
                lin = (lin + tab_buf[slots[g]]) * r
                for n in range(HZ):
                    q = lin[n * HDIM : (n + 1) * HDIM].astype(BF16)
                    k = lin[B + n * HDIM : B + (n + 1) * HDIM].astype(BF16)
                    v_hi, v_lo = two(lin[QK + n * C : QK + (n + 1) * C])
                    items[g, n] = q, k, jnp.concatenate([v_hi, v_lo, ones_rows], axis=0)
            if 0 <= g - 1 < G:
                for n in range(HZ):
                    q, k, _ = items[g - 1, n]
                    scores[g - 1, n] = dot(k, q, 0, 0)
            if 0 <= g - 2 < G:
                for n in range(HZ):
                    block = scores.pop((g - 2, n))
                    top = jnp.max(block, axis=0, keepdims=True)
                    p = jnp.exp2(block - top).astype(BF16)
                    o = dot(items[g - 2, n][2], p)
                    out = out + (o[0:C] + o[C : 2 * C]) / o[2 * C : 2 * C + 1]
        return out, eps

    spread = [key for act, key in PLAN if act == "spread"]
    local = [key for act, key in PLAN if act == "local"]
    state, local_eps, drift, flying = {}, {}, {}, {}
    outward = sorted(
        range(1, 2 * PL), key=lambda d: (-(d // PL + (d % PL // H > 0)), -(d // PL))
    )

    def launch(key, slots):
        i, j = key
        x = start
        for m in range(j if i else 0):
            x = x + drift[(min(i - 1, m), m)]
        state[key] = x
        part, local_eps[key] = evaluate(x, j, slots)
        k = count[0]
        count[0] += 1
        if key in spread:
            slot = plane_buf.at[spread.index(key), e * PL + q_me]
            slot[...] = part.astype(BF16)
            peers = [group_peer(d) for d in outward]
        else:
            slot = chip_buf.at[local.index(key), h]
            slot[...] = part
            peers = [{"head": 1 - h}]
        for peer in peers:
            pltpu.make_async_remote_copy(
                src_ref=slot,
                dst_ref=slot,
                send_sem=ssem.at[k],
                recv_sem=rsem.at[k],
                device_id=peer,
                device_id_type=MESH,
            ).start()
        flying[key] = k

    def settle(key, sem):
        if key in spread:
            others = plane_buf.at[spread.index(key), pl.ds(0, 2 * PL - 1)]
        else:
            others = chip_buf.at[local.index(key), 0]
        pltpu.make_async_copy(others, others, sem).wait()

    def land(key):
        j, k = key[1], flying[key]
        settle(key, rsem.at[k])
        total = local_eps[key]
        if key in spread:
            for i in range(2 * PL):
                total = total + plane_buf[spread.index(key), i].astype(F32)
        else:
            for i in range(H):
                total = total + chip_buf[local.index(key), i]
        drift[key] = keeps[j] * state[key] + coefs[j] * total
        settle(key, ssem.at[k])

    def clear(_):
        for copy in started:
            copy.wait_send()
        started.clear()

    def gather(_):
        build(set_own, set_own, f)
        build(set_near, set_near, f)
        for copies, member in ((across, e), (passed, e_near)):
            for copy in copies:
                copy.wait_recv()
            twin = 2 * (1 - f) + member
            build(twin, twin, 1 - f)

    def norms_now(_):
        lane = lax.broadcasted_iota(jnp.int32, res_ref.shape, 1)
        res = jnp.zeros(res_ref.shape, F32)
        old = [start] * S
        for it in range(ITERS):
            new, run = [], start
            for j in range(S):
                new.append(run)
                if j < S - 1:
                    run = run + drift[(min(it, j), j)]
            square = jnp.zeros((C, N), F32)
            for j in range(1, S):
                change = new[j] - old[j]
                square = square + change * change
            square = jnp.sum(
                jnp.sum(square, axis=0, keepdims=True), axis=1, keepdims=True
            )
            res = jnp.where(lane == it, jnp.sqrt(square / (S * C * N) + 1e-06), res)
            old = new
        res_ref[...] = res

    acts = {
        "clear": clear,
        "share": share_rest,
        "forward": forward,
        "gather": gather,
        "land": land,
        "norms": norms_now,
        "spread": lambda key: launch(key, [2 * F]),
        "local": lambda key: launch(key, list(range(2 * F))),
    }
    for act, key in PLAN:
        acts[act](key)
    final = jnp.zeros((C, N), F32)
    for j in range(S):
        final = jnp.where(s == j, state[(j, j)] + drift[(j, j)], final)
    half = final[:, 0:rows]
    for i in range(1, F):
        half = jnp.where(f == i, final[:, i * rows : (i + 1) * rows], half)
    traj_ref[0] = half


PLAN = (
    ("share", None),
    ("spread", (0, 0)),
    ("forward", 6),
    ("spread", (0, 1)),
    ("land", (0, 0)),
    ("forward", 1),
    ("spread", (1, 1)),
    ("land", (0, 1)),
    ("spread", (0, 2)),
    ("spread", (1, 2)),
    ("gather", None),
    ("clear", None),
    ("land", (1, 1)),
    ("local", (2, 2)),
    ("land", (2, 2)),
    ("local", (3, 3)),
    ("land", (0, 2)),
    ("land", (1, 2)),
    ("norms", None),
    ("land", (3, 3)),
)


def local_heads(
    start_noise,
    position,
    time_table,
    time_index,
    sched_index,
    coef_keep,
    coef_noise,
    w_in,
    norm_gain,
    w_qkv,
    w_proj,
    w_final,
):
    S, F, H = (lax.axis_size(a) for a in ("step", "frame", "head"))
    R = w_qkv.shape[0]
    C, rows = start_noise.shape
    D = position.shape[1]
    N = rows * F
    PL = F * H
    HZ = w_qkv.shape[2] // (F * 2 * HDIM)
    B = HZ * HDIM
    QK = 2 * B
    V = HZ * C
    late = 2 * V + (QK + V) // 4
    n_spread = sum(act == "spread" for act, _ in PLAN)
    n_local = sum(act == "local" for act, _ in PLAN)
    n_sems = 2 * (S - 1) + 3 + 5 * 7 + n_spread + n_local
    vmem = pl.BlockSpec(memory_space=pltpu.VMEM)
    smem = pl.BlockSpec(memory_space=pltpu.SMEM)
    here = pl.BlockSpec(memory_space=pl.ANY)
    traj, res = pl.pallas_call(
        functools.partial(kernel, S, F, H),
        out_shape=(pltpu.VMEM((1, C, rows), F32), pltpu.VMEM((1, ITERS), F32)),
        in_specs=[here, here, here, smem, smem] + [here] * 7,
        out_specs=(vmem, vmem),
        scratch_shapes=[
            pltpu.VMEM((rows, D), BF16),
            pltpu.VMEM(time_table.shape, BF16),
            pltpu.VMEM((1, coef_keep.shape[0]), F32),
            pltpu.VMEM((1, coef_noise.shape[0]), F32),
            pltpu.VMEM(w_in.shape, BF16),
            pltpu.VMEM((D,), F32),
            pltpu.VMEM((3, R, w_qkv.shape[2]), BF16),
            pltpu.VMEM(w_proj.shape, BF16),
            pltpu.VMEM(w_final.shape, BF16),
            pltpu.VMEM((2, QK + B, R), BF16),
            pltpu.VMEM((D, rows), BF16),
            pltpu.VMEM((R, rows), BF16),
            pltpu.VMEM((32, D), F32),
            pltpu.VMEM((32, R), BF16),
            pltpu.VMEM((2, B, N + 32), BF16),
            pltpu.VMEM((3, QK, rows), F32),
            pltpu.VMEM((3, QK, rows), BF16),
            pltpu.VMEM((3, QK, rows), BF16),
            pltpu.VMEM((3, QK, rows), BF16),
            pltpu.VMEM((3, QK, rows), BF16),
            pltpu.VMEM((S, C, 2 * B), BF16),
            pltpu.VMEM((F, C, rows), F32),
            pltpu.VMEM((S, 8, time_table.shape[0]), F32),
            pltpu.VMEM((F, 2 * C + 16, rows), F32),
            pltpu.VMEM((2 * F, F, QK, rows), BF16),
            pltpu.VMEM((2 * F, late, rows), BF16),
            pltpu.VMEM((2 * F + 1, QK + V, 32), BF16),
            pltpu.VMEM((2 * F + 1, QK + V, N), F32),
            pltpu.VMEM((S, 2 * C, N), F32),
            pltpu.VMEM((n_spread, 2 * PL, C, N), BF16),
            pltpu.VMEM((n_local, H, C, N), F32),
            pltpu.SemaphoreType.DMA((n_sems + 12,)),
            pltpu.SemaphoreType.DMA((n_sems,)),
        ],
        compiler_params=pltpu.CompilerParams(
            collective_id=0, has_side_effects=True, vmem_limit_bytes=60 * 1024 * 1024
        ),
    )(
        start_noise,
        position,
        time_table,
        time_index,
        sched_index,
        coef_keep[None],
        coef_noise[None],
        w_in,
        norm_gain,
        jnp.transpose(w_qkv, (1, 0, 2)),
        w_proj,
        w_final,
    )
    return traj, res.reshape(ITERS)


def one_head_each(mesh, start_noise, time_index, w_qkv, time_table):
    S, F, H = (mesh.shape[a] for a in ("step", "frame", "head"))
    return (
        S == ITERS
        and time_index.shape[0] == S
        and w_qkv.shape[2] == S * F * H * HDIM
        and w_qkv.shape[0] % (16 * S) == 0
        and start_noise.shape[1] % (128 * F) == 0
        and start_noise.shape[1] // F <= time_table.shape[0]
        and time_table.shape[0] % 128 == 0
    )


def solution(mesh):
    def call(*args):
        fits = one_head_each(mesh, args[0], args[3], args[9], args[2])
        return jax.shard_map(
            local_heads if fits else local_any,
            mesh=mesh,
            in_specs=(
                P("parts", "frame"),
                P("frame", None),
                P(),
                P("step"),
                P("step"),
                P(),
                P(),
                P(),
                P(),
                P("step", None, "head"),
                P("step", "head"),
                P(),
            ),
            out_specs=(P("step", "parts", "frame"), P("parts")),
            check_vma=False,
        )(*args)

    return call
```

```python
import functools
import math

import jax
import jax.numpy as jnp
from jax import lax
from jax.experimental import pallas as pl
from jax.experimental.pallas import tpu as pltpu
from jax.sharding import PartitionSpec as P

HDIM = 72
ITERS = 4


def entering(value, axis, combine, identity):
    count, here = (lax.axis_size(axis), lax.axis_index(axis))
    everything = lax.all_gather(value, axis)
    start = jnp.broadcast_to(jnp.asarray(identity, value.dtype), value.shape)

    def hop(k, before):
        reached = k < here
        new = combine(before, everything[k])
        return jnp.where(reached, new, before)

    return lax.fori_loop(0, count, hop, start)


def add_terms(first, second):
    return first + second


def local_any(
    start_noise,
    position,
    time_table,
    time_index,
    sched_index,
    coef_keep,
    coef_noise,
    w_in,
    norm_gain,
    w_qkv,
    w_proj,
    w_final,
):
    w_qkv_all, w_proj_all = (
        lax.all_gather(w_qkv, "step", axis=0, tiled=True),
        lax.all_gather(w_proj, "step", axis=0, tiled=True),
    )
    batch_steps = time_index.shape[0]
    row_count = start_noise.shape[1]
    table_rows = time_table.shape[0]
    pick_time = (time_index[:, None] == jnp.arange(table_rows)[None, :]).astype(jnp.bfloat16)
    time_embed = jnp.dot(pick_time, time_table, preferred_element_type=jnp.float32)
    pick_sched = (sched_index[:, None] == jnp.arange(table_rows)[None, :]).astype(jnp.float32)
    keep_rate = jnp.sum(pick_sched * coef_keep[None, :], axis=1)
    noise_rate = jnp.sum(pick_sched * coef_noise[None, :], axis=1)
    heads_local = w_qkv_all.shape[2] // HDIM
    cell_count = (
        batch_steps
        * lax.axis_size("step")
        * start_noise.shape[0]
        * row_count
        * lax.axis_size("frame")
    )
    states = start_noise[None]
    drift_term = jnp.zeros_like(states)
    residual_list = []
    for iteration in range(ITERS):
        latent_bf = states.astype(jnp.bfloat16)
        hidden = (
            jnp.einsum("bcr,cd->brd", latent_bf, w_in, preferred_element_type=jnp.float32)
            + position
            + time_embed[:, None, :]
        )
        normed = (
            hidden * lax.rsqrt(jnp.mean(hidden * hidden, axis=2, keepdims=True) + 1e-06) * norm_gain
        ).astype(jnp.bfloat16)
        projected = jnp.einsum(
            "brd,dkq->brkq", normed, w_qkv_all, preferred_element_type=jnp.float32
        ).astype(jnp.bfloat16)
        queries = projected[:, :, 0].reshape(batch_steps, row_count, heads_local, HDIM)
        score_scale = 1.0 / math.sqrt(HDIM)
        keys_values = projected[:, :, 1:3]
        piece = lax.all_gather(keys_values, "frame", axis=1, tiled=True)
        top_old = jnp.full((batch_steps, heads_local, row_count), -1e30, jnp.float32)
        piece_rows = piece.shape[1]
        keys_blk = piece[:, :, 0].reshape(batch_steps, piece_rows, heads_local, HDIM)
        values_blk = piece[:, :, 1].reshape(batch_steps, piece_rows, heads_local, HDIM)
        scores = (
            jnp.einsum("bqhe,bkhe->bhqk", queries, keys_blk, preferred_element_type=jnp.float32)
            * score_scale
        )
        top_new = jnp.maximum(top_old, jnp.max(scores, axis=3))
        weights_exp = jnp.exp(scores - top_new[:, :, :, None])
        total_new = jnp.sum(weights_exp, axis=3)
        update = jnp.einsum(
            "bhqk,bkhe->bqhe",
            weights_exp.astype(jnp.bfloat16),
            values_blk,
            preferred_element_type=jnp.float32,
        )
        accum = update
        top_final, total_final, accum = (top_new, total_new, accum)
        attended = accum / jnp.transpose(total_final, (0, 2, 1))[:, :, :, None]
        attn_mixed = attended.reshape(batch_steps, row_count, heads_local * HDIM).astype(
            jnp.bfloat16
        )
        partial_value = jnp.einsum(
            "brq,dq->brd", attn_mixed, w_proj_all, preferred_element_type=jnp.float32
        )
        head_total = lax.psum(partial_value, "head")
        joined = (hidden + head_total).astype(jnp.bfloat16)
        predicted = jnp.einsum("cd,brd->bcr", w_final, joined, preferred_element_type=jnp.float32)
        drift_term = keep_rate[:, None, None] * states + noise_rate[:, None, None] * predicted
        local_incl = jnp.cumsum(drift_term, axis=0)
        local_total = local_incl[-1]
        earlier = entering(local_total, "step", add_terms, jnp.zeros_like(local_total))
        before = earlier[None] + (local_incl - drift_term)
        new_states = start_noise[None] + before
        change = new_states - states
        square_sum = jnp.sum(change * change)
        summed = lax.psum(square_sum, ("step", "frame"))
        residual_list.append(jnp.sqrt(summed / cell_count + 1e-06))
        states = new_states
    residual_norms = jnp.stack(residual_list)
    trajectory = states + drift_term
    return (trajectory, residual_norms)


MESH = pl.DeviceIdType.MESH
F32 = jnp.float32
BF16 = jnp.bfloat16


def dot(a, b, ca=1, cb=0):
    return lax.dot_general(a, b, (((ca,), (cb,)), ((), ())), preferred_element_type=F32)


def dot_exact(a, b):
    return lax.dot_general(
        a, b, (((1,), (0,)), ((), ())), precision=lax.Precision.HIGHEST, preferred_element_type=F32
    )


def two(a):
    high = a.astype(BF16)
    return high, (a - high.astype(F32)).astype(BF16)


def kernel(
    S,
    F,
    H,
    noise_hbm,
    pos_hbm,
    table_hbm,
    tidx_ref,
    sidx_ref,
    keep_hbm,
    coef_hbm,
    win_hbm,
    gain_hbm,
    wqkv_hbm,
    wproj_hbm,
    wfin_hbm,
    traj_ref,
    res_ref,
    pos_ref,
    table_ref,
    keep_ref,
    coef_ref,
    win_ref,
    gain_ref,
    wqkv_ref,
    wproj_ref,
    wfin_ref,
    wt_ref,
    at_ref,
    at_peer,
    side_ref,
    side_cut,
    pv_ref,
    own_ref,
    near_send,
    near_recv,
    far_send,
    far_recv,
    mix_buf,
    noise_buf,
    meta_buf,
    ends_buf,
    fin_qk,
    fin_late,
    big_buf,
    tab_buf,
    base_buf,
    plane_buf,
    chip_buf,
    ssem,
    rsem,
):
    s, f, h = (lax.axis_index(a) for a in ("step", "frame", "head"))
    loads = [
        pltpu.make_async_copy(src, dst, ssem.at[n])
        for n, (src, dst) in enumerate(
            (
                (keep_hbm, keep_ref),
                (coef_hbm, coef_ref),
                (gain_hbm, gain_ref),
                (pos_hbm, pos_ref),
                (wqkv_hbm.at[0], wqkv_ref.at[0]),
                (wqkv_hbm.at[1], wqkv_ref.at[1]),
                (wqkv_hbm.at[2], wqkv_ref.at[2]),
                (wfin_hbm, wfin_ref),
                (wproj_hbm, wproj_ref),
                (noise_hbm, noise_buf.at[f]),
                (table_hbm, table_ref),
                (win_hbm, win_ref),
            )
        )
    ]
    for copy in loads:
        copy.start()
    PL = F * H
    q_me = f * H + h
    C, rows = noise_buf.shape[1:]
    D = pos_ref.shape[1]
    N = rows * F
    R = wqkv_ref.shape[1]
    lanes = table_ref.shape[0]
    e = lax.rem(s, 2)
    e_near = 1 - e
    s_near = s + 1 - 2 * e
    s_far = lax.rem(s + 2, S)
    HZ = wqkv_ref.shape[2] // (F * 2 * HDIM)
    B = HZ * HDIM
    QK = 2 * B
    V = HZ * C

    def step_peer(d):
        return {"step": lax.rem(s + d, S)}

    def group_peer(d):
        dz, df, dh = d // PL, d % PL // H, d % H
        return {
            "step": s_near if dz else s,
            "frame": lax.rem(f + df, F),
            "head": lax.rem(h + dh, H),
        }

    frame_peer = {"frame": 1 - f}

    barrier = pltpu.get_barrier_semaphore()
    for d in range(1, PL):
        pl.semaphore_signal(barrier, inc=1, device_id=group_peer(d), device_id_type=MESH)
    for d in range(1, S):
        pl.semaphore_signal(barrier, inc=1, device_id=step_peer(d), device_id_type=MESH)

    reused = ("across", "share", "pass", "late", "pass late", "ends")
    fresh = ("near", "far", "turn", "meta", "mix", "noise")
    outs = {name: n for n, name in enumerate(reused)}
    outs.update((name, len(loads) + n) for n, name in enumerate(fresh))
    spare = list(range(len(reused), len(loads)))
    spare += list(range(len(loads) + len(fresh), ssem.shape[0]))
    ins = {}

    def prepare(src, dst, peer, out, into):
        return pltpu.make_async_remote_copy(
            src_ref=src,
            dst_ref=dst,
            send_sem=ssem.at[outs[out]],
            recv_sem=rsem.at[ins.setdefault(into, len(ins))],
            device_id=peer,
            device_id_type=MESH,
        )

    def send(src, dst, peer, out, into):
        copy = prepare(src, dst, peer, out, into)
        copy.start()
        return copy

    def settle(ref, sem):
        pltpu.make_async_copy(ref, ref, sem).wait()

    def arrive(ref, into):
        settle(ref, rsem.at[ins[into]])

    for copy in loads[:3]:
        copy.wait()
    row_id = lax.broadcasted_iota(jnp.int32, (8, lanes), 0)
    lane_id = lax.broadcasted_iota(jnp.int32, (1, lanes), 1)
    hot_t = jnp.where(lane_id == tidx_ref[0], 1.0, 0.0)
    hot_s = lane_id == sidx_ref[0]
    keep = jnp.sum(jnp.where(hot_s, keep_ref[...], 0.0), axis=1, keepdims=True)
    coef = jnp.sum(jnp.where(hot_s, coef_ref[...], 0.0), axis=1, keepdims=True)
    meta_buf[s] = jnp.where(row_id == 0, hot_t, jnp.where(row_id == 1, keep, coef))
    loads[3].wait()
    gain = gain_ref[...].reshape(1, D)
    pos = pos_ref[...]
    at_ref[...] = jnp.transpose(pos.astype(F32) * gain).astype(BF16)

    def turn_weights(parts):
        for i in range(F):

            @pl.when(f == i)
            def _():
                for p in parts:
                    turned = jnp.transpose(wqkv_ref[p, :, i * 2 * B : (i + 1) * 2 * B])
                    for t in range(2):
                        wt_ref[t, p * B : (p + 1) * B] = turned[t * B : (t + 1) * B]

    for p in range(2):
        loads[4 + p].wait()
    turn_weights((0, 1))
    mine = pl.ds(pl.multiple_of(s * R, R), R)
    at_mine = at_ref[mine]
    near_send[0] = dot(wt_ref[e_near, 0:QK], at_mine).astype(BF16)
    pl.semaphore_wait(barrier, S - 1 + PL - 1)
    to_near, to_far = {"step": s_near}, {"step": s_far}
    near, far = {}, {}

    def send_near(i, low, high):
        window = pl.ds(low, high - low)
        near[i, low] = send(
            near_send.at[i, window],
            near_recv.at[i, window],
            to_near,
            "late" if i == 2 else "near",
            ("near", i, low),
        )

    pieces = [(low, low + QK // 3) for low in range(0, QK, QK // 3)]
    order = sorted(range(1, S), key=lambda d: abs(d - S / 2))
    for d in order:
        send(meta_buf.at[s], meta_buf.at[s], step_peer(d), "meta", "meta")
    send_near(0, *pieces[0])
    turn = send(at_ref.at[mine], at_peer, frame_peer, "turn", "turn")
    for piece in pieces[1:]:
        send_near(0, *piece)
    for copy in loads[7:9]:
        copy.wait()
    rows_of = wfin_ref[:, 0:R].astype(F32)
    for j in range(1, S):
        rows_of = jnp.where(s == j, wfin_ref[:, j * R : (j + 1) * R].astype(F32), rows_of)
    folded = dot(rows_of.astype(BF16), wproj_ref[...])
    picked = folded[:, 0 : 2 * B]
    for i in range(1, F):
        picked = jnp.where(f == i, folded[:, i * 2 * B : (i + 1) * 2 * B], picked)
    mix_buf[s] = picked.astype(BF16)
    for d in order:
        send(mix_buf.at[s], mix_buf.at[s], step_peer(d), "mix", "mix")
    loads[9].wait()
    sides = [send(noise_buf.at[f], noise_buf.at[f], frame_peer, "noise", "noise")]
    own_ref[0] = dot(wt_ref[e, 0:QK], at_mine)
    loads[6].wait()
    turn_weights((2,))

    def pass_on(i, low, high):
        near[i, low].wait_recv()
        total = own_ref[i, low:high] + near_recv[i, low:high].astype(F32)
        far_send[i, low:high] = total.astype(BF16)
        window = pl.ds(low, high - low)
        far[i, low] = send(
            far_send.at[i, window],
            far_recv.at[i, window],
            to_far,
            "late" if i == 2 else "far",
            ("far", i, low),
        )

    pv_ref[0, :, 0:rows] = dot(wt_ref[e, QK : QK + B], at_mine).astype(BF16)
    pv_ref[1, :, 0:rows] = dot(wt_ref[e_near, QK : QK + B], at_mine).astype(BF16)
    for copy in loads[10:]:
        copy.wait()
    w_in = win_ref[...]
    ends = jnp.concatenate([w_in, wfin_ref[...]], axis=0)
    ends_in = dot(ends, w_in, 1, 1)
    posf = pos.astype(F32)
    sq_hi, sq_lo = two(posf * posf)
    ones = jnp.ones((8, D), BF16)
    ends_buf[f, 0 : 2 * C] = dot(ends, pos, 1, 1)
    ends_buf[f, 2 * C : 2 * C + 8] = dot(ones, sq_hi, 1, 1) + dot(ones, sq_lo, 1, 1)

    for piece in pieces:
        pass_on(0, *piece)
    turn.wait_recv()
    at_other = at_peer[...]
    near_send[1] = dot(wt_ref[e_near, 0:QK], at_other).astype(BF16)
    for piece in pieces:
        send_near(1, *piece)
    own_ref[1] = dot(wt_ref[e, 0:QK], at_other)
    pv_ref[0, :, rows : 2 * rows] = dot(wt_ref[e, QK : QK + B], at_other).astype(BF16)
    pv_ref[1, :, rows : 2 * rows] = dot(wt_ref[e_near, QK : QK + B], at_other).astype(BF16)

    side_ref[0:C] = w_in.astype(F32)
    arrive(meta_buf.at[pl.ds(0, S - 1)], "meta")
    arrive(mix_buf.at[pl.ds(0, S - 1)], "mix")
    metas = [meta_buf[j] for j in range(S)]
    hot = jnp.concatenate(
        [m[0:1] for m in metas] + [jnp.zeros((8 - S, lanes), F32)], axis=0
    ).astype(BF16)
    keeps = [jnp.concatenate([m[1:2, :rows]] * F, axis=1) for m in metas]
    coefs = [jnp.concatenate([m[2:3, :rows]] * F, axis=1) for m in metas]
    temb = dot(hot, table_ref[...])
    side_ref[C : C + 8] = temb
    side_ref[C + 8 :] = jnp.zeros((32 - C - 8, D), F32)
    for j in range(S):

        @pl.when(s == j)
        def _():
            cut = slice(j * R, (j + 1) * R)
            side_cut[...] = (side_ref[:, cut] * gain[:, cut]).astype(BF16)

    side_mine = side_cut[...]
    mix = mix_buf[0].astype(F32)
    for j in range(1, S):
        mix = mix + mix_buf[j].astype(F32)
    mix_lane = lax.broadcasted_iota(jnp.int32, (V, B), 1) // HDIM
    mix_row = lax.broadcasted_iota(jnp.int32, (V, B), 0) // C

    def late_rows(role, member):
        turned = dot(wt_ref[member], side_mine, 1, 1)
        pv_ref[role, :, 2 * rows : 2 * rows + 32] = turned[QK:].astype(BF16)
        part = jnp.where(member == 0, mix[:, 0:B], mix[:, B : 2 * B])
        block = jnp.where(
            mix_lane == mix_row, jnp.concatenate([part] * HZ, axis=0), 0.0
        )
        block_hi, block_lo = two(block)
        values = dot(jnp.concatenate([block_hi, block_lo], axis=0), pv_ref[role])
        values = values[0:V] + values[V : 2 * V]
        packs = []
        for arr in (turned[0:QK], values[:, 2 * rows : 2 * rows + 32]):
            size = arr.shape[0] // 4
            packs.append(
                jnp.concatenate([arr[g * size : (g + 1) * size] for g in range(4)], axis=1)
            )
        return jnp.concatenate(
            [values[:, 0:rows], values[:, rows : 2 * rows]] + packs, axis=0
        )

    LATE = 2 * V + (QK + V) // 4
    near_send[2, 0:LATE] = late_rows(1, e_near).astype(BF16)
    send_near(2, 0, LATE)
    own_ref[2, 0:LATE] = late_rows(0, e)
    temb_b = temb.astype(BF16)
    ends_buf[f, 2 * C + 8 : 2 * C + 16] = dot(temb_b, pos, 1, 1)
    sides.append(send(ends_buf.at[f], ends_buf.at[f], frame_peer, "ends", "ends"))
    ends_t = dot(ends, temb_b, 1, 1)
    norm_t = jnp.sum(temb * temb, axis=1, keepdims=True)
    for piece in pieces:
        pass_on(1, *piece)

    scale = 1.4426950408889634 / math.sqrt(HDIM)
    qk_row = lax.broadcasted_iota(jnp.int32, (QK, 1), 0)
    row_scale = jnp.where(qk_row < B, scale, 1.0)
    set_own, set_near = 2 * f + e, 2 * f + e_near
    halves = (f, 1 - f)

    def whole(i, low, high):
        far[i, low].wait_recv()
        total = far_send[i, low:high].astype(F32) + far_recv[i, low:high].astype(F32)
        return total.astype(BF16)

    def finish(i, low, high):
        total = whole(i, low, high)
        window = pl.ds(low, high - low)
        if i < 2:
            fin_qk[set_own, halves[i], low:high] = total
            ref = fin_qk.at[set_own, halves[i], window]
            twin = fin_qk.at[set_near, halves[i], window]
        else:
            fin_late[set_own] = total
            ref = fin_late.at[set_own]
            twin = fin_late.at[set_near]
        return ref, twin

    shared = []

    def hand_on(refs, kind):
        send(refs[0], refs[0], frame_peer, kind or "across", kind and "late" or "across")

    def share(refs, kind):
        copy = send(refs[0], refs[0], to_near, kind or "share", ("share", len(shared)))
        shared.append((copy, refs[1], kind))

    def offer(refs, kind=None):
        hand_on(refs, kind)
        share(refs, kind)

    def forward(_):
        for copy, twin, kind in shared:
            copy.wait_recv()
            send(
                twin,
                twin,
                frame_peer,
                "pass late" if kind else "pass",
                "late" if kind else "pass",
            )

    ready = [finish(0, *piece) for piece in pieces]
    pass_on(2, 0, LATE)
    for refs in ready:
        offer(refs)
    for copy in sides:
        copy.wait_recv()
    start = jnp.concatenate([noise_buf[i] for i in range(F)], axis=1)
    ends_all = jnp.concatenate([ends_buf[i] for i in range(F)], axis=1)
    ends_pos = ends_all[0 : 2 * C]
    norm_p = ends_all[2 * C : 2 * C + 1]
    cross = ends_all[2 * C + 8 : 2 * C + 16]
    norms = [norm_p + 2.0 * cross[j : j + 1] + norm_t[j : j + 1] for j in range(S)]
    for j in range(S):
        base_buf[j] = jnp.concatenate(
            [
                2.0 * (ends_pos[0:C] + ends_t[0:C, j : j + 1]),
                ends_pos[C : 2 * C] + ends_t[C : 2 * C, j : j + 1],
            ],
            axis=0,
        )
    ends_hi, ends_lo = two(
        jnp.concatenate([ends_in, jnp.zeros((2 * C, 32 - C), F32)], axis=1)
    )
    ends_big = jnp.concatenate([ends_hi, ends_lo], axis=0)
    size = QK // 4

    def build(slot, group, frame):
        last = fin_late[group].astype(F32)
        one, other = last[0:V], last[V : 2 * V]
        packed = last[2 * V : LATE]
        big_qk = jnp.concatenate(
            [packed[0:size, 32 * g : 32 * g + 32] for g in range(4)], axis=0
        )
        big_v = jnp.concatenate(
            [packed[size:, 32 * g : 32 * g + 32] for g in range(4)], axis=0
        )
        big_buf[slot, 0:QK] = (big_qk * row_scale).astype(BF16)
        big_buf[slot, QK:] = big_v.astype(BF16)
        for i in range(F):
            cut = slice(i * rows, (i + 1) * rows)
            tab_buf[slot, 0:QK, cut] = fin_qk[group, i].astype(F32) * row_scale
            tab_buf[slot, QK:, cut] = jnp.where(frame == i, one, other)

    ready = [finish(1, *piece) for piece in pieces]
    for refs in ready:
        offer(refs)
    ready = finish(2, 0, LATE)
    build(4, set_own, f)

    def share_rest(_):
        offer(ready, "late")

    hot_row = lax.broadcasted_iota(jnp.int32, (32 - C, N), 0)
    ones_rows = jnp.ones((C, N), BF16)

    def evaluate(x, j, slots):
        xb = x.astype(BF16)
        pick = jnp.where(hot_row == j, 1.0, 0.0).astype(BF16)
        x_in = jnp.concatenate([xb, pick], axis=0)
        base = base_buf[j]
        out = jnp.zeros((C, N), F32)
        items, scores, r, eps = {}, {}, None, None
        G = len(slots)
        for g in range(G + 2):
            if g < G:
                big = big_buf[slots[g]]
                if g == 0:
                    lin = dot(jnp.concatenate([ends_big, big], axis=0), x_in)
                    tail = lin[0 : 2 * C] + lin[2 * C : 4 * C]
                    lin = lin[4 * C :]
                    square = jnp.sum(
                        xb.astype(F32) * (tail[0:C] + base[0:C]), axis=0, keepdims=True
                    )
                    square = jnp.maximum(square + norms[j], 0.0)
                    r = lax.rsqrt(square * (1.0 / D) + 1e-06)
                    eps = tail[C : 2 * C] + base[C : 2 * C]
                else:
                    lin = dot(big, x_in)
                lin = (lin + tab_buf[slots[g]]) * r
                for n in range(HZ):
                    q = lin[n * HDIM : (n + 1) * HDIM].astype(BF16)
                    k = lin[B + n * HDIM : B + (n + 1) * HDIM].astype(BF16)
                    v_hi, v_lo = two(lin[QK + n * C : QK + (n + 1) * C])
                    items[g, n] = q, k, jnp.concatenate([v_hi, v_lo, ones_rows], axis=0)
            if 0 <= g - 1 < G:
                for n in range(HZ):
                    q, k, _ = items[g - 1, n]
                    scores[g - 1, n] = dot(k, q, 0, 0)
            if 0 <= g - 2 < G:
                for n in range(HZ):
                    block = scores.pop((g - 2, n))
                    top = jnp.max(block, axis=0, keepdims=True)
                    p = jnp.exp2(block - top).astype(BF16)
                    o = dot(items[g - 2, n][2], p)
                    out = out + (o[0:C] + o[C : 2 * C]) / o[2 * C : 2 * C + 1]
        return out, eps

    spread = [key for act, key in PLAN if act == "spread"]
    local = [key for act, key in PLAN if act == "local"]
    state, local_eps, drift, flying = {}, {}, {}, {}
    rounds_at = rsem.shape[0] - len(spread) - len(local)
    outward = sorted(
        range(1, 2 * PL), key=lambda d: (-(d // PL + (d % PL // H > 0)), -(d // PL))
    )

    def launch(key, slots):
        i, j = key
        x = start
        for m in range(j if i else 0):
            x = x + drift[(min(i - 1, m), m)]
        state[key] = x
        part, local_eps[key] = evaluate(x, j, slots)
        k = flying[key] = len(flying)
        if key in spread:
            slot = plane_buf.at[spread.index(key), e * PL + q_me]
            slot[...] = part.astype(BF16)
            peers = [group_peer(d) for d in outward]
        else:
            slot = chip_buf.at[local.index(key), h]
            slot[...] = part
            peers = [{"head": 1 - h}]
        for peer in peers:
            pltpu.make_async_remote_copy(
                src_ref=slot,
                dst_ref=slot,
                send_sem=ssem.at[spare[k]],
                recv_sem=rsem.at[rounds_at + k],
                device_id=peer,
                device_id_type=MESH,
            ).start()

    def land(key):
        j, k = key[1], flying[key]
        if key in spread:
            others = plane_buf.at[spread.index(key), pl.ds(0, 2 * PL - 1)]
        else:
            others = chip_buf.at[local.index(key), 0]
        settle(others, rsem.at[rounds_at + k])
        total = local_eps[key]
        if key in spread:
            for i in range(2 * PL):
                total = total + plane_buf[spread.index(key), i].astype(F32)
        else:
            for i in range(H):
                total = total + chip_buf[local.index(key), i]
        drift[key] = keeps[j] * state[key] + coefs[j] * total
        settle(others, ssem.at[spare[k]])

    def clear(_):
        for out, ref in (
            ("near", near_send.at[pl.ds(0, 2)]),
            ("far", far_send.at[pl.ds(0, 2)]),
            ("across", fin_qk.at[0]),
            ("share", fin_qk.at[0]),
            ("pass", fin_qk.at[0]),
            ("late", fin_late),
            ("pass late", fin_late.at[0]),
            ("turn", at_peer),
            ("meta", meta_buf.at[pl.ds(0, S - 1)]),
            ("mix", mix_buf.at[pl.ds(0, S - 1)]),
            ("noise", noise_buf.at[0]),
            ("ends", ends_buf.at[0]),
        ):
            settle(ref, ssem.at[outs[out]])

    def gather(_):
        build(set_own, set_own, f)
        build(set_near, set_near, f)
        arrive(fin_qk.at[0], "across")
        arrive(fin_qk.at[0], "pass")
        arrive(fin_late.at[pl.ds(0, 2)], "late")
        for member in (e, e_near):
            twin = 2 * (1 - f) + member
            build(twin, twin, 1 - f)

    def norms_now(_):
        lane = lax.broadcasted_iota(jnp.int32, res_ref.shape, 1)
        res = jnp.zeros(res_ref.shape, F32)
        old = [start] * S
        for it in range(ITERS):
            new, run = [], start
            for j in range(S):
                new.append(run)
                if j < S - 1:
                    run = run + drift[(min(it, j), j)]
            square = jnp.zeros((C, N), F32)
            for j in range(1, S):
                change = new[j] - old[j]
                square = square + change * change
            square = jnp.sum(
                jnp.sum(square, axis=0, keepdims=True), axis=1, keepdims=True
            )
            res = jnp.where(lane == it, jnp.sqrt(square / (S * C * N) + 1e-06), res)
            old = new
        res_ref[...] = res

    acts = {
        "clear": clear,
        "share": share_rest,
        "forward": forward,
        "gather": gather,
        "land": land,
        "norms": norms_now,
        "spread": lambda key: launch(key, [2 * F]),
        "local": lambda key: launch(key, list(range(2 * F))),
    }
    for act, key in PLAN:
        acts[act](key)
    final = jnp.zeros((C, N), F32)
    for j in range(S):
        final = jnp.where(s == j, state[(j, j)] + drift[(j, j)], final)
    half = final[:, 0:rows]
    for i in range(1, F):
        half = jnp.where(f == i, final[:, i * rows : (i + 1) * rows], half)
    traj_ref[0] = half


PLAN = (
    ("share", None),
    ("spread", (0, 0)),
    ("spread", (0, 1)),
    ("forward", None),
    ("land", (0, 0)),
    ("spread", (1, 1)),
    ("spread", (0, 2)),
    ("land", (0, 1)),
    ("spread", (1, 2)),
    ("gather", None),
    ("clear", None),
    ("land", (1, 1)),
    ("local", (2, 2)),
    ("land", (2, 2)),
    ("local", (3, 3)),
    ("land", (0, 2)),
    ("land", (1, 2)),
    ("norms", None),
    ("land", (3, 3)),
)


def local_heads(
    start_noise,
    position,
    time_table,
    time_index,
    sched_index,
    coef_keep,
    coef_noise,
    w_in,
    norm_gain,
    w_qkv,
    w_proj,
    w_final,
):
    S, F, H = (lax.axis_size(a) for a in ("step", "frame", "head"))
    R = w_qkv.shape[0]
    C, rows = start_noise.shape
    D = position.shape[1]
    N = rows * F
    PL = F * H
    HZ = w_qkv.shape[2] // (F * 2 * HDIM)
    B = HZ * HDIM
    QK = 2 * B
    V = HZ * C
    late = 2 * V + (QK + V) // 4
    n_spread = sum(act == "spread" for act, _ in PLAN)
    n_local = sum(act == "local" for act, _ in PLAN)
    n_evals = n_spread + n_local
    vmem = pl.BlockSpec(memory_space=pltpu.VMEM)
    smem = pl.BlockSpec(memory_space=pltpu.SMEM)
    here = pl.BlockSpec(memory_space=pl.ANY)
    traj, res = pl.pallas_call(
        functools.partial(kernel, S, F, H),
        out_shape=(pltpu.VMEM((1, C, rows), F32), pltpu.VMEM((1, ITERS), F32)),
        in_specs=[here, here, here, smem, smem] + [here] * 7,
        out_specs=(vmem, vmem),
        scratch_shapes=[
            pltpu.VMEM((rows, D), BF16),
            pltpu.VMEM(time_table.shape, BF16),
            pltpu.VMEM((1, coef_keep.shape[0]), F32),
            pltpu.VMEM((1, coef_noise.shape[0]), F32),
            pltpu.VMEM(w_in.shape, BF16),
            pltpu.VMEM((D,), F32),
            pltpu.VMEM((3, R, w_qkv.shape[2]), BF16),
            pltpu.VMEM(w_proj.shape, BF16),
            pltpu.VMEM(w_final.shape, BF16),
            pltpu.VMEM((2, QK + B, R), BF16),
            pltpu.VMEM((D, rows), BF16),
            pltpu.VMEM((R, rows), BF16),
            pltpu.VMEM((32, D), F32),
            pltpu.VMEM((32, R), BF16),
            pltpu.VMEM((2, B, N + 32), BF16),
            pltpu.VMEM((3, QK, rows), F32),
            pltpu.VMEM((3, QK, rows), BF16),
            pltpu.VMEM((3, QK, rows), BF16),
            pltpu.VMEM((3, QK, rows), BF16),
            pltpu.VMEM((3, QK, rows), BF16),
            pltpu.VMEM((S, C, 2 * B), BF16),
            pltpu.VMEM((F, C, rows), F32),
            pltpu.VMEM((S, 8, time_table.shape[0]), F32),
            pltpu.VMEM((F, 2 * C + 16, rows), F32),
            pltpu.VMEM((2 * F, F, QK, rows), BF16),
            pltpu.VMEM((2 * F, late, rows), BF16),
            pltpu.VMEM((2 * F + 1, QK + V, 32), BF16),
            pltpu.VMEM((2 * F + 1, QK + V, N), F32),
            pltpu.VMEM((S, 2 * C, N), F32),
            pltpu.VMEM((n_spread, 2 * PL, C, N), BF16),
            pltpu.VMEM((n_local, H, C, N), F32),
            pltpu.SemaphoreType.DMA((14 + 6 + n_evals - 8,)),
            pltpu.SemaphoreType.DMA((3 * 7 + 8 + n_evals,)),
        ],
        compiler_params=pltpu.CompilerParams(
            collective_id=0, has_side_effects=True, vmem_limit_bytes=60 * 1024 * 1024
        ),
    )(
        start_noise,
        position,
        time_table,
        time_index,
        sched_index,
        coef_keep[None],
        coef_noise[None],
        w_in,
        norm_gain,
        jnp.transpose(w_qkv, (1, 0, 2)),
        w_proj,
        w_final,
    )
    return traj, res.reshape(ITERS)


def one_head_each(mesh, start_noise, time_index, w_qkv, time_table):
    S, F, H = (mesh.shape[a] for a in ("step", "frame", "head"))
    return (
        S == ITERS
        and time_index.shape[0] == S
        and w_qkv.shape[2] == S * F * H * HDIM
        and w_qkv.shape[0] % (16 * S) == 0
        and start_noise.shape[1] % (128 * F) == 0
        and start_noise.shape[1] // F <= time_table.shape[0]
        and time_table.shape[0] % 128 == 0
    )


def solution(mesh):
    def call(*args):
        fits = one_head_each(mesh, args[0], args[3], args[9], args[2])
        return jax.shard_map(
            local_heads if fits else local_any,
            mesh=mesh,
            in_specs=(
                P("parts", "frame"),
                P("frame", None),
                P(),
                P("step"),
                P("step"),
                P(),
                P(),
                P(),
                P(),
                P("step", None, "head"),
                P("step", "head"),
                P(),
            ),
            out_specs=(P("step", "parts", "frame"), P("parts")),
            check_vma=False,
        )(*args)

    return call
```

```python
import functools
import math

import jax
import jax.numpy as jnp
from jax import lax
from jax.experimental import pallas as pl
from jax.experimental.pallas import tpu as pltpu
from jax.sharding import PartitionSpec as P

HDIM = 72
ITERS = 4


def entering(value, axis, combine, identity):
    count, here = (lax.axis_size(axis), lax.axis_index(axis))
    everything = lax.all_gather(value, axis)
    start = jnp.broadcast_to(jnp.asarray(identity, value.dtype), value.shape)

    def hop(k, before):
        reached = k < here
        new = combine(before, everything[k])
        return jnp.where(reached, new, before)

    return lax.fori_loop(0, count, hop, start)


def add_terms(first, second):
    return first + second


def local_any(
    start_noise,
    position,
    time_table,
    time_index,
    sched_index,
    coef_keep,
    coef_noise,
    w_in,
    norm_gain,
    w_qkv,
    w_proj,
    w_final,
):
    w_qkv_all, w_proj_all = (
        lax.all_gather(w_qkv, "step", axis=0, tiled=True),
        lax.all_gather(w_proj, "step", axis=0, tiled=True),
    )
    batch_steps = time_index.shape[0]
    row_count = start_noise.shape[1]
    table_rows = time_table.shape[0]
    pick_time = (time_index[:, None] == jnp.arange(table_rows)[None, :]).astype(jnp.bfloat16)
    time_embed = jnp.dot(pick_time, time_table, preferred_element_type=jnp.float32)
    pick_sched = (sched_index[:, None] == jnp.arange(table_rows)[None, :]).astype(jnp.float32)
    keep_rate = jnp.sum(pick_sched * coef_keep[None, :], axis=1)
    noise_rate = jnp.sum(pick_sched * coef_noise[None, :], axis=1)
    heads_local = w_qkv_all.shape[2] // HDIM
    cell_count = (
        batch_steps
        * lax.axis_size("step")
        * start_noise.shape[0]
        * row_count
        * lax.axis_size("frame")
    )
    states = start_noise[None]
    drift_term = jnp.zeros_like(states)
    residual_list = []
    for iteration in range(ITERS):
        latent_bf = states.astype(jnp.bfloat16)
        hidden = (
            jnp.einsum("bcr,cd->brd", latent_bf, w_in, preferred_element_type=jnp.float32)
            + position
            + time_embed[:, None, :]
        )
        normed = (
            hidden * lax.rsqrt(jnp.mean(hidden * hidden, axis=2, keepdims=True) + 1e-06) * norm_gain
        ).astype(jnp.bfloat16)
        projected = jnp.einsum(
            "brd,dkq->brkq", normed, w_qkv_all, preferred_element_type=jnp.float32
        ).astype(jnp.bfloat16)
        queries = projected[:, :, 0].reshape(batch_steps, row_count, heads_local, HDIM)
        score_scale = 1.0 / math.sqrt(HDIM)
        keys_values = projected[:, :, 1:3]
        piece = lax.all_gather(keys_values, "frame", axis=1, tiled=True)
        top_old = jnp.full((batch_steps, heads_local, row_count), -1e30, jnp.float32)
        piece_rows = piece.shape[1]
        keys_blk = piece[:, :, 0].reshape(batch_steps, piece_rows, heads_local, HDIM)
        values_blk = piece[:, :, 1].reshape(batch_steps, piece_rows, heads_local, HDIM)
        scores = (
            jnp.einsum("bqhe,bkhe->bhqk", queries, keys_blk, preferred_element_type=jnp.float32)
            * score_scale
        )
        top_new = jnp.maximum(top_old, jnp.max(scores, axis=3))
        weights_exp = jnp.exp(scores - top_new[:, :, :, None])
        total_new = jnp.sum(weights_exp, axis=3)
        update = jnp.einsum(
            "bhqk,bkhe->bqhe",
            weights_exp.astype(jnp.bfloat16),
            values_blk,
            preferred_element_type=jnp.float32,
        )
        accum = update
        top_final, total_final, accum = (top_new, total_new, accum)
        attended = accum / jnp.transpose(total_final, (0, 2, 1))[:, :, :, None]
        attn_mixed = attended.reshape(batch_steps, row_count, heads_local * HDIM).astype(
            jnp.bfloat16
        )
        partial_value = jnp.einsum(
            "brq,dq->brd", attn_mixed, w_proj_all, preferred_element_type=jnp.float32
        )
        head_total = lax.psum(partial_value, "head")
        joined = (hidden + head_total).astype(jnp.bfloat16)
        predicted = jnp.einsum("cd,brd->bcr", w_final, joined, preferred_element_type=jnp.float32)
        drift_term = keep_rate[:, None, None] * states + noise_rate[:, None, None] * predicted
        local_incl = jnp.cumsum(drift_term, axis=0)
        local_total = local_incl[-1]
        earlier = entering(local_total, "step", add_terms, jnp.zeros_like(local_total))
        before = earlier[None] + (local_incl - drift_term)
        new_states = start_noise[None] + before
        change = new_states - states
        square_sum = jnp.sum(change * change)
        summed = lax.psum(square_sum, ("step", "frame"))
        residual_list.append(jnp.sqrt(summed / cell_count + 1e-06))
        states = new_states
    residual_norms = jnp.stack(residual_list)
    trajectory = states + drift_term
    return (trajectory, residual_norms)


MESH = pl.DeviceIdType.MESH
F32 = jnp.float32
BF16 = jnp.bfloat16


def dot(a, b, ca=1, cb=0):
    return lax.dot_general(a, b, (((ca,), (cb,)), ((), ())), preferred_element_type=F32)


def dot_exact(a, b):
    return lax.dot_general(
        a, b, (((1,), (0,)), ((), ())), precision=lax.Precision.HIGHEST, preferred_element_type=F32
    )


def two(a):
    high = a.astype(BF16)
    return high, (a - high.astype(F32)).astype(BF16)


def kernel(
    S,
    F,
    H,
    noise_hbm,
    pos_hbm,
    table_hbm,
    tidx_ref,
    sidx_ref,
    keep_hbm,
    coef_hbm,
    win_hbm,
    gain_hbm,
    wqkv_hbm,
    wproj_hbm,
    wfin_hbm,
    traj_ref,
    res_ref,
    pos_ref,
    table_ref,
    keep_ref,
    coef_ref,
    win_ref,
    gain_ref,
    wqkv_ref,
    wproj_ref,
    wfin_ref,
    wt_ref,
    at_ref,
    at_peer,
    side_ref,
    side_cut,
    pv_ref,
    own_ref,
    near_send,
    near_recv,
    far_send,
    far_recv,
    mix_buf,
    noise_buf,
    meta_buf,
    ends_buf,
    fin_qk,
    fin_late,
    big_buf,
    tab_buf,
    base_buf,
    plane_buf,
    chip_buf,
    ssem,
    rsem,
):
    s, f, h = (lax.axis_index(a) for a in ("step", "frame", "head"))
    loads = [
        pltpu.make_async_copy(src, dst, ssem.at[n])
        for n, (src, dst) in enumerate(
            (
                (keep_hbm, keep_ref),
                (coef_hbm, coef_ref),
                (gain_hbm, gain_ref),
                (pos_hbm, pos_ref),
                (wqkv_hbm.at[0], wqkv_ref.at[0]),
                (wqkv_hbm.at[1], wqkv_ref.at[1]),
                (wqkv_hbm.at[2], wqkv_ref.at[2]),
                (wfin_hbm, wfin_ref),
                (wproj_hbm, wproj_ref),
                (noise_hbm, noise_buf.at[f]),
                (table_hbm, table_ref),
                (win_hbm, win_ref),
            )
        )
    ]
    for copy in loads:
        copy.start()
    PL = F * H
    q_me = f * H + h
    C, rows = noise_buf.shape[1:]
    D = pos_ref.shape[1]
    N = rows * F
    R = wqkv_ref.shape[1]
    lanes = table_ref.shape[0]
    e = lax.rem(s, 2)
    e_near = 1 - e
    s_near = s + 1 - 2 * e
    s_far = lax.rem(s + 2, S)
    HZ = wqkv_ref.shape[2] // (F * 2 * HDIM)
    B = HZ * HDIM
    QK = 2 * B
    V = HZ * C

    def step_peer(d):
        return {"step": lax.rem(s + d, S)}

    def group_peer(d):
        dz, df, dh = d // PL, d % PL // H, d % H
        return {
            "step": s_near if dz else s,
            "frame": lax.rem(f + df, F),
            "head": lax.rem(h + dh, H),
        }

    frame_peer = {"frame": 1 - f}

    barrier = pltpu.get_barrier_semaphore()
    for d in range(1, PL):
        pl.semaphore_signal(barrier, inc=1, device_id=group_peer(d), device_id_type=MESH)
    for d in range(1, S):
        pl.semaphore_signal(barrier, inc=1, device_id=step_peer(d), device_id_type=MESH)

    reused = ("across", "share", "pass", "late", "pass late", "ends")
    fresh = ("near", "far", "turn", "meta", "mix", "noise")
    outs = {name: n for n, name in enumerate(reused)}
    outs.update((name, len(loads) + n) for n, name in enumerate(fresh))
    spare = list(range(len(reused), len(loads)))
    spare += list(range(len(loads) + len(fresh), ssem.shape[0]))
    ins = {}

    def prepare(src, dst, peer, out, into):
        return pltpu.make_async_remote_copy(
            src_ref=src,
            dst_ref=dst,
            send_sem=ssem.at[outs[out]],
            recv_sem=rsem.at[ins.setdefault(into, len(ins))],
            device_id=peer,
            device_id_type=MESH,
        )

    def send(src, dst, peer, out, into):
        copy = prepare(src, dst, peer, out, into)
        copy.start()
        return copy

    def settle(ref, sem):
        pltpu.make_async_copy(ref, ref, sem).wait()

    def arrive(ref, into):
        settle(ref, rsem.at[ins[into]])

    for copy in loads[:3]:
        copy.wait()
    row_id = lax.broadcasted_iota(jnp.int32, (8, lanes), 0)
    lane_id = lax.broadcasted_iota(jnp.int32, (1, lanes), 1)
    hot_t = jnp.where(lane_id == tidx_ref[0], 1.0, 0.0)
    hot_s = lane_id == sidx_ref[0]
    keep = jnp.sum(jnp.where(hot_s, keep_ref[...], 0.0), axis=1, keepdims=True)
    coef = jnp.sum(jnp.where(hot_s, coef_ref[...], 0.0), axis=1, keepdims=True)
    meta_buf[s] = jnp.where(row_id == 0, hot_t, jnp.where(row_id == 1, keep, coef))
    loads[3].wait()
    gain = gain_ref[...].reshape(1, D)
    pos = pos_ref[...]
    at_ref[...] = jnp.transpose(pos.astype(F32) * gain).astype(BF16)

    def turn_weights(parts):
        for i in range(F):

            @pl.when(f == i)
            def _():
                for p in parts:
                    turned = jnp.transpose(wqkv_ref[p, :, i * 2 * B : (i + 1) * 2 * B])
                    for t in range(2):
                        wt_ref[t, p * B : (p + 1) * B] = turned[t * B : (t + 1) * B]

    for p in range(2):
        loads[4 + p].wait()
    turn_weights((0, 1))
    mine = pl.ds(pl.multiple_of(s * R, R), R)
    at_mine = at_ref[mine]
    near_send[0] = dot(wt_ref[e_near, 0:QK], at_mine).astype(BF16)
    pl.semaphore_wait(barrier, S - 1 + PL - 1)
    to_near, to_far = {"step": s_near}, {"step": s_far}
    near, far = {}, {}

    def send_near(i, low, high):
        window = pl.ds(low, high - low)
        near[i, low] = send(
            near_send.at[i, window],
            near_recv.at[i, window],
            to_near,
            "late" if i == 2 else "near",
            ("near", i, low),
        )

    pieces = [(low, low + QK // 3) for low in range(0, QK, QK // 3)]
    order = sorted(range(1, S), key=lambda d: abs(d - S / 2))
    for d in order:
        send(meta_buf.at[s], meta_buf.at[s], step_peer(d), "meta", "meta")
    send_near(0, *pieces[0])
    turn = send(at_ref.at[mine], at_peer, frame_peer, "turn", "turn")
    for piece in pieces[1:]:
        send_near(0, *piece)
    for copy in loads[7:9]:
        copy.wait()
    rows_of = wfin_ref[:, 0:R].astype(F32)
    for j in range(1, S):
        rows_of = jnp.where(s == j, wfin_ref[:, j * R : (j + 1) * R].astype(F32), rows_of)
    folded = dot(rows_of.astype(BF16), wproj_ref[...])
    picked = folded[:, 0 : 2 * B]
    for i in range(1, F):
        picked = jnp.where(f == i, folded[:, i * 2 * B : (i + 1) * 2 * B], picked)
    mix_buf[s] = picked.astype(BF16)
    for d in order:
        send(mix_buf.at[s], mix_buf.at[s], step_peer(d), "mix", "mix")
    loads[9].wait()
    sides = [send(noise_buf.at[f], noise_buf.at[f], frame_peer, "noise", "noise")]
    own_ref[0] = dot(wt_ref[e, 0:QK], at_mine)
    loads[6].wait()
    turn_weights((2,))

    def pass_on(i, low, high):
        near[i, low].wait_recv()
        total = own_ref[i, low:high] + near_recv[i, low:high].astype(F32)
        far_send[i, low:high] = total.astype(BF16)
        window = pl.ds(low, high - low)
        far[i, low] = send(
            far_send.at[i, window],
            far_recv.at[i, window],
            to_far,
            "late" if i == 2 else "far",
            ("far", i, low),
        )

    pv_ref[0, :, 0:rows] = dot(wt_ref[e, QK : QK + B], at_mine).astype(BF16)
    pv_ref[1, :, 0:rows] = dot(wt_ref[e_near, QK : QK + B], at_mine).astype(BF16)
    for copy in loads[10:]:
        copy.wait()
    w_in = win_ref[...]
    ends = jnp.concatenate([w_in, wfin_ref[...]], axis=0)
    ends_in = dot(ends, w_in, 1, 1)
    posf = pos.astype(F32)
    sq_hi, sq_lo = two(posf * posf)
    ones = jnp.ones((8, D), BF16)
    ends_buf[f, 0 : 2 * C] = dot(ends, pos, 1, 1)
    ends_buf[f, 2 * C : 2 * C + 8] = dot(ones, sq_hi, 1, 1) + dot(ones, sq_lo, 1, 1)

    for piece in pieces:
        pass_on(0, *piece)
    turn.wait_recv()
    at_other = at_peer[...]
    near_send[1] = dot(wt_ref[e_near, 0:QK], at_other).astype(BF16)
    for piece in pieces:
        send_near(1, *piece)
    own_ref[1] = dot(wt_ref[e, 0:QK], at_other)
    pv_ref[0, :, rows : 2 * rows] = dot(wt_ref[e, QK : QK + B], at_other).astype(BF16)
    pv_ref[1, :, rows : 2 * rows] = dot(wt_ref[e_near, QK : QK + B], at_other).astype(BF16)

    side_ref[0:C] = w_in.astype(F32)
    arrive(meta_buf.at[pl.ds(0, S - 1)], "meta")
    metas = [meta_buf[j] for j in range(S)]
    hot = jnp.concatenate(
        [m[0:1] for m in metas] + [jnp.zeros((8 - S, lanes), F32)], axis=0
    ).astype(BF16)
    keeps = [jnp.concatenate([m[1:2, :rows]] * F, axis=1) for m in metas]
    coefs = [jnp.concatenate([m[2:3, :rows]] * F, axis=1) for m in metas]
    temb = dot(hot, table_ref[...])
    side_ref[C : C + 8] = temb
    side_ref[C + 8 :] = jnp.zeros((32 - C - 8, D), F32)
    for j in range(S):

        @pl.when(s == j)
        def _():
            cut = slice(j * R, (j + 1) * R)
            side_cut[...] = (side_ref[:, cut] * gain[:, cut]).astype(BF16)

    side_mine = side_cut[...]
    turned_of = []
    for role, member in ((0, e), (1, e_near)):
        turned = dot(wt_ref[member], side_mine, 1, 1)
        pv_ref[role, :, 2 * rows : 2 * rows + 32] = turned[QK:].astype(BF16)
        turned_of.append(turned[0:QK])
    arrive(mix_buf.at[pl.ds(0, S - 1)], "mix")
    mix = mix_buf[0].astype(F32)
    for j in range(1, S):
        mix = mix + mix_buf[j].astype(F32)
    mix_lane = lax.broadcasted_iota(jnp.int32, (V, B), 1) // HDIM
    mix_row = lax.broadcasted_iota(jnp.int32, (V, B), 0) // C

    def late_rows(role, member):
        part = jnp.where(member == 0, mix[:, 0:B], mix[:, B : 2 * B])
        block = jnp.where(
            mix_lane == mix_row, jnp.concatenate([part] * HZ, axis=0), 0.0
        )
        block_hi, block_lo = two(block)
        values = dot(jnp.concatenate([block_hi, block_lo], axis=0), pv_ref[role])
        values = values[0:V] + values[V : 2 * V]
        packs = []
        for arr in (turned_of[role], values[:, 2 * rows : 2 * rows + 32]):
            size = arr.shape[0] // 4
            packs.append(
                jnp.concatenate([arr[g * size : (g + 1) * size] for g in range(4)], axis=1)
            )
        return jnp.concatenate(
            [values[:, 0:rows], values[:, rows : 2 * rows]] + packs, axis=0
        )

    LATE = 2 * V + (QK + V) // 4
    near_send[2, 0:LATE] = late_rows(1, e_near).astype(BF16)
    send_near(2, 0, LATE)
    own_ref[2, 0:LATE] = late_rows(0, e)
    temb_b = temb.astype(BF16)
    ends_buf[f, 2 * C + 8 : 2 * C + 16] = dot(temb_b, pos, 1, 1)
    sides.append(send(ends_buf.at[f], ends_buf.at[f], frame_peer, "ends", "ends"))
    ends_t = dot(ends, temb_b, 1, 1)
    norm_t = jnp.sum(temb * temb, axis=1, keepdims=True)
    for piece in pieces:
        pass_on(1, *piece)

    scale = 1.4426950408889634 / math.sqrt(HDIM)
    qk_row = lax.broadcasted_iota(jnp.int32, (QK, 1), 0)
    row_scale = jnp.where(qk_row < B, scale, 1.0)
    set_own, set_near = 2 * f + e, 2 * f + e_near
    halves = (f, 1 - f)

    def whole(i, low, high):
        far[i, low].wait_recv()
        total = far_send[i, low:high].astype(F32) + far_recv[i, low:high].astype(F32)
        return total.astype(BF16)

    def finish(i, low, high):
        total = whole(i, low, high)
        window = pl.ds(low, high - low)
        if i < 2:
            fin_qk[set_own, halves[i], low:high] = total
            ref = fin_qk.at[set_own, halves[i], window]
            twin = fin_qk.at[set_near, halves[i], window]
        else:
            fin_late[set_own] = total
            ref = fin_late.at[set_own]
            twin = fin_late.at[set_near]
        return ref, twin

    shared = []

    def hand_on(refs, kind):
        send(refs[0], refs[0], frame_peer, kind or "across", kind and "late" or "across")

    def share(refs, kind):
        copy = send(refs[0], refs[0], to_near, kind or "share", ("share", len(shared)))
        shared.append((copy, refs[1], kind))

    def offer(refs, kind=None):
        hand_on(refs, kind)
        share(refs, kind)

    def forward(_):
        for copy, twin, kind in shared:
            copy.wait_recv()
            send(
                twin,
                twin,
                frame_peer,
                "pass late" if kind else "pass",
                "late" if kind else "pass",
            )

    ready = [finish(0, *piece) for piece in pieces]
    pass_on(2, 0, LATE)
    for refs in ready:
        offer(refs)
    for copy in sides:
        copy.wait_recv()
    start = jnp.concatenate([noise_buf[i] for i in range(F)], axis=1)
    ends_all = jnp.concatenate([ends_buf[i] for i in range(F)], axis=1)
    ends_pos = ends_all[0 : 2 * C]
    norm_p = ends_all[2 * C : 2 * C + 1]
    cross = ends_all[2 * C + 8 : 2 * C + 16]
    norms = [norm_p + 2.0 * cross[j : j + 1] + norm_t[j : j + 1] for j in range(S)]
    for j in range(S):
        base_buf[j] = jnp.concatenate(
            [
                2.0 * (ends_pos[0:C] + ends_t[0:C, j : j + 1]),
                ends_pos[C : 2 * C] + ends_t[C : 2 * C, j : j + 1],
            ],
            axis=0,
        )
    ends_hi, ends_lo = two(
        jnp.concatenate([ends_in, jnp.zeros((2 * C, 32 - C), F32)], axis=1)
    )
    ends_big = jnp.concatenate([ends_hi, ends_lo], axis=0)
    size = QK // 4

    def build(slot, group, frame):
        last = fin_late[group].astype(F32)
        one, other = last[0:V], last[V : 2 * V]
        packed = last[2 * V : LATE]
        big_qk = jnp.concatenate(
            [packed[0:size, 32 * g : 32 * g + 32] for g in range(4)], axis=0
        )
        big_v = jnp.concatenate(
            [packed[size:, 32 * g : 32 * g + 32] for g in range(4)], axis=0
        )
        big_buf[slot, 0:QK] = (big_qk * row_scale).astype(BF16)
        big_buf[slot, QK:] = big_v.astype(BF16)
        for i in range(F):
            cut = slice(i * rows, (i + 1) * rows)
            tab_buf[slot, 0:QK, cut] = fin_qk[group, i].astype(F32) * row_scale
            tab_buf[slot, QK:, cut] = jnp.where(frame == i, one, other)

    ready = [finish(1, *piece) for piece in pieces]
    for refs in ready:
        offer(refs)
    ready = finish(2, 0, LATE)
    build(4, set_own, f)

    def share_rest(_):
        offer(ready, "late")

    hot_row = lax.broadcasted_iota(jnp.int32, (32 - C, N), 0)
    ones_rows = jnp.ones((C, N), BF16)

    def evaluate(x, j, slots):
        xb = x.astype(BF16)
        pick = jnp.where(hot_row == j, 1.0, 0.0).astype(BF16)
        x_in = jnp.concatenate([xb, pick], axis=0)
        base = base_buf[j]
        out = jnp.zeros((C, N), F32)
        items, scores, r, eps = {}, {}, None, None
        G = len(slots)
        for g in range(G + 2):
            if g < G:
                big = big_buf[slots[g]]
                if g == 0:
                    lin = dot(jnp.concatenate([ends_big, big], axis=0), x_in)
                    tail = lin[0 : 2 * C] + lin[2 * C : 4 * C]
                    lin = lin[4 * C :]
                    square = jnp.sum(
                        xb.astype(F32) * (tail[0:C] + base[0:C]), axis=0, keepdims=True
                    )
                    square = jnp.maximum(square + norms[j], 0.0)
                    r = lax.rsqrt(square * (1.0 / D) + 1e-06)
                    eps = tail[C : 2 * C] + base[C : 2 * C]
                else:
                    lin = dot(big, x_in)
                lin = (lin + tab_buf[slots[g]]) * r
                for n in range(HZ):
                    q = lin[n * HDIM : (n + 1) * HDIM].astype(BF16)
                    k = lin[B + n * HDIM : B + (n + 1) * HDIM].astype(BF16)
                    v_hi, v_lo = two(lin[QK + n * C : QK + (n + 1) * C])
                    items[g, n] = q, k, jnp.concatenate([v_hi, v_lo, ones_rows], axis=0)
            if 0 <= g - 1 < G:
                for n in range(HZ):
                    q, k, _ = items[g - 1, n]
                    scores[g - 1, n] = dot(k, q, 0, 0)
            if 0 <= g - 2 < G:
                for n in range(HZ):
                    block = scores.pop((g - 2, n))
                    top = jnp.max(block, axis=0, keepdims=True)
                    p = jnp.exp2(block - top).astype(BF16)
                    o = dot(items[g - 2, n][2], p)
                    out = out + (o[0:C] + o[C : 2 * C]) / o[2 * C : 2 * C + 1]
        return out, eps

    spread = [key for act, key in PLAN if act == "spread"]
    local = [key for act, key in PLAN if act == "local"]
    state, local_eps, drift, flying = {}, {}, {}, {}
    rounds_at = rsem.shape[0] - len(spread) - len(local)
    outward = sorted(
        range(1, 2 * PL), key=lambda d: (-(d // PL + (d % PL // H > 0)), -(d // PL))
    )

    def launch(key, slots):
        i, j = key
        x = start
        for m in range(j if i else 0):
            x = x + drift[(min(i - 1, m), m)]
        state[key] = x
        part, local_eps[key] = evaluate(x, j, slots)
        k = flying[key] = len(flying)
        if key in spread:
            slot = plane_buf.at[spread.index(key), e * PL + q_me]
            slot[...] = part.astype(BF16)
            peers = [group_peer(d) for d in outward]
        else:
            slot = chip_buf.at[local.index(key), h]
            slot[...] = part
            peers = [{"head": 1 - h}]
        for peer in peers:
            pltpu.make_async_remote_copy(
                src_ref=slot,
                dst_ref=slot,
                send_sem=ssem.at[spare[k]],
                recv_sem=rsem.at[rounds_at + k],
                device_id=peer,
                device_id_type=MESH,
            ).start()

    def land(key):
        j, k = key[1], flying[key]
        if key in spread:
            others = plane_buf.at[spread.index(key), pl.ds(0, 2 * PL - 1)]
        else:
            others = chip_buf.at[local.index(key), 0]
        settle(others, rsem.at[rounds_at + k])
        total = local_eps[key]
        if key in spread:
            for i in range(2 * PL):
                total = total + plane_buf[spread.index(key), i].astype(F32)
        else:
            for i in range(H):
                total = total + chip_buf[local.index(key), i]
        drift[key] = keeps[j] * state[key] + coefs[j] * total
        settle(others, ssem.at[spare[k]])

    def clear(_):
        for out, ref in (
            ("near", near_send.at[pl.ds(0, 2)]),
            ("far", far_send.at[pl.ds(0, 2)]),
            ("across", fin_qk.at[0]),
            ("share", fin_qk.at[0]),
            ("pass", fin_qk.at[0]),
            ("late", fin_late),
            ("pass late", fin_late.at[0]),
            ("turn", at_peer),
            ("meta", meta_buf.at[pl.ds(0, S - 1)]),
            ("mix", mix_buf.at[pl.ds(0, S - 1)]),
            ("noise", noise_buf.at[0]),
            ("ends", ends_buf.at[0]),
        ):
            settle(ref, ssem.at[outs[out]])

    def gather(_):
        build(set_own, set_own, f)
        build(set_near, set_near, f)
        arrive(fin_qk.at[0], "across")
        arrive(fin_qk.at[0], "pass")
        arrive(fin_late.at[pl.ds(0, 2)], "late")
        for member in (e, e_near):
            twin = 2 * (1 - f) + member
            build(twin, twin, 1 - f)

    def norms_now(_):
        lane = lax.broadcasted_iota(jnp.int32, res_ref.shape, 1)
        res = jnp.zeros(res_ref.shape, F32)
        old = [start] * S
        for it in range(ITERS):
            new, run = [], start
            for j in range(S):
                new.append(run)
                if j < S - 1:
                    run = run + drift[(min(it, j), j)]
            square = jnp.zeros((C, N), F32)
            for j in range(1, S):
                change = new[j] - old[j]
                square = square + change * change
            square = jnp.sum(
                jnp.sum(square, axis=0, keepdims=True), axis=1, keepdims=True
            )
            res = jnp.where(lane == it, jnp.sqrt(square / (S * C * N) + 1e-06), res)
            old = new
        res_ref[...] = res

    acts = {
        "clear": clear,
        "share": share_rest,
        "forward": forward,
        "gather": gather,
        "land": land,
        "norms": norms_now,
        "spread": lambda key: launch(key, [2 * F]),
        "local": lambda key: launch(key, list(range(2 * F))),
    }
    for act, key in PLAN:
        acts[act](key)
    final = jnp.zeros((C, N), F32)
    for j in range(S):
        final = jnp.where(s == j, state[(j, j)] + drift[(j, j)], final)
    half = final[:, 0:rows]
    for i in range(1, F):
        half = jnp.where(f == i, final[:, i * rows : (i + 1) * rows], half)
    traj_ref[0] = half


PLAN = (
    ("share", None),
    ("spread", (0, 0)),
    ("spread", (0, 1)),
    ("forward", None),
    ("land", (0, 0)),
    ("spread", (1, 1)),
    ("spread", (0, 2)),
    ("land", (0, 1)),
    ("spread", (1, 2)),
    ("gather", None),
    ("clear", None),
    ("land", (1, 1)),
    ("local", (2, 2)),
    ("land", (2, 2)),
    ("local", (3, 3)),
    ("land", (0, 2)),
    ("land", (1, 2)),
    ("norms", None),
    ("land", (3, 3)),
)


def local_heads(
    start_noise,
    position,
    time_table,
    time_index,
    sched_index,
    coef_keep,
    coef_noise,
    w_in,
    norm_gain,
    w_qkv,
    w_proj,
    w_final,
):
    S, F, H = (lax.axis_size(a) for a in ("step", "frame", "head"))
    R = w_qkv.shape[0]
    C, rows = start_noise.shape
    D = position.shape[1]
    N = rows * F
    PL = F * H
    HZ = w_qkv.shape[2] // (F * 2 * HDIM)
    B = HZ * HDIM
    QK = 2 * B
    V = HZ * C
    late = 2 * V + (QK + V) // 4
    n_spread = sum(act == "spread" for act, _ in PLAN)
    n_local = sum(act == "local" for act, _ in PLAN)
    n_evals = n_spread + n_local
    vmem = pl.BlockSpec(memory_space=pltpu.VMEM)
    smem = pl.BlockSpec(memory_space=pltpu.SMEM)
    here = pl.BlockSpec(memory_space=pl.ANY)
    traj, res = pl.pallas_call(
        functools.partial(kernel, S, F, H),
        out_shape=(pltpu.VMEM((1, C, rows), F32), pltpu.VMEM((1, ITERS), F32)),
        in_specs=[here, here, here, smem, smem] + [here] * 7,
        out_specs=(vmem, vmem),
        scratch_shapes=[
            pltpu.VMEM((rows, D), BF16),
            pltpu.VMEM(time_table.shape, BF16),
            pltpu.VMEM((1, coef_keep.shape[0]), F32),
            pltpu.VMEM((1, coef_noise.shape[0]), F32),
            pltpu.VMEM(w_in.shape, BF16),
            pltpu.VMEM((D,), F32),
            pltpu.VMEM((3, R, w_qkv.shape[2]), BF16),
            pltpu.VMEM(w_proj.shape, BF16),
            pltpu.VMEM(w_final.shape, BF16),
            pltpu.VMEM((2, QK + B, R), BF16),
            pltpu.VMEM((D, rows), BF16),
            pltpu.VMEM((R, rows), BF16),
            pltpu.VMEM((32, D), F32),
            pltpu.VMEM((32, R), BF16),
            pltpu.VMEM((2, B, N + 32), BF16),
            pltpu.VMEM((3, QK, rows), F32),
            pltpu.VMEM((3, QK, rows), BF16),
            pltpu.VMEM((3, QK, rows), BF16),
            pltpu.VMEM((3, QK, rows), BF16),
            pltpu.VMEM((3, QK, rows), BF16),
            pltpu.VMEM((S, C, 2 * B), BF16),
            pltpu.VMEM((F, C, rows), F32),
            pltpu.VMEM((S, 8, time_table.shape[0]), F32),
            pltpu.VMEM((F, 2 * C + 16, rows), F32),
            pltpu.VMEM((2 * F, F, QK, rows), BF16),
            pltpu.VMEM((2 * F, late, rows), BF16),
            pltpu.VMEM((2 * F + 1, QK + V, 32), BF16),
            pltpu.VMEM((2 * F + 1, QK + V, N), F32),
            pltpu.VMEM((S, 2 * C, N), F32),
            pltpu.VMEM((n_spread, 2 * PL, C, N), BF16),
            pltpu.VMEM((n_local, H, C, N), F32),
            pltpu.SemaphoreType.DMA((14 + 6 + n_evals - 8,)),
            pltpu.SemaphoreType.DMA((3 * 7 + 8 + n_evals,)),
        ],
        compiler_params=pltpu.CompilerParams(
            collective_id=0, has_side_effects=True, vmem_limit_bytes=60 * 1024 * 1024
        ),
    )(
        start_noise,
        position,
        time_table,
        time_index,
        sched_index,
        coef_keep[None],
        coef_noise[None],
        w_in,
        norm_gain,
        jnp.transpose(w_qkv, (1, 0, 2)),
        w_proj,
        w_final,
    )
    return traj, res.reshape(ITERS)


def one_head_each(mesh, start_noise, time_index, w_qkv, time_table):
    S, F, H = (mesh.shape[a] for a in ("step", "frame", "head"))
    return (
        S == ITERS
        and time_index.shape[0] == S
        and w_qkv.shape[2] == S * F * H * HDIM
        and w_qkv.shape[0] % (16 * S) == 0
        and F == 2
        and H == 2
        and start_noise.shape[1] == 128 * F
        and start_noise.shape[0] == 16 * mesh.shape["parts"]
        and start_noise.shape[1] // F <= time_table.shape[0]
        and time_table.shape[0] % 128 == 0
    )


def solution(mesh):
    def call(*args):
        fits = one_head_each(mesh, args[0], args[3], args[9], args[2])
        return jax.shard_map(
            local_heads if fits else local_any,
            mesh=mesh,
            in_specs=(
                P("parts", "frame"),
                P("frame", None),
                P(),
                P("step"),
                P("step"),
                P(),
                P(),
                P(),
                P(),
                P("step", None, "head"),
                P("step", "head"),
                P(),
            ),
            out_specs=(P("step", "parts", "frame"), P("parts")),
            check_vma=False,
        )(*args)

    return call
```

```python
import functools
import math

import jax
import jax.numpy as jnp
from jax import lax
from jax.experimental import pallas as pl
from jax.experimental.pallas import tpu as pltpu
from jax.sharding import PartitionSpec as P

HDIM = 72
ITERS = 4


def entering(value, axis, combine, identity):
    count, here = (lax.axis_size(axis), lax.axis_index(axis))
    everything = lax.all_gather(value, axis)
    start = jnp.broadcast_to(jnp.asarray(identity, value.dtype), value.shape)

    def hop(k, before):
        reached = k < here
        new = combine(before, everything[k])
        return jnp.where(reached, new, before)

    return lax.fori_loop(0, count, hop, start)


def add_terms(first, second):
    return first + second


def local_any(
    start_noise,
    position,
    time_table,
    time_index,
    sched_index,
    coef_keep,
    coef_noise,
    w_in,
    norm_gain,
    w_qkv,
    w_proj,
    w_final,
):
    w_qkv_all, w_proj_all = (
        lax.all_gather(w_qkv, "step", axis=0, tiled=True),
        lax.all_gather(w_proj, "step", axis=0, tiled=True),
    )
    batch_steps = time_index.shape[0]
    row_count = start_noise.shape[1]
    table_rows = time_table.shape[0]
    pick_time = (time_index[:, None] == jnp.arange(table_rows)[None, :]).astype(jnp.bfloat16)
    time_embed = jnp.dot(pick_time, time_table, preferred_element_type=jnp.float32)
    pick_sched = (sched_index[:, None] == jnp.arange(table_rows)[None, :]).astype(jnp.float32)
    keep_rate = jnp.sum(pick_sched * coef_keep[None, :], axis=1)
    noise_rate = jnp.sum(pick_sched * coef_noise[None, :], axis=1)
    heads_local = w_qkv_all.shape[2] // HDIM
    cell_count = (
        batch_steps
        * lax.axis_size("step")
        * start_noise.shape[0]
        * row_count
        * lax.axis_size("frame")
    )
    states = start_noise[None]
    drift_term = jnp.zeros_like(states)
    residual_list = []
    for iteration in range(ITERS):
        latent_bf = states.astype(jnp.bfloat16)
        hidden = (
            jnp.einsum("bcr,cd->brd", latent_bf, w_in, preferred_element_type=jnp.float32)
            + position
            + time_embed[:, None, :]
        )
        normed = (
            hidden * lax.rsqrt(jnp.mean(hidden * hidden, axis=2, keepdims=True) + 1e-06) * norm_gain
        ).astype(jnp.bfloat16)
        projected = jnp.einsum(
            "brd,dkq->brkq", normed, w_qkv_all, preferred_element_type=jnp.float32
        ).astype(jnp.bfloat16)
        queries = projected[:, :, 0].reshape(batch_steps, row_count, heads_local, HDIM)
        score_scale = 1.0 / math.sqrt(HDIM)
        keys_values = projected[:, :, 1:3]
        piece = lax.all_gather(keys_values, "frame", axis=1, tiled=True)
        top_old = jnp.full((batch_steps, heads_local, row_count), -1e30, jnp.float32)
        piece_rows = piece.shape[1]
        keys_blk = piece[:, :, 0].reshape(batch_steps, piece_rows, heads_local, HDIM)
        values_blk = piece[:, :, 1].reshape(batch_steps, piece_rows, heads_local, HDIM)
        scores = (
            jnp.einsum("bqhe,bkhe->bhqk", queries, keys_blk, preferred_element_type=jnp.float32)
            * score_scale
        )
        top_new = jnp.maximum(top_old, jnp.max(scores, axis=3))
        weights_exp = jnp.exp(scores - top_new[:, :, :, None])
        total_new = jnp.sum(weights_exp, axis=3)
        update = jnp.einsum(
            "bhqk,bkhe->bqhe",
            weights_exp.astype(jnp.bfloat16),
            values_blk,
            preferred_element_type=jnp.float32,
        )
        accum = update
        top_final, total_final, accum = (top_new, total_new, accum)
        attended = accum / jnp.transpose(total_final, (0, 2, 1))[:, :, :, None]
        attn_mixed = attended.reshape(batch_steps, row_count, heads_local * HDIM).astype(
            jnp.bfloat16
        )
        partial_value = jnp.einsum(
            "brq,dq->brd", attn_mixed, w_proj_all, preferred_element_type=jnp.float32
        )
        head_total = lax.psum(partial_value, "head")
        joined = (hidden + head_total).astype(jnp.bfloat16)
        predicted = jnp.einsum("cd,brd->bcr", w_final, joined, preferred_element_type=jnp.float32)
        drift_term = keep_rate[:, None, None] * states + noise_rate[:, None, None] * predicted
        local_incl = jnp.cumsum(drift_term, axis=0)
        local_total = local_incl[-1]
        earlier = entering(local_total, "step", add_terms, jnp.zeros_like(local_total))
        before = earlier[None] + (local_incl - drift_term)
        new_states = start_noise[None] + before
        change = new_states - states
        square_sum = jnp.sum(change * change)
        summed = lax.psum(square_sum, ("step", "frame"))
        residual_list.append(jnp.sqrt(summed / cell_count + 1e-06))
        states = new_states
    residual_norms = jnp.stack(residual_list)
    trajectory = states + drift_term
    return (trajectory, residual_norms)


MESH = pl.DeviceIdType.MESH
F32 = jnp.float32
BF16 = jnp.bfloat16


def dot(a, b, ca=1, cb=0):
    return lax.dot_general(a, b, (((ca,), (cb,)), ((), ())), preferred_element_type=F32)


def dot_exact(a, b):
    return lax.dot_general(
        a, b, (((1,), (0,)), ((), ())), precision=lax.Precision.HIGHEST, preferred_element_type=F32
    )


def two(a):
    high = a.astype(BF16)
    return high, (a - high.astype(F32)).astype(BF16)


def kernel(
    S,
    F,
    H,
    noise_hbm,
    pos_hbm,
    table_hbm,
    tidx_ref,
    sidx_ref,
    keep_hbm,
    coef_hbm,
    win_hbm,
    gain_hbm,
    wqkv_hbm,
    wproj_hbm,
    wfin_hbm,
    traj_ref,
    res_ref,
    pos_ref,
    table_ref,
    keep_ref,
    coef_ref,
    win_ref,
    gain_ref,
    wqkv_ref,
    wproj_ref,
    wfin_ref,
    wt_ref,
    at_ref,
    at_peer,
    side_ref,
    side_cut,
    pv_ref,
    own_ref,
    near_send,
    near_recv,
    far_send,
    far_recv,
    mix_buf,
    noise_buf,
    meta_buf,
    ends_buf,
    fin_qk,
    fin_late,
    big_buf,
    tab_buf,
    base_buf,
    plane_buf,
    chip_buf,
    ssem,
    rsem,
):
    s, f, h = (lax.axis_index(a) for a in ("step", "frame", "head"))
    loads = [
        pltpu.make_async_copy(src, dst, ssem.at[n])
        for n, (src, dst) in enumerate(
            (
                (keep_hbm, keep_ref),
                (coef_hbm, coef_ref),
                (gain_hbm, gain_ref),
                (pos_hbm, pos_ref),
                (wqkv_hbm.at[0], wqkv_ref.at[0]),
                (wqkv_hbm.at[1], wqkv_ref.at[1]),
                (wqkv_hbm.at[2], wqkv_ref.at[2]),
                (wfin_hbm, wfin_ref),
                (wproj_hbm, wproj_ref),
                (noise_hbm, noise_buf.at[f]),
                (table_hbm, table_ref),
                (win_hbm, win_ref),
            )
        )
    ]
    for copy in loads:
        copy.start()
    PL = F * H
    q_me = f * H + h
    C, rows = noise_buf.shape[1:]
    D = pos_ref.shape[1]
    N = rows * F
    R = wqkv_ref.shape[1]
    lanes = table_ref.shape[0]
    e = lax.rem(s, 2)
    e_near = 1 - e
    s_near = s + 1 - 2 * e
    s_far = lax.rem(s + 2, S)
    HZ = wqkv_ref.shape[2] // (F * 2 * HDIM)
    B = HZ * HDIM
    QK = 2 * B
    V = HZ * C

    def step_peer(d):
        return {"step": lax.rem(s + d, S)}

    def group_peer(d):
        dz, df, dh = d // PL, d % PL // H, d % H
        return {
            "step": s_near if dz else s,
            "frame": lax.rem(f + df, F),
            "head": lax.rem(h + dh, H),
        }

    frame_peer = {"frame": 1 - f}

    barrier = pltpu.get_barrier_semaphore()
    for d in range(1, PL):
        pl.semaphore_signal(barrier, inc=1, device_id=group_peer(d), device_id_type=MESH)
    for d in range(1, S):
        pl.semaphore_signal(barrier, inc=1, device_id=step_peer(d), device_id_type=MESH)

    reused = ("across", "share", "pass", "late", "pass late", "ends")
    fresh = ("near", "far", "turn", "meta", "mix", "noise")
    outs = {name: n for n, name in enumerate(reused)}
    outs.update((name, len(loads) + n) for n, name in enumerate(fresh))
    spare = list(range(len(reused), len(loads)))
    spare += list(range(len(loads) + len(fresh), ssem.shape[0]))
    ins = {}

    def prepare(src, dst, peer, out, into):
        return pltpu.make_async_remote_copy(
            src_ref=src,
            dst_ref=dst,
            send_sem=ssem.at[outs[out]],
            recv_sem=rsem.at[ins.setdefault(into, len(ins))],
            device_id=peer,
            device_id_type=MESH,
        )

    def send(src, dst, peer, out, into):
        copy = prepare(src, dst, peer, out, into)
        copy.start()
        return copy

    def settle(ref, sem):
        pltpu.make_async_copy(ref, ref, sem).wait()

    def arrive(ref, into):
        settle(ref, rsem.at[ins[into]])

    for copy in loads[:3]:
        copy.wait()
    row_id = lax.broadcasted_iota(jnp.int32, (8, lanes), 0)
    lane_id = lax.broadcasted_iota(jnp.int32, (1, lanes), 1)
    hot_t = jnp.where(lane_id == tidx_ref[0], 1.0, 0.0)
    hot_s = lane_id == sidx_ref[0]
    keep = jnp.sum(jnp.where(hot_s, keep_ref[...], 0.0), axis=1, keepdims=True)
    coef = jnp.sum(jnp.where(hot_s, coef_ref[...], 0.0), axis=1, keepdims=True)
    meta_buf[s] = jnp.where(row_id == 0, hot_t, jnp.where(row_id == 1, keep, coef))
    loads[3].wait()
    gain = gain_ref[...].reshape(1, D)
    pos = pos_ref[...]
    at_ref[...] = jnp.transpose(pos.astype(F32) * gain).astype(BF16)

    def turn_weights(parts):
        for i in range(F):

            @pl.when(f == i)
            def _():
                for p in parts:
                    turned = jnp.transpose(wqkv_ref[p, :, i * 2 * B : (i + 1) * 2 * B])
                    for t in range(2):
                        wt_ref[t, p * B : (p + 1) * B] = turned[t * B : (t + 1) * B]

    for p in range(2):
        loads[4 + p].wait()
    turn_weights((0, 1))
    mine = pl.ds(pl.multiple_of(s * R, R), R)
    at_mine = at_ref[mine]
    near_send[0] = dot(wt_ref[e_near, 0:QK], at_mine).astype(BF16)
    pl.semaphore_wait(barrier, S - 1 + PL - 1)
    to_near, to_far = {"step": s_near}, {"step": s_far}
    near, far = {}, {}

    def send_near(i, low, high):
        window = pl.ds(low, high - low)
        near[i, low] = send(
            near_send.at[i, window],
            near_recv.at[i, window],
            to_near,
            "late" if i == 2 else "near",
            ("near", i, low),
        )

    pieces = [(low, low + QK // 3) for low in range(0, QK, QK // 3)]
    order = sorted(range(1, S), key=lambda d: abs(d - S / 2))
    for d in order:
        send(meta_buf.at[s], meta_buf.at[s], step_peer(d), "meta", "meta")
    send_near(0, *pieces[0])
    turn = send(at_ref.at[mine], at_peer, frame_peer, "turn", "turn")
    for piece in pieces[1:]:
        send_near(0, *piece)
    for copy in loads[7:9]:
        copy.wait()
    rows_of = wfin_ref[:, 0:R].astype(F32)
    for j in range(1, S):
        rows_of = jnp.where(s == j, wfin_ref[:, j * R : (j + 1) * R].astype(F32), rows_of)
    folded = dot(rows_of.astype(BF16), wproj_ref[...])
    picked = folded[:, 0 : 2 * B]
    for i in range(1, F):
        picked = jnp.where(f == i, folded[:, i * 2 * B : (i + 1) * 2 * B], picked)
    mix_buf[s] = picked.astype(BF16)
    for d in order:
        send(mix_buf.at[s], mix_buf.at[s], step_peer(d), "mix", "mix")
    loads[9].wait()
    sides = [send(noise_buf.at[f], noise_buf.at[f], frame_peer, "noise", "noise")]
    own_ref[0] = dot(wt_ref[e, 0:QK], at_mine)
    loads[6].wait()
    turn_weights((2,))

    def pass_on(i, low, high):
        near[i, low].wait_recv()
        total = own_ref[i, low:high] + near_recv[i, low:high].astype(F32)
        far_send[i, low:high] = total.astype(BF16)
        window = pl.ds(low, high - low)
        far[i, low] = send(
            far_send.at[i, window],
            far_recv.at[i, window],
            to_far,
            "late" if i == 2 else "far",
            ("far", i, low),
        )

    pv_ref[0, :, 0:rows] = dot(wt_ref[e, QK : QK + B], at_mine).astype(BF16)
    pv_ref[1, :, 0:rows] = dot(wt_ref[e_near, QK : QK + B], at_mine).astype(BF16)
    for copy in loads[10:]:
        copy.wait()
    w_in = win_ref[...]
    ends = jnp.concatenate([w_in, wfin_ref[...]], axis=0)
    ends_in = dot(ends, w_in, 1, 1)
    posf = pos.astype(F32)
    sq_hi, sq_lo = two(posf * posf)
    ones = jnp.ones((8, D), BF16)
    ends_buf[f, 0 : 2 * C] = dot(ends, pos, 1, 1)
    ends_buf[f, 2 * C : 2 * C + 8] = dot(ones, sq_hi, 1, 1) + dot(ones, sq_lo, 1, 1)

    for piece in pieces:
        pass_on(0, *piece)
    turn.wait_recv()
    at_other = at_peer[...]
    near_send[1] = dot(wt_ref[e_near, 0:QK], at_other).astype(BF16)
    for piece in pieces:
        send_near(1, *piece)
    own_ref[1] = dot(wt_ref[e, 0:QK], at_other)
    pv_ref[0, :, rows : 2 * rows] = dot(wt_ref[e, QK : QK + B], at_other).astype(BF16)
    pv_ref[1, :, rows : 2 * rows] = dot(wt_ref[e_near, QK : QK + B], at_other).astype(BF16)

    side_ref[0:C] = w_in.astype(F32)
    arrive(meta_buf.at[pl.ds(0, S - 1)], "meta")
    metas = [meta_buf[j] for j in range(S)]
    hot = jnp.concatenate(
        [m[0:1] for m in metas] + [jnp.zeros((8 - S, lanes), F32)], axis=0
    ).astype(BF16)
    keeps = [jnp.concatenate([m[1:2, :rows]] * F, axis=1) for m in metas]
    coefs = [jnp.concatenate([m[2:3, :rows]] * F, axis=1) for m in metas]
    temb = dot(hot, table_ref[...])
    side_ref[C : C + 8] = temb
    side_ref[C + 8 :] = jnp.zeros((32 - C - 8, D), F32)
    for j in range(S):

        @pl.when(s == j)
        def _():
            cut = slice(j * R, (j + 1) * R)
            side_cut[...] = (side_ref[:, cut] * gain[:, cut]).astype(BF16)

    side_mine = side_cut[...]
    turned_of = []
    for role, member in ((0, e), (1, e_near)):
        turned = dot(wt_ref[member], side_mine, 1, 1)
        pv_ref[role, :, 2 * rows : 2 * rows + 32] = turned[QK:].astype(BF16)
        turned_of.append(turned[0:QK])
    arrive(mix_buf.at[pl.ds(0, S - 1)], "mix")
    mix = mix_buf[0].astype(F32)
    for j in range(1, S):
        mix = mix + mix_buf[j].astype(F32)
    mix_lane = lax.broadcasted_iota(jnp.int32, (V, B), 1) // HDIM
    mix_row = lax.broadcasted_iota(jnp.int32, (V, B), 0) // C

    def late_rows(role, member):
        part = jnp.where(member == 0, mix[:, 0:B], mix[:, B : 2 * B])
        block = jnp.where(
            mix_lane == mix_row, jnp.concatenate([part] * HZ, axis=0), 0.0
        )
        block_hi, block_lo = two(block)
        values = dot(jnp.concatenate([block_hi, block_lo], axis=0), pv_ref[role])
        values = values[0:V] + values[V : 2 * V]
        packs = []
        for arr in (turned_of[role], values[:, 2 * rows : 2 * rows + 32]):
            size = arr.shape[0] // 4
            packs.append(
                jnp.concatenate([arr[g * size : (g + 1) * size] for g in range(4)], axis=1)
            )
        return jnp.concatenate(
            [values[:, 0:rows], values[:, rows : 2 * rows]] + packs, axis=0
        )

    LATE = 2 * V + (QK + V) // 4
    near_send[2, 0:LATE] = late_rows(1, e_near).astype(BF16)
    send_near(2, 0, LATE)
    own_ref[2, 0:LATE] = late_rows(0, e)
    temb_b = temb.astype(BF16)
    ends_buf[f, 2 * C + 8 : 2 * C + 16] = dot(temb_b, pos, 1, 1)
    sides.append(send(ends_buf.at[f], ends_buf.at[f], frame_peer, "ends", "ends"))
    ends_t = dot(ends, temb_b, 1, 1)
    norm_t = jnp.sum(temb * temb, axis=1, keepdims=True)
    for piece in pieces:
        pass_on(1, *piece)

    scale = 1.4426950408889634 / math.sqrt(HDIM)
    qk_row = lax.broadcasted_iota(jnp.int32, (QK, 1), 0)
    row_scale = jnp.where(qk_row < B, scale, 1.0)
    set_own, set_near = 2 * f + e, 2 * f + e_near
    halves = (f, 1 - f)

    def whole(i, low, high):
        far[i, low].wait_recv()
        total = far_send[i, low:high].astype(F32) + far_recv[i, low:high].astype(F32)
        return total.astype(BF16)

    def finish(i, low, high):
        total = whole(i, low, high)
        window = pl.ds(low, high - low)
        if i < 2:
            fin_qk[set_own, halves[i], low:high] = total
            ref = fin_qk.at[set_own, halves[i], window]
            twin = fin_qk.at[set_near, halves[i], window]
        else:
            fin_late[set_own] = total
            ref = fin_late.at[set_own]
            twin = fin_late.at[set_near]
        return ref, twin

    shared = []

    def hand_on(refs, kind):
        send(refs[0], refs[0], frame_peer, kind or "across", kind and "late" or "across")

    def share(refs, kind):
        copy = send(refs[0], refs[0], to_near, kind or "share", ("share", len(shared)))
        shared.append((copy, refs[1], kind))

    def offer(refs, kind=None):
        hand_on(refs, kind)
        share(refs, kind)

    def forward(_):
        for copy, twin, kind in shared:
            copy.wait_recv()
            send(
                twin,
                twin,
                frame_peer,
                "pass late" if kind else "pass",
                "late" if kind else "pass",
            )

    ready = [finish(0, *piece) for piece in pieces]
    pass_on(2, 0, LATE)
    for refs in ready:
        offer(refs)
    for copy in sides:
        copy.wait_recv()
    start = jnp.concatenate([noise_buf[i] for i in range(F)], axis=1)
    ends_all = jnp.concatenate([ends_buf[i] for i in range(F)], axis=1)
    ends_pos = ends_all[0 : 2 * C]
    norm_p = ends_all[2 * C : 2 * C + 1]
    cross = ends_all[2 * C + 8 : 2 * C + 16]
    norms = [norm_p + 2.0 * cross[j : j + 1] + norm_t[j : j + 1] for j in range(S)]
    for j in range(S):
        base_buf[j] = jnp.concatenate(
            [
                2.0 * (ends_pos[0:C] + ends_t[0:C, j : j + 1]),
                ends_pos[C : 2 * C] + ends_t[C : 2 * C, j : j + 1],
            ],
            axis=0,
        )
    ends_hi, ends_lo = two(
        jnp.concatenate([ends_in, jnp.zeros((2 * C, 32 - C), F32)], axis=1)
    )
    ends_big = jnp.concatenate([ends_hi, ends_lo], axis=0)
    size = QK // 4

    def build(slot, group, frame):
        last = fin_late[group].astype(F32)
        one, other = last[0:V], last[V : 2 * V]
        packed = last[2 * V : LATE]
        big_qk = jnp.concatenate(
            [packed[0:size, 32 * g : 32 * g + 32] for g in range(4)], axis=0
        )
        big_v = jnp.concatenate(
            [packed[size:, 32 * g : 32 * g + 32] for g in range(4)], axis=0
        )
        big_buf[slot, 0:QK] = (big_qk * row_scale).astype(BF16)
        big_buf[slot, QK:] = big_v.astype(BF16)
        for i in range(F):
            cut = slice(i * rows, (i + 1) * rows)
            tab_buf[slot, 0:QK, cut] = fin_qk[group, i].astype(F32) * row_scale
            tab_buf[slot, QK:, cut] = jnp.where(frame == i, one, other)

    ready = [finish(1, *piece) for piece in pieces]
    for refs in ready:
        offer(refs)
    ready = finish(2, 0, LATE)
    build(4, set_own, f)

    def share_rest(_):
        offer(ready, "late")

    hot_row = lax.broadcasted_iota(jnp.int32, (32 - C, N), 0)
    ones_rows = jnp.ones((C, N), BF16)

    def evaluate(x, j, slots):
        xb = x.astype(BF16)
        pick = jnp.where(hot_row == j, 1.0, 0.0).astype(BF16)
        x_in = jnp.concatenate([xb, pick], axis=0)
        base = base_buf[j]
        out = jnp.zeros((C, N), F32)
        items, scores, r, eps = {}, {}, None, None
        G = len(slots)
        for g in range(G + 3):
            if g < G:
                big = big_buf[slots[g]]
                if g == 0:
                    lin = dot(jnp.concatenate([ends_big, big], axis=0), x_in)
                    tail = lin[0 : 2 * C] + lin[2 * C : 4 * C]
                    lin = lin[4 * C :]
                    square = jnp.sum(
                        xb.astype(F32) * (tail[0:C] + base[0:C]), axis=0, keepdims=True
                    )
                    square = jnp.maximum(square + norms[j], 0.0)
                    r = lax.rsqrt(square * (1.0 / D) + 1e-06)
                    eps = tail[C : 2 * C] + base[C : 2 * C]
                else:
                    lin = dot(big, x_in)
                lin = (lin + tab_buf[slots[g]]) * r
                for n in range(HZ):
                    q = lin[n * HDIM : (n + 1) * HDIM].astype(BF16)
                    k = lin[B + n * HDIM : B + (n + 1) * HDIM].astype(BF16)
                    v_hi, v_lo = two(lin[QK + n * C : QK + (n + 1) * C])
                    items[g, n] = q, k, jnp.concatenate([v_hi, v_lo, ones_rows], axis=0)
            if 0 <= g - 2 < G:
                for n in range(HZ):
                    q, k, _ = items[g - 2, n]
                    scores[g - 2, n] = dot(k, q, 0, 0)
            if 0 <= g - 3 < G:
                for n in range(HZ):
                    block = scores.pop((g - 3, n))
                    top = jnp.max(block, axis=0, keepdims=True)
                    p = jnp.exp2(block - top).astype(BF16)
                    o = dot(items[g - 3, n][2], p)
                    out = out + (o[0:C] + o[C : 2 * C]) / o[2 * C : 2 * C + 1]
        return out, eps

    spread = [key for act, key in PLAN if act == "spread"]
    local = [key for act, key in PLAN if act == "local"]
    state, local_eps, drift, flying = {}, {}, {}, {}
    rounds_at = rsem.shape[0] - len(spread) - len(local)
    outward = sorted(
        range(1, 2 * PL), key=lambda d: (-(d // PL + (d % PL // H > 0)), -(d // PL))
    )

    def launch(key, slots):
        i, j = key
        x = start
        for m in range(j if i else 0):
            x = x + drift[(min(i - 1, m), m)]
        state[key] = x
        part, local_eps[key] = evaluate(x, j, slots)
        k = flying[key] = len(flying)
        if key in spread:
            slot = plane_buf.at[spread.index(key), e * PL + q_me]
            slot[...] = part.astype(BF16)
            peers = [group_peer(d) for d in outward]
        else:
            slot = chip_buf.at[local.index(key), h]
            slot[...] = part
            peers = [{"head": 1 - h}]
        for peer in peers:
            pltpu.make_async_remote_copy(
                src_ref=slot,
                dst_ref=slot,
                send_sem=ssem.at[spare[k]],
                recv_sem=rsem.at[rounds_at + k],
                device_id=peer,
                device_id_type=MESH,
            ).start()

    def land(key):
        j, k = key[1], flying[key]
        if key in spread:
            others = plane_buf.at[spread.index(key), pl.ds(0, 2 * PL - 1)]
        else:
            others = chip_buf.at[local.index(key), 0]
        settle(others, rsem.at[rounds_at + k])
        total = local_eps[key]
        if key in spread:
            for i in range(2 * PL):
                total = total + plane_buf[spread.index(key), i].astype(F32)
        else:
            for i in range(H):
                total = total + chip_buf[local.index(key), i]
        drift[key] = keeps[j] * state[key] + coefs[j] * total
        settle(others, ssem.at[spare[k]])

    def clear(_):
        for out, ref in (
            ("near", near_send.at[pl.ds(0, 2)]),
            ("far", far_send.at[pl.ds(0, 2)]),
            ("across", fin_qk.at[0]),
            ("share", fin_qk.at[0]),
            ("pass", fin_qk.at[0]),
            ("late", fin_late),
            ("pass late", fin_late.at[0]),
            ("turn", at_peer),
            ("meta", meta_buf.at[pl.ds(0, S - 1)]),
            ("mix", mix_buf.at[pl.ds(0, S - 1)]),
            ("noise", noise_buf.at[0]),
            ("ends", ends_buf.at[0]),
        ):
            settle(ref, ssem.at[outs[out]])

    def gather(_):
        build(set_own, set_own, f)
        build(set_near, set_near, f)
        arrive(fin_qk.at[0], "across")
        arrive(fin_qk.at[0], "pass")
        arrive(fin_late.at[pl.ds(0, 2)], "late")
        for member in (e, e_near):
            twin = 2 * (1 - f) + member
            build(twin, twin, 1 - f)

    def norms_now(_):
        lane = lax.broadcasted_iota(jnp.int32, res_ref.shape, 1)
        res = jnp.zeros(res_ref.shape, F32)
        old = [start] * S
        for it in range(ITERS):
            new, run = [], start
            for j in range(S):
                new.append(run)
                if j < S - 1:
                    run = run + drift[(min(it, j), j)]
            square = jnp.zeros((C, N), F32)
            for j in range(1, S):
                change = new[j] - old[j]
                square = square + change * change
            square = jnp.sum(
                jnp.sum(square, axis=0, keepdims=True), axis=1, keepdims=True
            )
            res = jnp.where(lane == it, jnp.sqrt(square / (S * C * N) + 1e-06), res)
            old = new
        res_ref[...] = res

    acts = {
        "clear": clear,
        "share": share_rest,
        "forward": forward,
        "gather": gather,
        "land": land,
        "norms": norms_now,
        "spread": lambda key: launch(key, [2 * F]),
        "local": lambda key: launch(key, list(range(2 * F))),
    }
    for act, key in PLAN:
        acts[act](key)
    final = jnp.zeros((C, N), F32)
    for j in range(S):
        final = jnp.where(s == j, state[(j, j)] + drift[(j, j)], final)
    half = final[:, 0:rows]
    for i in range(1, F):
        half = jnp.where(f == i, final[:, i * rows : (i + 1) * rows], half)
    traj_ref[0] = half


PLAN = (
    ("share", None),
    ("spread", (0, 0)),
    ("spread", (0, 1)),
    ("forward", None),
    ("land", (0, 0)),
    ("spread", (1, 1)),
    ("spread", (0, 2)),
    ("land", (0, 1)),
    ("spread", (1, 2)),
    ("gather", None),
    ("clear", None),
    ("land", (1, 1)),
    ("local", (2, 2)),
    ("land", (2, 2)),
    ("local", (3, 3)),
    ("land", (0, 2)),
    ("land", (1, 2)),
    ("norms", None),
    ("land", (3, 3)),
)


def local_heads(
    start_noise,
    position,
    time_table,
    time_index,
    sched_index,
    coef_keep,
    coef_noise,
    w_in,
    norm_gain,
    w_qkv,
    w_proj,
    w_final,
):
    S, F, H = (lax.axis_size(a) for a in ("step", "frame", "head"))
    R = w_qkv.shape[0]
    C, rows = start_noise.shape
    D = position.shape[1]
    N = rows * F
    PL = F * H
    HZ = w_qkv.shape[2] // (F * 2 * HDIM)
    B = HZ * HDIM
    QK = 2 * B
    V = HZ * C
    late = 2 * V + (QK + V) // 4
    n_spread = sum(act == "spread" for act, _ in PLAN)
    n_local = sum(act == "local" for act, _ in PLAN)
    n_evals = n_spread + n_local
    vmem = pl.BlockSpec(memory_space=pltpu.VMEM)
    smem = pl.BlockSpec(memory_space=pltpu.SMEM)
    here = pl.BlockSpec(memory_space=pl.ANY)
    traj, res = pl.pallas_call(
        functools.partial(kernel, S, F, H),
        out_shape=(pltpu.VMEM((1, C, rows), F32), pltpu.VMEM((1, ITERS), F32)),
        in_specs=[here, here, here, smem, smem] + [here] * 7,
        out_specs=(vmem, vmem),
        scratch_shapes=[
            pltpu.VMEM((rows, D), BF16),
            pltpu.VMEM(time_table.shape, BF16),
            pltpu.VMEM((1, coef_keep.shape[0]), F32),
            pltpu.VMEM((1, coef_noise.shape[0]), F32),
            pltpu.VMEM(w_in.shape, BF16),
            pltpu.VMEM((D,), F32),
            pltpu.VMEM((3, R, w_qkv.shape[2]), BF16),
            pltpu.VMEM(w_proj.shape, BF16),
            pltpu.VMEM(w_final.shape, BF16),
            pltpu.VMEM((2, QK + B, R), BF16),
            pltpu.VMEM((D, rows), BF16),
            pltpu.VMEM((R, rows), BF16),
            pltpu.VMEM((32, D), F32),
            pltpu.VMEM((32, R), BF16),
            pltpu.VMEM((2, B, N + 32), BF16),
            pltpu.VMEM((3, QK, rows), F32),
            pltpu.VMEM((3, QK, rows), BF16),
            pltpu.VMEM((3, QK, rows), BF16),
            pltpu.VMEM((3, QK, rows), BF16),
            pltpu.VMEM((3, QK, rows), BF16),
            pltpu.VMEM((S, C, 2 * B), BF16),
            pltpu.VMEM((F, C, rows), F32),
            pltpu.VMEM((S, 8, time_table.shape[0]), F32),
            pltpu.VMEM((F, 2 * C + 16, rows), F32),
            pltpu.VMEM((2 * F, F, QK, rows), BF16),
            pltpu.VMEM((2 * F, late, rows), BF16),
            pltpu.VMEM((2 * F + 1, QK + V, 32), BF16),
            pltpu.VMEM((2 * F + 1, QK + V, N), F32),
            pltpu.VMEM((S, 2 * C, N), F32),
            pltpu.VMEM((n_spread, 2 * PL, C, N), BF16),
            pltpu.VMEM((n_local, H, C, N), F32),
            pltpu.SemaphoreType.DMA((14 + 6 + n_evals - 8,)),
            pltpu.SemaphoreType.DMA((3 * 7 + 8 + n_evals,)),
        ],
        compiler_params=pltpu.CompilerParams(
            collective_id=0, has_side_effects=True, vmem_limit_bytes=60 * 1024 * 1024
        ),
    )(
        start_noise,
        position,
        time_table,
        time_index,
        sched_index,
        coef_keep[None],
        coef_noise[None],
        w_in,
        norm_gain,
        jnp.transpose(w_qkv, (1, 0, 2)),
        w_proj,
        w_final,
    )
    return traj, res.reshape(ITERS)


def one_head_each(mesh, start_noise, time_index, w_qkv, time_table):
    S, F, H = (mesh.shape[a] for a in ("step", "frame", "head"))
    return (
        S == ITERS
        and time_index.shape[0] == S
        and w_qkv.shape[2] == S * F * H * HDIM
        and w_qkv.shape[0] % (16 * S) == 0
        and F == 2
        and H == 2
        and start_noise.shape[1] == 128 * F
        and start_noise.shape[0] == 16 * mesh.shape["parts"]
        and start_noise.shape[1] // F <= time_table.shape[0]
        and time_table.shape[0] % 128 == 0
    )


def solution(mesh):
    def call(*args):
        fits = one_head_each(mesh, args[0], args[3], args[9], args[2])
        return jax.shard_map(
            local_heads if fits else local_any,
            mesh=mesh,
            in_specs=(
                P("parts", "frame"),
                P("frame", None),
                P(),
                P("step"),
                P("step"),
                P(),
                P(),
                P(),
                P(),
                P("step", None, "head"),
                P("step", "head"),
                P(),
            ),
            out_specs=(P("step", "parts", "frame"), P("parts")),
            check_vma=False,
        )(*args)

    return call
```
